128 devices in a mesh: ctx: 8 (over z, x_lo), tp: 4 (over x_hi, core), dp: 4 (over y).
Axes of the slice: x: 4 (x_hi: 2, x_lo: 2; x = x_hi * 2 + x_lo), y: 4, z: 4, core: 2. Of those that a mesh axis runs over, the one named last changes fastest.
Arguments:
- hidden: bfloat16 [4, 4096, 4096], P('dp', 'ctx', 'tp'), may hold values from -6 to 6
- target: bfloat16 [4, 4096, 4096], P('dp', 'ctx', 'tp'), may hold values from -24 to 24
- gain: float32 [4096], replicated, may hold values from 0.5 to 1.5
- w_query: bfloat16 [4096, 2048], P(('ctx', 'dp'), 'tp'), may hold values from -2.15625 to 2.15625
- w_key: bfloat16 [4096, 512], P(('ctx', 'dp'), 'tp'), may hold values from -0.09375 to 0.09375
- value_matrix: bfloat16 [4096, 512], P(('ctx', 'dp'), 'tp'), may hold values from -0.09375 to 0.09375
- w_out: bfloat16 [2048, 4096], P('tp', ('ctx', 'dp')), may hold values from -0.125 to 0.125
- block_order: int32 [16], replicated, may hold values from 0 to 15, each once
Outputs:
- branch: bfloat16 [4, 4096, 4096], P('dp', 'ctx', 'tp')
- loss: float32 [], replicated
The draws below stay inside these ranges and needn't reach their ends.
Inputs may be any that keep to these rules, and one draw needn't show every extreme that they name: block_order is a permutation of 0 to 15.
All inputs are finite; a program needn't handle non-finite values.
Results may differ from the reference program's by a relative error of at most 0.013.
The reference program's roundings to bfloat16 on the way (of `normed` and `attn`) count: a program that leaves them out, or rounds other values in their place, can miss the bound.
Values may be sent and summed in bfloat16 or wider, within the bound.
No kernel may reach another device: no remote copies, remote signals or barrier semaphores. Data moves between devices by JAX's collectives and lax.ppermute only.
A program may use at most 128 MiB of HBM per device.

```python
import math
import jax
import jax.numpy as jnp
from jax import lax

MODEL_WIDTH = 4096
QUERY_HEADS = 16
KEY_VALUE_HEADS = 4
HEAD_SIZE = 128
CH = 256
SEQUENCE_LENGTH = 4096
SEQS = 4
N_CTX = 8
N_TP = 4


def key_weights(key):
    random_jitter = jax.random.normal(jax.random.fold_in(key, 11), (MODEL_WIDTH, KEY_VALUE_HEADS * HEAD_SIZE), jnp.float32)
    return jnp.clip(random_jitter, -6.0, 6.0) / MODEL_WIDTH ** 0.5


def draw_w_key(key, part):
    return key_weights(key).astype(jnp.bfloat16)


def draw_w_query(key, part):
    random_jitter = jax.random.normal(jax.random.fold_in(key, 23), (MODEL_WIDTH, QUERY_HEADS * HEAD_SIZE), jnp.float32)
    base = jnp.clip(random_jitter, -6.0, 6.0) * (3.0 / MODEL_WIDTH ** 0.5)
    return base.astype(jnp.bfloat16)


def draw_hidden(key, part):
    base = jnp.clip(jax.random.normal(jax.random.fold_in(key, 41), (SEQS, SEQUENCE_LENGTH, MODEL_WIDTH), jnp.float32), -6.0, 6.0)
    return base.astype(jnp.bfloat16)


def draw_target(key, part):
    fraction = jnp.arange(SEQUENCE_LENGTH, dtype=jnp.float32) / (SEQUENCE_LENGTH - 1)
    scale = jnp.exp(fraction * jnp.log(6.0))
    noise = jnp.clip(jax.random.normal(jax.random.fold_in(key, 67), (SEQS, SEQUENCE_LENGTH, MODEL_WIDTH), jnp.float32), -4.0, 4.0)
    return jnp.clip(noise * scale[None, :, None], -24.0, 24.0).astype(jnp.bfloat16)


def shard_levels(rng, extent, cuts, least, largest):
    def one(dim, shards_of):
        steps = jax.random.uniform(jax.random.fold_in(jax.random.fold_in(rng, 6), dim), (shards_of,), jnp.float32, least / len(cuts), largest / len(cuts))
        return jnp.repeat(jnp.exp(steps), extent[dim] // shards_of).reshape((-1,) + (1,) * (len(extent) - dim - 1))

    factor_of = one(*cuts[0])
    for cut in cuts[1:]:
        factor_of = factor_of * one(*cut)
    return factor_of


def normal_values(own_key, extent, scale, bound, shards=(), kind=jnp.bfloat16):
    values = scale * jax.random.normal(own_key, extent, jnp.float32)
    if shards:
        values = values * shard_levels(own_key, extent, shards, -0.22, 0.18)
    return jnp.clip(values, -bound, bound).astype(kind)


def setup_inputs(seed: int = 0) -> dict:
    seeds = jax.random.split(jax.random.key(seed), 9)
    hidden = draw_hidden(jax.random.fold_in(seeds[8], 71), 0)
    target = draw_target(jax.random.fold_in(seeds[8], 71), 0)
    gain = jnp.clip(1.0 + 0.1 * jax.random.normal(seeds[2], (MODEL_WIDTH,), jnp.float32), 0.5, 1.5)
    w_query = draw_w_query(jax.random.fold_in(seeds[8], 71), 0)
    w_key = draw_w_key(jax.random.fold_in(seeds[8], 71), 0)
    value_matrix = normal_values(seeds[5], (MODEL_WIDTH, KEY_VALUE_HEADS * HEAD_SIZE), MODEL_WIDTH ** -0.5, 0.09375, ((0, 32), (1, 4)))
    w_out = normal_values(seeds[6], (QUERY_HEADS * HEAD_SIZE, MODEL_WIDTH), (QUERY_HEADS * HEAD_SIZE) ** -0.5, 0.125, ((0, 4), (1, 32)))
    block_order = jax.random.permutation(seeds[7], 2 * N_CTX).astype(jnp.int32)
    return {"hidden": hidden, "target": target, "gain": gain, "w_query": w_query, "w_key": w_key, "value_matrix": value_matrix, "w_out": w_out, "block_order": block_order}


rope_base = 500000.0

def apply_rotary(values, token_places):
    half = values.shape[-1] // 2
    freqs = rope_base ** (-(jnp.arange(half, dtype=jnp.float32) * 2.0) / values.shape[-1])
    angles = token_places.astype(jnp.float32)[:, None] * freqs[None, :]
    cosine = jnp.cos(angles)[:, None, :]
    sine = jnp.sin(angles)[:, None, :]
    first = values[..., :half]
    second = values[..., half:]
    return jnp.concatenate([first * cosine - second * sine, second * cosine + first * sine], axis=-1)

def one_sequence(states, gain, w_query, w_key, value_matrix, w_out, token_places):
    query_group = QUERY_HEADS // KEY_VALUE_HEADS
    wide = states.astype(jnp.float32)
    normed = (wide * lax.rsqrt(lax.optimization_barrier(jnp.mean(wide * wide, axis=1, keepdims=True)) + 1e-05) * gain[None, :]).astype(jnp.bfloat16)
    query_rows = jnp.dot(normed, w_query, preferred_element_type=jnp.float32)
    key = jnp.dot(normed, w_key, preferred_element_type=jnp.float32)
    value_rows = jnp.dot(normed, value_matrix, preferred_element_type=jnp.float32)
    query_rows = apply_rotary(query_rows.reshape(SEQUENCE_LENGTH, QUERY_HEADS, HEAD_SIZE), token_places).astype(jnp.bfloat16).reshape(SEQUENCE_LENGTH, KEY_VALUE_HEADS, query_group, HEAD_SIZE)
    key = apply_rotary(key.reshape(SEQUENCE_LENGTH, KEY_VALUE_HEADS, HEAD_SIZE), token_places).astype(jnp.bfloat16)
    value_rows = value_rows.astype(jnp.bfloat16).reshape(SEQUENCE_LENGTH, KEY_VALUE_HEADS, HEAD_SIZE)
    scale = 1.0 / HEAD_SIZE ** 0.5
    block_rows = math.gcd(SEQUENCE_LENGTH, 1024)

    def head_split(index):
        qhead = lax.dynamic_index_in_dim(query_rows, index, 1, False)
        khead = lax.dynamic_index_in_dim(key, index, 1, False).astype(jnp.float32)
        vhead = lax.dynamic_index_in_dim(value_rows, index, 1, False).astype(jnp.float32)

        def per_block(number):
            first_row = (number * block_rows).astype(jnp.int32)
            qpart = lax.dynamic_slice_in_dim(qhead, first_row, block_rows, 0).astype(jnp.float32)
            qplaces = lax.dynamic_slice_in_dim(token_places, first_row, block_rows, 0)
            allowed = qplaces[:, None] >= token_places[None, :]
            scores = jnp.einsum('qgd,kd->gqk', qpart, khead) * scale
            scores = jnp.where(allowed[None], scores, -1e+30)
            peak = lax.optimization_barrier(jnp.max(scores, axis=-1, keepdims=True))
            weights = jnp.where(allowed[None], jnp.exp(scores - peak), 0.0)
            total = lax.optimization_barrier(jnp.sum(weights, axis=-1))
            rounded = weights.astype(jnp.bfloat16).astype(jnp.float32)
            mixed = jnp.einsum('gqk,kd->qgd', rounded, vhead)
            return (mixed / jnp.transpose(total)[:, :, None]).astype(jnp.bfloat16)
        pieces = lax.map(per_block, jnp.arange(SEQUENCE_LENGTH // block_rows, dtype=jnp.int32))
        return pieces.reshape(SEQUENCE_LENGTH, query_group, HEAD_SIZE)
    head_list = lax.map(head_split, jnp.arange(KEY_VALUE_HEADS, dtype=jnp.int32))
    attn = jnp.transpose(head_list, (1, 0, 2, 3)).reshape(SEQUENCE_LENGTH, QUERY_HEADS * HEAD_SIZE)
    width = QUERY_HEADS * HEAD_SIZE // N_TP
    summed = jnp.zeros((SEQUENCE_LENGTH, MODEL_WIDTH), jnp.float32)
    for part in range(N_TP):
        partial_term = jnp.dot(attn[:, part * width:(part + 1) * width], w_out[part * width:(part + 1) * width], preferred_element_type=jnp.float32)
        summed = summed + partial_term.astype(jnp.bfloat16).astype(jnp.float32)
    return summed.astype(jnp.bfloat16)

def reference(hidden, target, gain, w_query, w_key, value_matrix, w_out, block_order):
    rows = jnp.arange(SEQUENCE_LENGTH, dtype=jnp.int32)
    token_places = (jnp.take(block_order, rows // CH).astype(jnp.int32) * CH + rows % CH).astype(jnp.int32)
    outputs = []
    squares = jnp.zeros((), jnp.float32)
    for index in range(SEQS):
        result = one_sequence(hidden[index], gain, w_query, w_key, value_matrix, w_out, token_places)
        outputs.append(result)
        resid = hidden[index].astype(jnp.float32) + result.astype(jnp.float32) - target[index].astype(jnp.float32)
        squares = squares + jnp.sum(resid * resid)
    loss = squares / (SEQS * SEQUENCE_LENGTH * MODEL_WIDTH)
    return (jnp.stack(outputs), loss)
```

```python
import functools

import jax
import jax.numpy as jnp
import numpy as np
from jax import lax
from jax.experimental import pallas as pl
from jax.experimental.pallas import tpu as pltpu
from jax.sharding import Mesh
from jax.sharding import PartitionSpec as P

MODEL_WIDTH = 4096
HEAD_SIZE = 128
GROUP = 4
CH = 256
ROPE_BASE = 500000.0
Z, L, H, C, Y = "ctx_0", "ctx_1", "tp_0", "tp_1", "dp"
SIZE = {Z: 4, L: 2, H: 2, C: 2, Y: 4}
BACK = (0, 1, 3, 2)
LOG2E = 1.4426950408889634


def send(value, axes, where):
    order = [a for a in (Z, L, H, C, Y) if a in axes]
    sizes = [SIZE[a] for a in order]
    pairs = []
    for i in range(int(np.prod(sizes))):
        at = dict(zip(order, (int(k) for k in np.unravel_index(i, sizes))))
        to = where(*[at[a] for a in axes])
        if to is not None:
            goal = dict(zip(axes, to))
            pairs.append((i, int(np.ravel_multi_index([goal[a] for a in order], sizes))))
    return lax.ppermute(value, tuple(order), pairs)


def swap(value):
    return send(value, (C,), lambda c: (1 - c,))


def around(value, axis):
    out = [value]
    for by in BACK[1:]:
        out.append(send(value, (axis,), lambda i, by=by: ((i + by) % 4,)))
    return out


def along_x(value, step, from_home, to_home):
    def where(h, l, c):
        if from_home is not None and (c == l) != from_home:
            return None
        x = (2 * h + l + step) % 4
        goal = x % 2 if to_home else 1 - x % 2
        return (x // 2, x % 2, goal)

    return send(value, (H, L, C), where)


def norm_project(
    info, gain, cosine, sine, own, r1, fa, fb, pb, pc, pd, *rest
):
    weights = rest[:16]
    q_ref, kv_ref, x_s, w_s, n_s, acc_s, x_sem, w_sem = rest[16:]
    home = info[0]
    z, y, c = info[5], info[6], info[7]
    waits = []
    for i, (a, b) in enumerate(zip((own, r1, fa, fb), (r1, pb, pc, pd))):
        @pl.when(home == 1)
        def _(a=a, i=i):
            pltpu.make_async_copy(a, x_s.at[i], x_sem.at[i]).start()

        @pl.when(home == 0)
        def _(b=b, i=i):
            pltpu.make_async_copy(b, x_s.at[i], x_sem.at[i]).start()

    for k, w in enumerate(weights):
        part = lax.rem(c + k // 8, 2)
        color, far = (k % 8) // 4, BACK[k % 4]
        for n, near in enumerate(BACK):
            dz, dy = (far, near) if color == 0 else (near, far)
            row = part * 512 + lax.rem(y + 4 - dy, 4) * 128 + color * 64
            copy = pltpu.make_async_copy(
                w.at[n],
                w_s.at[lax.rem(z + 4 - dz, 4), pl.ds(pl.multiple_of(row, 64), 64), :],
                w_sem.at[k * 4 + n],
            )
            copy.start()
            waits.append(copy)

    tile = 64
    acc_s[:, :128] = jnp.zeros((512, 128), jnp.float32)
    for i in range(4):
        pltpu.make_async_copy(own, x_s.at[i], x_sem.at[i]).wait()

        def squares(t, carry, i=i):
            rows = pl.ds(t * tile, tile)
            x = x_s[i, rows, :].astype(jnp.float32)
            x = x * x
            part = x[:, :128]
            for k in range(1, 8):
                part = part + x[:, k * 128 : k * 128 + 128]
            acc_s[rows, :128] += part
            return carry

        lax.fori_loop(0, 512 // tile, squares, 0)
    for copy in waits:
        copy.wait()
    mean = jnp.sum(acc_s[:, :128], axis=1, keepdims=True) * (1.0 / MODEL_WIDTH)
    acc_s[:, 640:] = jnp.broadcast_to(lax.rsqrt(mean + 1e-05), (512, 128))
    total = None
    for i in range(4):
        j = info[1 + i]

        def scale(t, carry, i=i, j=j):
            rows = pl.ds(t * tile, tile)
            x = x_s[i, rows, :].astype(jnp.float32)
            x = x * acc_s[rows, 640:641] * gain[j]
            n_s[i, rows, :] = x.astype(jnp.bfloat16)
            return carry

        lax.fori_loop(0, 512 // tile, scale, 0)
    for i in range(4):
        j = info[1 + i]
        part = jnp.dot(n_s[i], w_s[j], preferred_element_type=jnp.float32)
        if i == 0:
            acc_s[...] = part
        else:
            acc_s[...] += part
    for b in range(2):
        rows = pl.ds(b * CH, CH)
        cb, sb = cosine[rows, :], sine[rows, :]
        for h in range(GROUP + 1):
            v = acc_s[rows, h * 128 : h * 128 + 128]
            v = (v * cb + pltpu.roll(v, 64, 1) * sb).astype(jnp.bfloat16)
            if h < GROUP:
                q_ref[b, h * CH : h * CH + CH, :] = v
            else:
                kv_ref[0, rows, :] = v
        kv_ref[1, rows, :] = acc_s[rows, 640:768].astype(jnp.bfloat16)


def attention(qpos, kpos, q_ref, *rest):
    pieces = rest[:8]
    out_ref, kv_s, s_s, m_s, l_s, o_s, sem = rest[8:]
    copies = [
        pltpu.make_async_copy(p, kv_s.at[k], sem.at[k]) for k, p in enumerate(pieces)
    ]
    for copy in copies:
        copy.start()
    for copy in copies:
        copy.wait()
    size = GROUP * CH
    factor = LOG2E / HEAD_SIZE**0.5
    for b in range(2):
        here = qpos[b]
        m_s[...] = jnp.full((size, 128), -1e30, jnp.float32)
        l_s[...] = jnp.zeros((size, 128), jnp.float32)
        o_s[...] = jnp.zeros((size, 128), jnp.float32)

        def scores(n, carry, b=b, here=here):
            there = kpos[n]

            def keys():
                k = kv_s[n // 2, 0, pl.ds(pl.multiple_of((n % 2) * CH, CH), CH), :]
                return lax.dot_general(
                    q_ref[b], k, (((1,), (1,)), ((), ())), preferred_element_type=jnp.float32
                )

            def keep(s):
                s_s[n] = s
                m_s[...] = jnp.maximum(m_s[...], jnp.maximum(s[:, :128], s[:, 128:]))

            @pl.when(there < here)
            def _():
                keep(keys())

            @pl.when(there == here)
            def _():
                s = keys().reshape(GROUP, CH, CH)
                row = lax.broadcasted_iota(jnp.int32, (1, CH, CH), 1)
                col = lax.broadcasted_iota(jnp.int32, (1, CH, CH), 2)
                keep(jnp.where(row >= col, s, -1e30).reshape(size, CH))

            return carry

        lax.fori_loop(0, 16, scores, 0)
        m_s[...] = jnp.broadcast_to(jnp.max(m_s[...], axis=1, keepdims=True), (size, 128))

        def weigh(n, carry, b=b, here=here):
            @pl.when(kpos[n] <= here)
            def _():
                m = m_s[...]
                p = jnp.exp2((s_s[n] - jnp.concatenate([m, m], axis=1)) * factor)
                l_s[...] += p[:, :128] + p[:, 128:]
                v = kv_s[n // 2, 1, pl.ds(pl.multiple_of((n % 2) * CH, CH), CH), :]
                o_s[...] += jnp.dot(
                    p.astype(jnp.bfloat16), v, preferred_element_type=jnp.float32
                )

            return carry

        lax.fori_loop(0, 16, weigh, 0)
        total = jnp.sum(l_s[...], axis=1, keepdims=True)
        o = (o_s[...] / total).astype(jnp.bfloat16)
        for h in range(GROUP):
            out_ref[b * CH : b * CH + CH, h * 128 : h * 128 + 128] = o[h * CH : h * CH + CH]


def out_project(info, hidden, target, own, a1, a2, a3, a4, *rest):
    weights = rest[:4]
    out_ref, loss_ref, a_s, w_s, acc_s, a_sem, w_sem = rest[4:]
    home, z, y, l = info[0], info[5], info[6], info[7]
    waits = []
    for k, w in enumerate(weights):
        yy = lax.rem(y + 4 - BACK[k], 4)
        for n, dz in enumerate(BACK):
            zz = lax.rem(z + 4 - dz, 4)
            for i in range(2):
                col = (lax.rem(l + i, 2) * 4 + yy) * 128
                copy = pltpu.make_async_copy(
                    w.at[n, i],
                    w_s.at[zz, :, pl.ds(pl.multiple_of(col, 128), 128)],
                    w_sem.at[k * 8 + n * 2 + i],
                )
                copy.start()
                waits.append(copy)

    @pl.when(home == 1)
    def _():
        pltpu.make_async_copy(own, a_s.at[0], a_sem.at[0]).start()

    @pl.when(home == 0)
    def _():
        pltpu.make_async_copy(a4, a_s.at[0], a_sem.at[0]).start()

    for i, a in enumerate((a1, a2, a3)):
        copy = pltpu.make_async_copy(a, a_s.at[1 + i], a_sem.at[1 + i])
        copy.start()
        waits.append(copy)
    pltpu.make_async_copy(own, a_s.at[0], a_sem.at[0]).wait()
    for copy in waits:
        copy.wait()
    for i in range(4):
        part = jnp.dot(a_s[i], w_s[info[1 + i]], preferred_element_type=jnp.float32)
        part = part.astype(jnp.bfloat16).astype(jnp.float32)
        if i == 0:
            acc_s[...] = part
        else:
            acc_s[...] += part
    tile = 32
    def finish(t, carry):
        rows = pl.ds(t * tile, tile)
        branch = acc_s[rows, :].astype(jnp.bfloat16)
        out_ref[rows, :] = branch
        r = hidden[rows, :].astype(jnp.float32) + branch.astype(jnp.float32)
        r = r - target[rows, :].astype(jnp.float32)
        r = r * r
        part = r[:, :128]
        for k in range(1, 8):
            part = part + r[:, k * 128 : k * 128 + 128]
        return carry + (part[:8] + part[8:16]) + (part[16:24] + part[24:])

    loss_ref[...] = lax.fori_loop(0, 512 // tile, finish, jnp.zeros((8, 128), jnp.float32))


def kernel(body, out_shape, scratch, ins, name):
    return pl.pallas_call(
        body,
        out_shape=out_shape,
        in_specs=ins,
        out_specs=jax.tree.map(lambda s: pl.BlockSpec(memory_space=pltpu.VMEM), out_shape),
        scratch_shapes=scratch,
        compiler_params=pltpu.CompilerParams(vmem_limit_bytes=60 * 2**20),
        name=name,
    )


SMEM = pl.BlockSpec(memory_space=pltpu.SMEM)
VMEM = pl.BlockSpec(memory_space=pltpu.VMEM)
ANY = pl.BlockSpec(memory_space=pl.ANY)


def shape(*dims, kind=jnp.bfloat16):
    return jax.ShapeDtypeStruct(dims, kind)


def on_device(hidden, target, gain, w_query, w_key, value_matrix, w_out, block_order):
    z, l, h, c, y = (lax.axis_index(a) for a in (Z, L, H, C, Y))
    home = (c == l).astype(jnp.int32)
    x = 2 * h + l
    left, right = ((x + 3) % 4) // 2, ((x + 1) % 4) // 2
    local = hidden[0]
    r1 = send(
        local,
        (H, L, C),
        lambda h, l, c: (
            ((2 * h + l + 1) % 4 // 2, 1 - l, l) if c == l else (h, l, l)
        ),
    )
    pb = along_x(local, -1, False, False)
    pc = along_x(local, 1, False, False)
    pd = along_x(local, -1, True, False)
    fa = along_x(r1, 1, False, True)
    fb = along_x(pb, -1, False, True)
    at_home = jnp.stack([2 * h + l, 2 * h + 1 - l, 2 * (1 - h) + l, 2 * (1 - h) + 1 - l])
    at_guest = jnp.stack([2 * left + 1 - l, 2 * right + l, 2 * left + l, 2 * right + 1 - l])
    chunk = jnp.where(home == 1, at_home, at_guest)
    w = jnp.concatenate([w_query, w_key, value_matrix], axis=1)
    w = send(w, (L, C), lambda l, c: (c, l))
    wa = around(jnp.stack(around(w[:64], Y)), Z)
    wb = around(jnp.stack(around(w[64:], Z)), Y)
    weights = wa + wb
    weights = weights + [swap(v) for v in weights]
    def turn(flip):
        return send(
            w_out,
            (Z, L, H, C),
            lambda z, l, h, c: (2 * h + c, (l + flip) % 2, z // 2, z % 2),
        )

    outs = around(jnp.stack(around(jnp.stack([turn(0), turn(1)]), Z)), Y)
    slots = lax.iota(jnp.int32, 16)

    def places(index):
        return jnp.sum(jnp.where(index[:, None] == slots[None, :], block_order[None, :], 0), axis=1)

    first = (z * 2 + c) * 2
    qpos = places(first + lax.iota(jnp.int32, 2))
    back = jnp.array(BACK, jnp.int32)
    zs = (z + 4 - back) % 4
    starts = jnp.concatenate([(zs * 2 + c) * 2, (zs * 2 + 1 - c) * 2])
    kpos = places((starts[:, None] + lax.iota(jnp.int32, 2)[None, :]).reshape(16))
    rows = (qpos[:, None] * CH + lax.iota(jnp.int32, CH)[None, :]).reshape(512)
    half = HEAD_SIZE // 2
    freqs = ROPE_BASE ** (-(jnp.arange(half, dtype=jnp.float32) * 2.0) / HEAD_SIZE)
    angles = rows.astype(jnp.float32)[:, None] * freqs[None, :]
    cosine, sine = jnp.cos(angles), jnp.sin(angles)
    cosine = jnp.concatenate([cosine, cosine], axis=1)
    sine = jnp.concatenate([-sine, sine], axis=1)
    info = jnp.concatenate([home[None], chunk, jnp.stack([z, y, c])]).astype(jnp.int32)
    q, kv = kernel(
        norm_project,
        (shape(2, GROUP * CH, HEAD_SIZE), shape(2, 512, HEAD_SIZE)),
        [
            pltpu.VMEM((4, 512, 1024), jnp.bfloat16),
            pltpu.VMEM((4, 1024, 768), jnp.bfloat16),
            pltpu.VMEM((4, 512, 1024), jnp.bfloat16),
            pltpu.VMEM((512, 768), jnp.float32),
            pltpu.SemaphoreType.DMA((4,)),
            pltpu.SemaphoreType.DMA((64,)),
        ],
        [SMEM, VMEM, VMEM, VMEM] + [ANY] * 23,
        "norm_project",
    )(info, gain.reshape(4, 1, 1024), cosine, sine, local, r1, fa, fb, pb, pc, pd, *weights)
    mine = around(kv, Z)
    pieces = mine + [swap(v) for v in mine]
    attn = kernel(
        attention,
        shape(512, GROUP * HEAD_SIZE),
        [
            pltpu.VMEM((8, 2, 512, HEAD_SIZE), jnp.bfloat16),
            pltpu.VMEM((16, GROUP * CH, CH), jnp.float32),
            pltpu.VMEM((GROUP * CH, 128), jnp.float32),
            pltpu.VMEM((GROUP * CH, 128), jnp.float32),
            pltpu.VMEM((GROUP * CH, 128), jnp.float32),
            pltpu.SemaphoreType.DMA((8,)),
        ],
        [SMEM, SMEM, VMEM] + [ANY] * 8,
        "attention",
    )(qpos.astype(jnp.int32), kpos.astype(jnp.int32), q, *pieces)
    def first_hop(h, l, c):
        step = 2 if c == l else 1
        x = (2 * h + l + step) % 4
        return (x // 2, x % 2, x % 2 if c == l else 1 - x % 2)

    def second_hop(h, l, c):
        if c == l:
            return (h, l, 1 - l)
        x = (2 * h + l + 3) % 4
        return (x // 2, x % 2, x % 2)

    a1 = send(attn, (H, L, C), first_hop)
    a2 = send(attn, (H, L, C), second_hop)
    a3 = swap(a1)
    a4 = send(a2, (L, C), lambda l, c: (l, 1 - l) if c == l else None)
    at_home = jnp.stack([x, x + 2, x + 1, x + 3])
    at_guest = jnp.stack([x + 1, x + 3, x, x + 2])
    groups = jnp.where(home == 1, at_home, at_guest) % 4
    info = jnp.concatenate([home[None], groups, jnp.stack([z, y, l])]).astype(jnp.int32)
    branch, squares = kernel(
        out_project,
        (shape(512, 1024), shape(8, 128, kind=jnp.float32)),
        [
            pltpu.VMEM((4, 512, 512), jnp.bfloat16),
            pltpu.VMEM((4, 512, 1024), jnp.bfloat16),
            pltpu.VMEM((512, 1024), jnp.float32),
            pltpu.SemaphoreType.DMA((4,)),
            pltpu.SemaphoreType.DMA((32,)),
        ],
        [SMEM, VMEM, VMEM] + [ANY] * 9,
        "out_project",
    )(info, local, target[0], attn, a1, a2, a3, a4, *outs)
    squares = squares + swap(squares)
    v = [squares] + [
        send(squares, (H, L), lambda h, l, k=k: ((2 * h + l + k) % 4 // 2, (l + k) % 2))
        for k in (1, 2, 3)
    ]
    squares = (v[0] + v[2]) + (v[1] + v[3])
    for axis in (Y, Z):
        v = around(squares, axis)
        squares = (v[0] + v[3]) + (v[1] + v[2])
    loss = jnp.sum(squares) / (4 * 4096 * MODEL_WIDTH)
    return (branch[None], loss)


def solution(mesh):
    split = Mesh(mesh.devices.reshape(4, 2, 2, 2, 4), (Z, L, H, C, Y))
    rows = P(Y, (Z, L), (H, C))
    weight = P((Z, L, Y), (H, C))
    return jax.shard_map(
        on_device,
        mesh=split,
        in_specs=(rows, rows, P(), weight, weight, weight, P((H, C), (Z, L, Y)), P()),
        out_specs=(rows, P()),
        check_vma=False,
    )
```

```python
import jax
import jax.numpy as jnp
import numpy as np
from jax import lax
from jax.experimental import pallas as pl
from jax.experimental.pallas import tpu as pltpu
from jax.sharding import Mesh
from jax.sharding import PartitionSpec as P

MODEL_WIDTH = 4096
HEAD_SIZE = 128
CH = 256
ROPE_BASE = 500000.0
Z, L, H, C, Y = "ctx_0", "ctx_1", "tp_0", "tp_1", "dp"
SIZE = {Z: 4, L: 2, H: 2, C: 2, Y: 4}
BACK = (0, 1, 3, 2)
LOG2E = 1.4426950408889634


def send(value, axes, where):
    order = [a for a in (Z, L, H, C, Y) if a in axes]
    sizes = [SIZE[a] for a in order]
    pairs = []
    for i in range(int(np.prod(sizes))):
        at = dict(zip(order, (int(k) for k in np.unravel_index(i, sizes))))
        to = where(*[at[a] for a in axes])
        if to is not None:
            goal = dict(zip(axes, to))
            pairs.append((i, int(np.ravel_multi_index([goal[a] for a in order], sizes))))
    return lax.ppermute(value, tuple(order), pairs)


def swap(value):
    return send(value, (C,), lambda c: (1 - c,))


def around(value, axis):
    out = [value]
    for by in BACK[1:]:
        out.append(send(value, (axis,), lambda i, by=by: ((i + by) % 4,)))
    return out


def along_x(value, step):
    def where(h, l):
        x = (2 * h + l + step) % 4
        return (x // 2, x % 2)

    return send(value, (H, L), where)


def norm_project(info, gain, cosine, sine, own, d0, sa, da, sb, db, fa, fb, dfa, dfb, w, *rest):
    q_ref, kv_ref, x_s, w_s, r_s, x_sem, w_sem = rest
    c, h, ha, hb = info[0], info[1], info[2], info[3]
    moves = []
    for src, rows, size, far, other in (
        (own, 0, 512, h, 0), (d0, 0, 512, h, 1),
        (sa, 512, 512, ha, 0), (da, 512, 512, ha, 1),
        (sb, 512, 512, hb, 0), (db, 512, 512, hb, 1),
        (fa, 0, 256, 1 - h, 0), (fb, 256, 256, 1 - h, 0),
        (dfa, 0, 256, 1 - h, 1), (dfb, 256, 256, 1 - h, 1),
    ):
        j = 2 * far + (c if other == 0 else 1 - c)
        col = pl.multiple_of(j * 1024, 1024)
        copy = pltpu.make_async_copy(
            src, x_s.at[pl.ds(rows, size), pl.ds(col, 1024)], x_sem.at[len(moves)]
        )
        copy.start()
        moves.append((copy, rows, size, col))
    waits = []
    for z in range(4):
        for y in range(4):
            for i in range(2):
                part = c if i == 0 else 1 - c
                row = z * 1024 + part * 512 + y * 128
                copy = pltpu.make_async_copy(
                    w.at[z * 4 + y, i],
                    w_s.at[pl.ds(pl.multiple_of(row, 128), 128), :],
                    w_sem.at[len(waits)],
                )
                copy.start()
                waits.append(copy)
    tile = 64
    r_s[...] = jnp.zeros((1024, 128), jnp.float32)
    for copy, first, size, col in moves:
        copy.wait()

        def squares(t, carry, first=first, col=col):
            rows = pl.ds(pl.multiple_of(first + t * tile, tile), tile)
            part = r_s[rows, :]
            for k in range(8):
                x = x_s[rows, pl.ds(col + k * 128, 128)].astype(jnp.float32)
                part = part + x * x
            r_s[rows, :] = part
            return carry

        lax.fori_loop(0, size // tile, squares, 0)
    mean = jnp.sum(r_s[...], axis=1, keepdims=True) * (1.0 / MODEL_WIDTH)
    r_s[...] = jnp.broadcast_to(lax.rsqrt(mean + 1e-05), (1024, 128))

    def scale(t, carry):
        rows = pl.ds(pl.multiple_of(t * 32, 32), 32)
        r = r_s[rows, :]
        for k in range(32):
            cols = slice(k * 128, k * 128 + 128)
            x = x_s[rows, cols].astype(jnp.float32)
            x_s[rows, cols] = (x * r * gain[:, cols]).astype(jnp.bfloat16)
        return carry

    lax.fori_loop(0, 32, scale, 0)
    for copy in waits:
        copy.wait()
    for b in range(4):
        rows = pl.ds(b * CH, CH)
        out = jnp.dot(x_s[rows, :], w_s[...], preferred_element_type=jnp.float32)
        cb, sb = cosine[0, rows, :], sine[0, rows, :]
        for i in range(2):
            v = out[:, i * 128 : i * 128 + 128]
            v = (v * cb + pltpu.roll(v, 64, 1) * sb).astype(jnp.bfloat16)
            q_ref[b, i * CH : i * CH + CH, :] = v
        v = out[:, 256:]
        v = v * cosine[1, rows, :] + pltpu.roll(v, 64, 1) * sine[1, rows, :]
        kv_ref[rows, :] = v.astype(jnp.bfloat16)


def attention(qpos, where, q_ref, *rest):
    pieces = rest[:8]
    near_ref, far_ref, kv_s, s_s, m_s, l_s, o_s, sem = rest[8:]
    c = qpos[4]
    copies = []
    for k, piece in enumerate(pieces):
        kind = c if k < 4 else 1 - c
        copies.append(
            pltpu.make_async_copy(
                piece, kv_s.at[kind, pl.ds((k % 4) * 1024, 1024), :], sem.at[k]
            )
        )
        copies[-1].start()
    for copy in copies:
        copy.wait()
    size = 2 * CH
    factor = LOG2E / HEAD_SIZE**0.5

    def one_block(b, carry):
        here = qpos[b]
        m_s[...] = jnp.full((size, 128), -1e30, jnp.float32)
        l_s[...] = jnp.zeros((size, 128), jnp.float32)
        o_s[...] = jnp.zeros((size, 128), jnp.float32)

        def keys(kind, p):
            return kv_s[kind, pl.ds(pl.multiple_of(where[p] * CH, CH), CH), :]

        def dots(t):
            return [
                lax.dot_general(
                    q_ref[b],
                    keys(0, 2 * t + i),
                    (((1,), (1,)), ((), ())),
                    preferred_element_type=jnp.float32,
                )
                for i in range(2)
            ]

        def keep(t, s0, s1):
            s_s[2 * t] = s0
            s_s[2 * t + 1] = s1
            top = jnp.maximum(
                jnp.maximum(s0[:, :128], s0[:, 128:]), jnp.maximum(s1[:, :128], s1[:, 128:])
            )
            m_s[...] = jnp.maximum(m_s[...], top)

        def scores(t, carry):
            keep(t, *dots(t))
            return carry

        pairs = here // 2
        lax.fori_loop(0, pairs, scores, 0)
        s0, s1 = dots(pairs)
        row = lax.rem(lax.broadcasted_iota(jnp.int32, (size, CH), 0), CH)
        gap = row - lax.broadcasted_iota(jnp.int32, (size, CH), 1) + (here - 2 * pairs) * CH
        keep(pairs, jnp.where(gap >= 0, s0, -1e30), jnp.where(gap >= CH, s1, -1e30))
        m_s[...] = jnp.broadcast_to(jnp.max(m_s[...], axis=1, keepdims=True), (size, 128))

        def weigh(t, carry):
            m = m_s[...]
            total = l_s[...]
            acc = o_s[...]
            for i in range(2):
                s = s_s[2 * t + i]
                p0 = jnp.exp2((s[:, :128] - m) * factor)
                p1 = jnp.exp2((s[:, 128:] - m) * factor)
                total = total + (p0 + p1)
                p = jnp.concatenate([p0, p1], axis=1).astype(jnp.bfloat16)
                acc = acc + jnp.dot(p, keys(1, 2 * t + i), preferred_element_type=jnp.float32)
            l_s[...] = total
            o_s[...] = acc
            return carry

        lax.fori_loop(0, pairs + 1, weigh, 0)
        total = jnp.sum(l_s[...], axis=1, keepdims=True)
        o_s[...] = o_s[...] / total
        rows = pl.ds(pl.multiple_of(lax.rem(b, 2) * CH, CH), CH)

        @pl.when(b < 2)
        def _():
            for i in range(2):
                near_ref[rows, i * 128 : i * 128 + 128] = o_s[
                    i * CH : i * CH + CH, :
                ].astype(jnp.bfloat16)

        @pl.when(b >= 2)
        def _():
            for i in range(2):
                far_ref[rows, i * 128 : i * 128 + 128] = o_s[
                    i * CH : i * CH + CH, :
                ].astype(jnp.bfloat16)

        return carry

    lax.fori_loop(0, 4, one_block, 0)


def out_project(info, hidden, target, *rest):
    pieces = rest[:8]
    weights = rest[8:12]
    out_ref, loss_ref, a_s, w_s, sem = rest[12:]
    c, z, y, l, x = info[0], info[1], info[2], info[3], info[4]
    waits = []

    def start(src, dst):
        copy = pltpu.make_async_copy(src, dst, sem.at[len(waits)])
        copy.start()
        waits.append(copy)

    for k, piece in enumerate(pieces):
        group = lax.rem(x + (0, 3, 1, 2)[k % 4], 4)
        core = c if k < 4 else 1 - c
        col = pl.multiple_of(group * 512 + core * 256, 256)
        start(piece, a_s.at[:, pl.ds(col, 256)])
    for i in range(2):
        for k, w in enumerate(weights):
            yy = lax.rem(y + 4 - BACK[k], 4)
            for n, dz in enumerate(BACK):
                zz = lax.rem(z + 4 - dz, 4)
                col = (lax.rem(l + i, 2) * 4 + yy) * 128
                start(
                    w.at[n, i],
                    w_s.at[
                        pl.ds(pl.multiple_of(zz * 512, 512), 512),
                        pl.ds(pl.multiple_of(col, 128), 128),
                    ],
                )
    for copy in waits:
        copy.wait()
    loss = jnp.zeros((8, 128), jnp.float32)
    for t in range(4):
        cols = slice(t * 256, t * 256 + 256)
        branch = jnp.dot(
            a_s[...], w_s[:, cols], preferred_element_type=jnp.float32
        ).astype(jnp.bfloat16)
        out_ref[:, cols] = branch
        r = hidden[:, cols].astype(jnp.float32) + branch.astype(jnp.float32)
        r = r - target[:, cols].astype(jnp.float32)
        r = (r * r).reshape(64, 8, 256)
        r = jnp.sum(r, axis=0)
        loss = loss + (r[:, :128] + r[:, 128:])
    loss_ref[...] = loss


def kernel(body, out_shape, scratch, ins):
    return pl.pallas_call(
        body,
        out_shape=out_shape,
        in_specs=ins,
        out_specs=jax.tree.map(lambda s: pl.BlockSpec(memory_space=pltpu.VMEM), out_shape),
        scratch_shapes=scratch,
        compiler_params=pltpu.CompilerParams(vmem_limit_bytes=60 * 2**20),
    )


SMEM = pl.BlockSpec(memory_space=pltpu.SMEM)
VMEM = pl.BlockSpec(memory_space=pltpu.VMEM)
ANY = pl.BlockSpec(memory_space=pl.ANY)


def shape(*dims, kind=jnp.bfloat16):
    return jax.ShapeDtypeStruct(dims, kind)


def body(hidden, target, gain, w_query, w_key, value_matrix, w_out, block_order):
    z, l, h, c, y = (lax.axis_index(a) for a in (Z, L, H, C, Y))
    x = 2 * h + l
    local = hidden[0]
    w0 = jnp.concatenate([w_query[:, :256], w_key], axis=1)
    w1 = jnp.concatenate([w_query[:, 256:], value_matrix], axis=1)
    wa = send(jnp.where(l == 0, w0, w1), (L, C), lambda l, c: (c, l))
    wb = send(jnp.where(l == 0, w1, w0), (L, C), lambda l, c: (c, 1 - l))
    w = jnp.stack([wa, wb])
    w = jnp.broadcast_to(w[None], (16,) + w.shape)
    w = lax.all_to_all(w, (Z, Y), 0, 0, tiled=True)
    sa = along_x(local, 1)
    sb = along_x(local, -1)
    d0 = swap(local)
    fa = along_x(sa[:256], 1)
    fb = along_x(sb[256:], -1)
    da, db = swap(sa), swap(sb)
    dfa, dfb = swap(fa), swap(fb)

    def turn(flip):
        return send(
            w_out, (Z, L, H, C), lambda z, l, h, c: (2 * h + c, (l + flip) % 2, z // 2, z % 2)
        )

    outs = around(jnp.stack(around(jnp.stack([turn(0), turn(1)]), Z)), Y)
    slots = lax.iota(jnp.int32, 16)

    def places(index):
        return jnp.sum(jnp.where(index[:, None] == slots[None, :], block_order[None, :], 0), axis=1)

    two = lax.iota(jnp.int32, 2)
    sides = jnp.stack([l, 1 - l])
    zs = (z + 4 - jnp.array(BACK, jnp.int32)) % 4
    index = (zs[:, None, None] * 2 + sides[None, :, None]) * 2 + two[None, None, :]
    kpos = places(index.reshape(16))
    qpos = kpos[:4]
    inverse = jnp.sum(jnp.where(kpos[None, :] == slots[:, None], slots[None, :], 0), axis=1)
    rows = (qpos[:, None] * CH + lax.iota(jnp.int32, CH)[None, :]).reshape(1024)
    half = HEAD_SIZE // 2
    freqs = ROPE_BASE ** (-(jnp.arange(half, dtype=jnp.float32) * 2.0) / HEAD_SIZE)
    angles = rows.astype(jnp.float32)[:, None] * freqs[None, :]
    cosine, sine = jnp.cos(angles), jnp.sin(angles)
    cosine = jnp.concatenate([cosine, cosine], axis=1)
    sine = jnp.concatenate([-sine, sine], axis=1)
    cosine = jnp.stack([cosine, jnp.where(c == 0, cosine, 1.0)])
    sine = jnp.stack([sine, jnp.where(c == 0, sine, 0.0)])
    info = jnp.stack([c, h, ((x + 3) % 4) // 2, ((x + 1) % 4) // 2]).astype(jnp.int32)
    q, kv = kernel(
        norm_project,
        (shape(4, 2 * CH, HEAD_SIZE), shape(1024, HEAD_SIZE)),
        [
            pltpu.VMEM((1024, 4096), jnp.bfloat16),
            pltpu.VMEM((4096, 384), jnp.bfloat16),
            pltpu.VMEM((1024, 128), jnp.float32),
            pltpu.SemaphoreType.DMA((10,)),
            pltpu.SemaphoreType.DMA((32,)),
        ],
        [SMEM, VMEM, VMEM, VMEM] + [ANY] * 11,
    )(
        info, gain.reshape(1, MODEL_WIDTH), cosine, sine,
        local, d0, sa, da, sb, db, fa, fb, dfa, dfb, w,
    )
    mine = around(kv, Z)
    pieces = mine + [swap(v) for v in mine]
    near, far = kernel(
        attention,
        (shape(512, 256), shape(512, 256)),
        [
            pltpu.VMEM((2, 4096, HEAD_SIZE), jnp.bfloat16),
            pltpu.VMEM((16, 2 * CH, CH), jnp.float32),
            pltpu.VMEM((2 * CH, 128), jnp.float32),
            pltpu.VMEM((2 * CH, 128), jnp.float32),
            pltpu.VMEM((2 * CH, 128), jnp.float32),
            pltpu.SemaphoreType.DMA((8,)),
        ],
        [SMEM, SMEM, VMEM] + [ANY] * 8,
    )(jnp.concatenate([qpos, c[None]]).astype(jnp.int32), inverse.astype(jnp.int32), q, *pieces)
    got = [near, along_x(far, 1), along_x(far, -1), along_x(near, 2)]
    got = got + [swap(v) for v in got]
    info = jnp.stack([c, z, y, l, x]).astype(jnp.int32)
    branch, squares = kernel(
        out_project,
        (shape(512, 1024), shape(8, 128, kind=jnp.float32)),
        [
            pltpu.VMEM((512, 2048), jnp.bfloat16),
            pltpu.VMEM((2048, 1024), jnp.bfloat16),
            pltpu.SemaphoreType.DMA((40,)),
        ],
        [SMEM, VMEM, VMEM] + [ANY] * 12,
    )(info, local, target[0], *got, *outs)
    squares = jnp.broadcast_to(squares[None], (128, 8, 128)).reshape(1024, 128)
    squares = lax.all_to_all(squares, (Z, L, H, C, Y), 0, 0, tiled=True)
    loss = jnp.sum(squares) / (4 * 4096 * MODEL_WIDTH)
    return (branch[None], loss)


def solution(mesh):
    split = Mesh(mesh.devices.reshape(4, 2, 2, 2, 4), (Z, L, H, C, Y))
    rows = P(Y, (Z, L), (H, C))
    weight = P((Z, L, Y), (H, C))
    return jax.shard_map(
        body,
        mesh=split,
        in_specs=(rows, rows, P(), weight, weight, weight, P((H, C), (Z, L, Y)), P()),
        out_specs=(rows, P()),
        check_vma=False,
    )
```

```python
import functools

import jax
import jax.numpy as jnp
import numpy as np
from jax import lax
from jax.experimental import pallas as pl
from jax.experimental.pallas import tpu as pltpu
from jax.sharding import Mesh
from jax.sharding import PartitionSpec as P

MODEL_WIDTH = 4096
HEAD_SIZE = 128
CH = 256
ROPE_BASE = 500000.0
Z, L, H, C, Y = "ctx_0", "ctx_1", "tp_0", "tp_1", "dp"
SIZE = {Z: 4, L: 2, H: 2, C: 2, Y: 4}
BACK = (0, 1, 3, 2)
LOG2E = 1.4426950408889634


def send(value, axes, where):
    order = [a for a in (Z, L, H, C, Y) if a in axes]
    sizes = [SIZE[a] for a in order]
    pairs = []
    for i in range(int(np.prod(sizes))):
        at = dict(zip(order, (int(k) for k in np.unravel_index(i, sizes))))
        to = where(*[at[a] for a in axes])
        if to is not None:
            goal = dict(zip(axes, to))
            pairs.append((i, int(np.ravel_multi_index([goal[a] for a in order], sizes))))
    return lax.ppermute(value, tuple(order), pairs)


def swap(value):
    return send(value, (C,), lambda c: (1 - c,))


def around(value, axis):
    out = [value]
    for by in BACK[1:]:
        out.append(send(value, (axis,), lambda i, by=by: ((i + by) % 4,)))
    return out


def along_x(value, step):
    def where(h, l):
        x = (2 * h + l + step) % 4
        return (x // 2, x % 2)

    return send(value, (H, L), where)


def norm(layout, info, gain, *rest):
    count = len(layout)
    sources = rest[:count]
    out_ref, r_s, sem = rest[count:]
    moves = []
    for src, (slot, rows, size) in zip(sources, layout):
        col = pl.multiple_of(info[slot] * 1024, 1024)
        copy = pltpu.make_async_copy(
            src, out_ref.at[pl.ds(rows, size), pl.ds(col, 1024)], sem.at[len(moves)]
        )
        copy.start()
        moves.append((copy, rows, size, col))
    tile = 64
    r_s[...] = jnp.zeros((512, 128), jnp.float32)
    for copy, first, size, col in moves:
        copy.wait()

        def squares(t, carry, first=first, col=col):
            rows = pl.ds(pl.multiple_of(first + t * tile, tile), tile)
            part = r_s[rows, :]
            for k in range(8):
                x = out_ref[rows, pl.ds(col + k * 128, 128)].astype(jnp.float32)
                part = part + x * x
            r_s[rows, :] = part
            return carry

        lax.fori_loop(0, size // tile, squares, 0)
    mean = jnp.sum(r_s[...], axis=1, keepdims=True) * (1.0 / MODEL_WIDTH)
    r_s[...] = jnp.broadcast_to(lax.rsqrt(mean + 1e-05), (512, 128))

    def scale(t, carry):
        rows = pl.ds(pl.multiple_of(t * 32, 32), 32)
        r = r_s[rows, :]
        for k in range(32):
            cols = slice(k * 128, k * 128 + 128)
            x = out_ref[rows, cols].astype(jnp.float32)
            out_ref[rows, cols] = (x * r * gain[:, cols]).astype(jnp.bfloat16)
        return carry

    lax.fori_loop(0, 16, scale, 0)


def project(first, width, info, cosine, sine, near, far, w, out_ref, w_s, sem):
    c = info[4]
    waits = []
    for z in range(4):
        for y in range(4):
            for i in range(2):
                part = c if i == 0 else 1 - c
                row = z * 1024 + part * 512 + y * 128
                copy = pltpu.make_async_copy(
                    w.at[z * 4 + y, i, :, pl.ds(first, width)],
                    w_s.at[pl.ds(pl.multiple_of(row, 128), 128), :],
                    sem.at[len(waits)],
                )
                copy.start()
                waits.append(copy)
    for copy in waits:
        copy.wait()
    for side, n in enumerate((near, far)):
        out = jnp.dot(n[...], w_s[...], preferred_element_type=jnp.float32)
        rows = pl.ds(side * 512, 512)
        cs, sn = cosine[rows, :], sine[rows, :]
        cb = jnp.concatenate([cs, cs], axis=1)
        sb = jnp.concatenate([-sn, sn], axis=1)
        for i in range(width // 128):
            v = out[:, i * 128 : i * 128 + 128]
            turned = v * cb + pltpu.roll(v, 64, 1) * sb
            if width == 128:
                out_ref[rows, :] = jnp.where(c == 0, turned, v).astype(jnp.bfloat16)
            else:
                turned = turned.astype(jnp.bfloat16)
                for b in range(2):
                    out_ref[side * 2 + b, i * CH : i * CH + CH, :] = turned[
                        b * CH : b * CH + CH
                    ]


def attention(first, qpos, where, q_ref, *rest):
    pieces = rest[:8]
    out_ref, kv_s, s_s, m_s, l_s, o_s, sem = rest[8:]
    c = qpos[4]
    copies = []
    for k, piece in enumerate(pieces):
        kind = c if k < 4 else 1 - c
        copies.append(
            pltpu.make_async_copy(
                piece, kv_s.at[kind, pl.ds((k % 4) * 1024, 1024), :], sem.at[k]
            )
        )
        copies[-1].start()
    size = 2 * CH
    factor = LOG2E / HEAD_SIZE**0.5
    m_s[...] = jnp.full((2, size, 128), -1e30, jnp.float32)
    l_s[...] = jnp.zeros((2, size, 128), jnp.float32)
    o_s[...] = jnp.zeros((2, size, 128), jnp.float32)
    for copy in copies:
        copy.wait()
    here = [qpos[first], qpos[first + 1]]
    pairs = [here[0] // 2, here[1] // 2]

    def keys(kind, p):
        return kv_s[kind, pl.ds(pl.multiple_of(where[p] * CH, CH), CH), :]

    def dots(b, t):
        return [
            lax.dot_general(
                q_ref[first + b],
                keys(0, 2 * t + i),
                (((1,), (1,)), ((), ())),
                preferred_element_type=jnp.float32,
            )
            for i in range(2)
        ]

    def keep(b, t, s0, s1):
        s_s[b, 2 * t] = s0
        s_s[b, 2 * t + 1] = s1
        top = jnp.maximum(
            jnp.maximum(s0[:, :128], s0[:, 128:]), jnp.maximum(s1[:, :128], s1[:, 128:])
        )
        m_s[b] = jnp.maximum(m_s[b], top)

    def scores(b, t):
        keep(b, t, *dots(b, t))

    def last_scores(b):
        t = pairs[b]
        s0, s1 = dots(b, t)
        row = lax.rem(lax.broadcasted_iota(jnp.int32, (size, CH), 0), CH)
        gap = row - lax.broadcasted_iota(jnp.int32, (size, CH), 1) + (here[b] - 2 * t) * CH
        keep(b, t, jnp.where(gap >= 0, s0, -1e30), jnp.where(gap >= CH, s1, -1e30))
        m_s[b] = jnp.broadcast_to(jnp.max(m_s[b], axis=1, keepdims=True), (size, 128))

    def weigh(b, t):
        m = m_s[b]
        total = l_s[b]
        acc = o_s[b]
        for i in range(2):
            s = s_s[b, 2 * t + i]
            p0 = jnp.exp2((s[:, :128] - m) * factor)
            p1 = jnp.exp2((s[:, 128:] - m) * factor)
            total = total + (p0 + p1)
            p = jnp.concatenate([p0, p1], axis=1).astype(jnp.bfloat16)
            acc = acc + jnp.dot(p, keys(1, 2 * t + i), preferred_element_type=jnp.float32)
        l_s[b] = total
        o_s[b] = acc

    def store(b):
        total = jnp.sum(l_s[b], axis=1, keepdims=True)
        o = (o_s[b] / total).astype(jnp.bfloat16)
        for i in range(2):
            out_ref[b * CH : b * CH + CH, i * 128 : i * 128 + 128] = o[i * CH : i * CH + CH]

    def loop(low, high, *work):
        def step(t, carry):
            for f, b in work:
                f(b, t)
            return carry

        lax.fori_loop(low, high, step, 0)

    loop(0, pairs[0], (scores, 0))
    last_scores(0)
    both = jnp.minimum(pairs[0] + 1, pairs[1])
    loop(0, both, (scores, 1), (weigh, 0))
    loop(both, pairs[1], (scores, 1))
    loop(both, pairs[0] + 1, (weigh, 0))
    store(0)
    last_scores(1)
    loop(0, pairs[1] + 1, (weigh, 1))
    store(1)


def out_project(info, hidden, target, *rest):
    pieces = rest[:8]
    weights = rest[8:12]
    out_ref, loss_ref, a_s, w_s, sem = rest[12:]
    c, z, y, l, x = info[0], info[1], info[2], info[3], info[4]
    waits = []

    def start(src, dst):
        copy = pltpu.make_async_copy(src, dst, sem.at[len(waits)])
        copy.start()
        waits.append(copy)

    for k, piece in enumerate(pieces):
        group = lax.rem(x + (0, 3, 1, 2)[k % 4], 4)
        core = c if k < 4 else 1 - c
        col = pl.multiple_of(group * 512 + core * 256, 256)
        start(piece, a_s.at[:, pl.ds(col, 256)])
    for i in range(2):
        for k, w in enumerate(weights):
            yy = lax.rem(y + 4 - BACK[k], 4)
            for n, dz in enumerate(BACK):
                zz = lax.rem(z + 4 - dz, 4)
                col = (lax.rem(l + i, 2) * 4 + yy) * 128
                start(
                    w.at[n, i],
                    w_s.at[
                        pl.ds(pl.multiple_of(zz * 512, 512), 512),
                        pl.ds(pl.multiple_of(col, 128), 128),
                    ],
                )
    for copy in waits:
        copy.wait()
    loss = jnp.zeros((8, 128), jnp.float32)
    for t in range(4):
        cols = slice(t * 256, t * 256 + 256)
        branch = jnp.dot(
            a_s[...], w_s[:, cols], preferred_element_type=jnp.float32
        ).astype(jnp.bfloat16)
        out_ref[:, cols] = branch
        r = hidden[:, cols].astype(jnp.float32) + branch.astype(jnp.float32)
        r = r - target[:, cols].astype(jnp.float32)
        r = (r * r).reshape(64, 8, 256)
        r = jnp.sum(r, axis=0)
        loss = loss + (r[:, :128] + r[:, 128:])
    loss_ref[...] = loss


def kernel(body, out_shape, scratch, ins, mib):
    return pl.pallas_call(
        body,
        out_shape=out_shape,
        in_specs=ins,
        out_specs=jax.tree.map(lambda s: pl.BlockSpec(memory_space=pltpu.VMEM), out_shape),
        scratch_shapes=scratch,
        compiler_params=pltpu.CompilerParams(vmem_limit_bytes=mib * 2**20),
    )


SMEM = pl.BlockSpec(memory_space=pltpu.SMEM)
VMEM = pl.BlockSpec(memory_space=pltpu.VMEM)
ANY = pl.BlockSpec(memory_space=pl.ANY)


def shape(*dims, kind=jnp.bfloat16):
    return jax.ShapeDtypeStruct(dims, kind)


def body(hidden, target, gain, w_query, w_key, value_matrix, w_out, block_order):
    z, l, h, c, y = (lax.axis_index(a) for a in (Z, L, H, C, Y))
    x = 2 * h + l
    local = hidden[0]
    w0 = jnp.concatenate([w_query[:, :256], w_key], axis=1)
    w1 = jnp.concatenate([w_query[:, 256:], value_matrix], axis=1)
    wa = send(jnp.where(l == 0, w0, w1), (L, C), lambda l, c: (c, l))
    wb = send(jnp.where(l == 0, w1, w0), (L, C), lambda l, c: (c, 1 - l))
    sa = along_x(local, 1)
    sb = along_x(local, -1)
    d0 = swap(local)
    w = jnp.stack([wa, wb])
    w = jnp.broadcast_to(w[None], (16,) + w.shape)
    w = lax.all_to_all(w, (Z, Y), 0, 0, tiled=True)
    fa = along_x(sa[:256], 1)
    fb = along_x(sb[256:], -1)
    da, db = swap(sa), swap(sb)
    dfa, dfb = swap(fa), swap(fb)

    def turn(flip):
        return send(
            w_out, (Z, L, H, C), lambda z, l, h, c: (2 * h + c, (l + flip) % 2, z // 2, z % 2)
        )

    outs = around(jnp.stack(around(jnp.stack([turn(0), turn(1)]), Z)), Y)
    slots = lax.iota(jnp.int32, 16)

    def places(index):
        return jnp.sum(jnp.where(index[:, None] == slots[None, :], block_order[None, :], 0), axis=1)

    two = lax.iota(jnp.int32, 2)
    sides = jnp.stack([l, 1 - l])
    zs = (z + 4 - jnp.array(BACK, jnp.int32)) % 4
    index = (zs[:, None, None] * 2 + sides[None, :, None]) * 2 + two[None, None, :]
    kpos = places(index.reshape(16))
    qpos = kpos[:4]
    inverse = jnp.sum(jnp.where(kpos[None, :] == slots[:, None], slots[None, :], 0), axis=1)
    rows = (qpos[:, None] * CH + lax.iota(jnp.int32, CH)[None, :]).reshape(1024)
    half = HEAD_SIZE // 2
    freqs = ROPE_BASE ** (-(jnp.arange(half, dtype=jnp.float32) * 2.0) / HEAD_SIZE)
    angles = rows.astype(jnp.float32)[:, None] * freqs[None, :]
    cosine, sine = jnp.cos(angles), jnp.sin(angles)
    ha, hb = ((x + 3) % 4) // 2, ((x + 1) % 4) // 2

    def normed(info, layout, *sources):
        return kernel(
            functools.partial(norm, layout),
            shape(512, MODEL_WIDTH),
            [pltpu.VMEM((512, 128), jnp.float32), pltpu.SemaphoreType.DMA((6,))],
            [SMEM, VMEM] + [ANY] * len(sources),
            12,
        )(info, gain.reshape(1, MODEL_WIDTH), *sources)

    far_info = jnp.stack([2 * ha + c, 2 * ha + 1 - c, 2 * hb + c, 2 * hb + 1 - c, c])
    near_info = jnp.stack([2 * h + c, 2 * h + 1 - c, 2 - 2 * h + c, 3 - 2 * h - c, c])
    far_info, near_info = far_info.astype(jnp.int32), near_info.astype(jnp.int32)
    whole = tuple((k, 0, 512) for k in range(4))
    halves = ((0, 0, 512), (1, 0, 512), (2, 0, 256), (2, 256, 256), (3, 0, 256), (3, 256, 256))
    far_rows = normed(far_info, whole, sa, da, sb, db)
    near_rows = normed(near_info, halves, local, d0, fa, fb, dfa, dfb)

    def projected(first, width, out):
        return kernel(
            functools.partial(project, first, width),
            out,
            [pltpu.VMEM((4096, width), jnp.bfloat16), pltpu.SemaphoreType.DMA((32,))],
            [SMEM, VMEM, VMEM, VMEM, VMEM, ANY],
            22,
        )(near_info, cosine, sine, near_rows, far_rows, w)

    kv = projected(256, 128, shape(1024, HEAD_SIZE))
    mine = around(kv, Z)
    pieces = mine + [swap(v) for v in mine]
    q = projected(0, 256, shape(4, 2 * CH, HEAD_SIZE))

    def attended(first):
        return kernel(
            functools.partial(attention, first),
            shape(512, 256),
            [
                pltpu.VMEM((2, 4096, HEAD_SIZE), jnp.bfloat16),
                pltpu.VMEM((2, 16, 2 * CH, CH), jnp.float32),
                pltpu.VMEM((2, 2 * CH, 128), jnp.float32),
                pltpu.VMEM((2, 2 * CH, 128), jnp.float32),
                pltpu.VMEM((2, 2 * CH, 128), jnp.float32),
                pltpu.SemaphoreType.DMA((8,)),
            ],
            [SMEM, SMEM, VMEM] + [ANY] * 8,
            28,
        )(qinfo, inverse.astype(jnp.int32), q, *pieces)

    qinfo = jnp.concatenate([qpos, c[None]]).astype(jnp.int32)
    far = attended(2)
    near = attended(0)
    got = [near, along_x(far, 1), along_x(far, -1), along_x(near, 2)]
    got = got + [swap(v) for v in got]
    info = jnp.stack([c, z, y, l, x]).astype(jnp.int32)
    branch, squares = kernel(
        out_project,
        (shape(512, 1024), shape(8, 128, kind=jnp.float32)),
        [
            pltpu.VMEM((512, 2048), jnp.bfloat16),
            pltpu.VMEM((2048, 1024), jnp.bfloat16),
            pltpu.SemaphoreType.DMA((40,)),
        ],
        [SMEM, VMEM, VMEM] + [ANY] * 12,
        24,
    )(info, local, target[0], *got, *outs)
    squares = jnp.broadcast_to(squares[None], (128, 8, 128)).reshape(1024, 128)
    squares = lax.all_to_all(squares, (Z, L, H, C, Y), 0, 0, tiled=True)
    loss = jnp.sum(squares) / (4 * 4096 * MODEL_WIDTH)
    return (branch[None], loss)


def solution(mesh):
    split = Mesh(mesh.devices.reshape(4, 2, 2, 2, 4), (Z, L, H, C, Y))
    rows = P(Y, (Z, L), (H, C))
    weight = P((Z, L, Y), (H, C))
    return jax.shard_map(
        body,
        mesh=split,
        in_specs=(rows, rows, P(), weight, weight, weight, P((H, C), (Z, L, Y)), P()),
        out_specs=(rows, P()),
        check_vma=False,
    )
```

```python
import functools

import jax
import jax.numpy as jnp
import numpy as np
from jax import lax
from jax.experimental import pallas as pl
from jax.experimental.pallas import tpu as pltpu
from jax.sharding import Mesh
from jax.sharding import PartitionSpec as P

MODEL_WIDTH = 4096
HEAD_SIZE = 128
CH = 256
ROPE_BASE = 500000.0
Z, L, H, C, Y = "ctx_0", "ctx_1", "tp_0", "tp_1", "dp"
SIZE = {Z: 4, L: 2, H: 2, C: 2, Y: 4}
BACK = (0, 1, 3, 2)
LOG2E = 1.4426950408889634


def send(value, axes, where):
    order = [a for a in (Z, L, H, C, Y) if a in axes]
    sizes = [SIZE[a] for a in order]
    pairs = []
    for i in range(int(np.prod(sizes))):
        at = dict(zip(order, (int(k) for k in np.unravel_index(i, sizes))))
        to = where(*[at[a] for a in axes])
        if to is not None:
            goal = dict(zip(axes, to))
            pairs.append((i, int(np.ravel_multi_index([goal[a] for a in order], sizes))))
    return lax.ppermute(value, tuple(order), pairs)


def swap(value):
    return send(value, (C,), lambda c: (1 - c,))


def around(value, axis):
    out = [value]
    for by in BACK[1:]:
        out.append(send(value, (axis,), lambda i, by=by: ((i + by) % 4,)))
    return out


def along_x(value, step):
    def where(h, l):
        x = (2 * h + l + step) % 4
        return (x // 2, x % 2)

    return send(value, (H, L), where)


def fetch(layout, info, sources, x_s, sem):
    moves = []
    for src, (slot, rows, size) in zip(sources, layout):
        col = pl.multiple_of(info[slot] * 1024, 1024)
        copy = pltpu.make_async_copy(
            src, x_s.at[pl.ds(rows, size), pl.ds(col, 1024)], sem.at[len(moves)]
        )
        copy.start()
        moves.append((copy, rows, size, col))
    return moves


def normalise(moves, gain, x_s, r_s, out_ref, out_sem):
    tile = 64
    r_s[...] = jnp.zeros((512, 128), jnp.float32)
    for copy, first, size, col in moves:
        copy.wait()

        def squares(t, carry, first=first, col=col):
            rows = pl.ds(pl.multiple_of(first + t * tile, tile), tile)
            part = r_s[rows, :]
            for k in range(8):
                x = x_s[rows, pl.ds(col + k * 128, 128)].astype(jnp.float32)
                part = part + x * x
            r_s[rows, :] = part
            return carry

        lax.fori_loop(0, size // tile, squares, 0)
    mean = jnp.sum(r_s[...], axis=1, keepdims=True) * (1.0 / MODEL_WIDTH)
    r_s[...] = jnp.broadcast_to(lax.rsqrt(mean + 1e-05), (512, 128))

    def scale(t, carry):
        rows = pl.ds(pl.multiple_of(t * 32, 32), 32)
        r = r_s[rows, :]
        for k in range(32):
            cols = slice(k * 128, k * 128 + 128)
            x = x_s[rows, cols].astype(jnp.float32)
            x_s[rows, cols] = (x * r * gain[:, cols]).astype(jnp.bfloat16)
        return carry

    copies = []
    for b in range(2):
        lax.fori_loop(b * 8, b * 8 + 8, scale, 0)
        rows = pl.ds(b * 256, 256)
        copies.append(pltpu.make_async_copy(x_s.at[rows, :], out_ref.at[rows, :], out_sem.at[b]))
        copies[-1].start()
    return copies


def norm(layout, info, gain, *rest):
    count = len(layout)
    out_ref, x_s, r_s, sem, out_sem = rest[count:]
    moves = fetch(layout, info, rest[:count], x_s, sem)
    for copy in normalise(moves, gain, x_s, r_s, out_ref, out_sem):
        copy.wait()


def weights_in(first, width, c, w, w_s, sem):
    waits = []
    for z in range(4):
        for y in range(4):
            for i in range(2):
                part = c if i == 0 else 1 - c
                row = z * 1024 + part * 512 + y * 128
                copy = pltpu.make_async_copy(
                    w.at[z * 4 + y, i, :, pl.ds(first, width)],
                    w_s.at[pl.ds(pl.multiple_of(row, 128), 128), :],
                    sem.at[len(waits)],
                )
                copy.start()
                waits.append(copy)
    return waits


def rope(v, cs, sn):
    cb = jnp.concatenate([cs, cs], axis=1)
    sb = jnp.concatenate([-sn, sn], axis=1)
    return v * cb + pltpu.roll(v, 64, 1) * sb


def norm_keys(layout, info, gain, cosine, sine, far, w, *rest):
    count = len(layout)
    kv_ref, out_ref, x_s, far_s, w_s, t_s, r_s, sem, out_sem, w_sem, f_sem = rest[count:]
    c = info[4]
    moves = fetch(layout, info, rest[:count], x_s, sem)
    waits = weights_in(256, 128, c, w, w_s, w_sem)
    for k, (src, dst) in enumerate(((far, far_s), (cosine, t_s.at[0]), (sine, t_s.at[1]))):
        waits.append(pltpu.make_async_copy(src, dst, f_sem.at[k]))
        waits[-1].start()
    copies = normalise(moves, gain, x_s, r_s, out_ref, out_sem)
    for copy in waits:
        copy.wait()
    for side, n in enumerate((x_s, far_s)):
        rows = pl.ds(side * 512, 512)
        v = jnp.dot(n[...], w_s[...], preferred_element_type=jnp.float32)
        turned = rope(v, t_s[0, rows, :], t_s[1, rows, :])
        kv_ref[rows, :] = jnp.where(c == 0, turned, v).astype(jnp.bfloat16)
    for copy in copies:
        copy.wait()


def queries(info, cosine, sine, near, far, w, q_ref, n_s, w_s, t_s, sem, w_sem):
    waits = weights_in(0, 256, info[4], w, w_s, w_sem)
    for k, (src, dst) in enumerate(
        ((cosine, t_s.at[0]), (sine, t_s.at[1]), (near, n_s.at[0]), (far, n_s.at[1]))
    ):
        waits.append(pltpu.make_async_copy(src, dst, sem.at[k]))
        waits[-1].start()
    for copy in waits[:-1]:
        copy.wait()
    for side in range(2):
        if side == 1:
            waits[-1].wait()
        out = jnp.dot(n_s[side], w_s[...], preferred_element_type=jnp.float32)
        rows = pl.ds(side * 512, 512)
        for i in range(2):
            v = out[:, i * 128 : i * 128 + 128]
            v = rope(v, t_s[0, rows, :], t_s[1, rows, :]).astype(jnp.bfloat16)
            for b in range(2):
                q_ref[side * 2 + b, i * CH : i * CH + CH, :] = v[b * CH : b * CH + CH]


def attention(first, qpos, where, q_ref, *rest):
    pieces = rest[:8]
    out_ref, kv_s, s_s, m_s, l_s, o_s, sem = rest[8:]
    c = qpos[4]
    copies = []
    for k, piece in enumerate(pieces):
        kind = c if k < 4 else 1 - c
        copies.append(
            pltpu.make_async_copy(
                piece, kv_s.at[kind, pl.ds((k % 4) * 1024, 1024), :], sem.at[k]
            )
        )
        copies[-1].start()
    size = 2 * CH
    factor = LOG2E / HEAD_SIZE**0.5
    m_s[...] = jnp.full((2, size, 128), -1e30, jnp.float32)
    l_s[...] = jnp.zeros((2, size, 128), jnp.float32)
    o_s[...] = jnp.zeros((2, size, 128), jnp.float32)
    for copy in copies:
        copy.wait()
    here = [qpos[first], qpos[first + 1]]
    pairs = [here[0] // 2, here[1] // 2]

    def keys(kind, p):
        return kv_s[kind, pl.ds(pl.multiple_of(where[p] * CH, CH), CH), :]

    def dots(b, t):
        return [
            lax.dot_general(
                q_ref[first + b],
                keys(0, 2 * t + i),
                (((1,), (1,)), ((), ())),
                preferred_element_type=jnp.float32,
            )
            for i in range(2)
        ]

    def keep(b, t, s0, s1):
        s_s[b, 2 * t] = s0
        s_s[b, 2 * t + 1] = s1
        top = jnp.maximum(
            jnp.maximum(s0[:, :128], s0[:, 128:]), jnp.maximum(s1[:, :128], s1[:, 128:])
        )
        m_s[b] = jnp.maximum(m_s[b], top)

    def scores(b, t):
        keep(b, t, *dots(b, t))

    def last_scores(b):
        t = pairs[b]
        s0, s1 = dots(b, t)
        row = lax.rem(lax.broadcasted_iota(jnp.int32, (size, CH), 0), CH)
        gap = row - lax.broadcasted_iota(jnp.int32, (size, CH), 1) + (here[b] - 2 * t) * CH
        keep(b, t, jnp.where(gap >= 0, s0, -1e30), jnp.where(gap >= CH, s1, -1e30))
        m_s[b] = jnp.broadcast_to(jnp.max(m_s[b], axis=1, keepdims=True), (size, 128))

    def weigh(b, t):
        m = m_s[b]
        total = l_s[b]
        acc = o_s[b]
        for i in range(2):
            s = s_s[b, 2 * t + i]
            p0 = jnp.exp2((s[:, :128] - m) * factor)
            p1 = jnp.exp2((s[:, 128:] - m) * factor)
            total = total + (p0 + p1)
            p = jnp.concatenate([p0, p1], axis=1).astype(jnp.bfloat16)
            acc = acc + jnp.dot(p, keys(1, 2 * t + i), preferred_element_type=jnp.float32)
        l_s[b] = total
        o_s[b] = acc

    def store(b):
        total = jnp.sum(l_s[b], axis=1, keepdims=True)
        o = (o_s[b] / total).astype(jnp.bfloat16)
        for i in range(2):
            out_ref[b * CH : b * CH + CH, i * 128 : i * 128 + 128] = o[i * CH : i * CH + CH]

    def loop(low, high, *work):
        def step(t, carry):
            for f, b in work:
                f(b, t)
            return carry

        lax.fori_loop(low, high, step, 0)

    loop(0, pairs[0], (scores, 0))
    last_scores(0)
    both = jnp.minimum(pairs[0] + 1, pairs[1])
    loop(0, both, (scores, 1), (weigh, 0))
    loop(both, pairs[1], (scores, 1))
    loop(both, pairs[0] + 1, (weigh, 0))
    store(0)
    last_scores(1)
    loop(0, pairs[1] + 1, (weigh, 1))
    store(1)


def out_project(info, hidden, target, *rest):
    pieces = rest[:8]
    weights = rest[8:16]
    out_ref, loss_ref, a_s, w_s, sem = rest[16:]
    c, z, y, l, x = info[0], info[1], info[2], info[3], info[4]
    waits = []

    def start(src, dst):
        copy = pltpu.make_async_copy(src, dst, sem.at[len(waits)])
        copy.start()
        waits.append(copy)

    for k, piece in enumerate(pieces):
        group = lax.rem(x + (0, 3, 1, 2)[k % 4], 4)
        core = c if k < 4 else 1 - c
        col = pl.multiple_of(group * 512 + core * 256, 256)
        start(piece, a_s.at[:, pl.ds(col, 256)])
    for i in range(2):
        for k, w in enumerate(weights):
            yy = lax.rem(y + 4 - BACK[k % 4], 4)
            for n in range(2):
                zz = lax.rem(z + 4 - BACK[k // 4 * 2 + n], 4)
                col = (lax.rem(l + i, 2) * 4 + yy) * 128
                start(
                    w.at[n, i],
                    w_s.at[
                        pl.ds(pl.multiple_of(zz * 512, 512), 512),
                        pl.ds(pl.multiple_of(col, 128), 128),
                    ],
                )
    for copy in waits:
        copy.wait()
    loss = jnp.zeros((8, 128), jnp.float32)
    for t in range(4):
        cols = slice(t * 256, t * 256 + 256)
        branch = jnp.dot(
            a_s[...], w_s[:, cols], preferred_element_type=jnp.float32
        ).astype(jnp.bfloat16)
        out_ref[:, cols] = branch
        r = hidden[:, cols].astype(jnp.float32) + branch.astype(jnp.float32)
        r = r - target[:, cols].astype(jnp.float32)
        r = (r * r).reshape(64, 8, 256)
        r = jnp.sum(r, axis=0)
        loss = loss + (r[:, :128] + r[:, 128:])
    loss_ref[...] = loss


def kernel(body, out_shape, scratch, ins, mib, outs=None):
    if outs is None:
        outs = jax.tree.map(lambda s: VMEM, out_shape)
    out_shape = jax.tree.map(
        lambda s, o: pltpu.HBM(s.shape, s.dtype) if o is FIX else s, out_shape, outs
    )
    call = pl.pallas_call(
        body,
        out_shape=out_shape,
        in_specs=ins,
        out_specs=outs,
        scratch_shapes=scratch,
        compiler_params=pltpu.CompilerParams(vmem_limit_bytes=mib * 2**20),
    )

    def run(*args):
        return call(
            *[
                pltpu.with_memory_space_constraint(v, pltpu.HBM) if i is FIX else v
                for v, i in zip(args, ins)
            ]
        )

    return run


SMEM = pl.BlockSpec(memory_space=pltpu.SMEM)
VMEM = pl.BlockSpec(memory_space=pltpu.VMEM)
ANY = pl.BlockSpec(memory_space=pl.ANY)
FIX = pl.BlockSpec(memory_space=pl.ANY)


def shape(*dims, kind=jnp.bfloat16):
    return jax.ShapeDtypeStruct(dims, kind)


def body(hidden, target, gain, w_query, w_key, value_matrix, w_out, block_order):
    z, l, h, c, y = (lax.axis_index(a) for a in (Z, L, H, C, Y))
    x = 2 * h + l
    local = hidden[0]
    w0 = jnp.concatenate([w_query[:, :256], w_key], axis=1)
    w1 = jnp.concatenate([w_query[:, 256:], value_matrix], axis=1)
    wa = send(jnp.where(l == 0, w0, w1), (L, C), lambda l, c: (c, l))
    wb = send(jnp.where(l == 0, w1, w0), (L, C), lambda l, c: (c, 1 - l))
    low, high = local[:256], local[256:]
    sal, sah = along_x(low, 1), along_x(high, 1)
    sbl, sbh = along_x(low, -1), along_x(high, -1)
    d0 = swap(local)
    w = jnp.stack([wa, wb])
    w = jnp.broadcast_to(w[None], (16,) + w.shape)
    w = lax.all_to_all(w, (Z, Y), 0, 0, tiled=True)
    fa, fb = along_x(sal, 1), along_x(sbh, -1)
    dal, dah, dbl, dbh = (
        swap(v) for v in (sal, sah, sbl, sbh)
    )
    dfa, dfb = swap(fa), swap(fb)

    def turn(flip):
        return send(
            w_out, (Z, L, H, C), lambda z, l, h, c: (2 * h + c, (l + flip) % 2, z // 2, z % 2)
        )

    o = around(jnp.stack([turn(0), turn(1)]), Z)
    oa, ob = jnp.stack(o[:2]), jnp.stack(o[2:])

    def along_y(value, by):
        return send(value, (Y,), lambda i: ((i + by) % 4,))

    oa1, ob1 = along_y(oa, 1), along_y(ob, 1)
    oa3, ob3 = along_y(oa, 3), along_y(ob, 3)
    oa2, ob2 = along_y(oa1, 1), along_y(ob3, 3)
    outs = [oa, oa1, oa3, oa2, ob, ob1, ob3, ob2]
    slots = lax.iota(jnp.int32, 16)

    def places(index):
        return jnp.sum(jnp.where(index[:, None] == slots[None, :], block_order[None, :], 0), axis=1)

    two = lax.iota(jnp.int32, 2)
    sides = jnp.stack([l, 1 - l])
    zs = (z + 4 - jnp.array(BACK, jnp.int32)) % 4
    index = (zs[:, None, None] * 2 + sides[None, :, None]) * 2 + two[None, None, :]
    kpos = places(index.reshape(16))
    qpos = kpos[:4]
    inverse = jnp.sum(jnp.where(kpos[None, :] == slots[:, None], slots[None, :], 0), axis=1)
    rows = (qpos[:, None] * CH + lax.iota(jnp.int32, CH)[None, :]).reshape(1024)
    half = HEAD_SIZE // 2
    freqs = ROPE_BASE ** (-(jnp.arange(half, dtype=jnp.float32) * 2.0) / HEAD_SIZE)
    angles = rows.astype(jnp.float32)[:, None] * freqs[None, :]
    cosine, sine = jnp.cos(angles), jnp.sin(angles)
    ha, hb = ((x + 3) % 4) // 2, ((x + 1) % 4) // 2

    far_info = jnp.stack([2 * ha + c, 2 * ha + 1 - c, 2 * hb + c, 2 * hb + 1 - c, c])
    near_info = jnp.stack([2 * h + c, 2 * h + 1 - c, 2 - 2 * h + c, 3 - 2 * h - c, c])
    far_info, near_info = far_info.astype(jnp.int32), near_info.astype(jnp.int32)
    gain = gain.reshape(1, MODEL_WIDTH)
    dma = pltpu.SemaphoreType.DMA
    rows_s = [pltpu.VMEM((512, MODEL_WIDTH), jnp.bfloat16)]
    table_s = [pltpu.VMEM((2, 1024, 64), jnp.float32), pltpu.VMEM((512, 128), jnp.float32)]
    layout = tuple((k // 2, k % 2 * 256, 256) for k in range(8))
    far_rows = kernel(
        functools.partial(norm, layout),
        shape(512, MODEL_WIDTH),
        rows_s + table_s[1:] + [dma((8,)), dma((2,))],
        [SMEM, VMEM] + [ANY] * 8,
        12,
        FIX,
    )(far_info, gain, sal, sah, dal, dah, sbl, sbh, dbl, dbh)
    layout = ((0, 0, 512), (1, 0, 512), (2, 0, 256), (2, 256, 256), (3, 0, 256), (3, 256, 256))
    kv, near_rows = kernel(
        functools.partial(norm_keys, layout),
        (shape(1024, HEAD_SIZE), shape(512, MODEL_WIDTH)),
        rows_s * 2
        + [pltpu.VMEM((4096, 128), jnp.bfloat16)]
        + table_s
        + [dma((6,)), dma((2,)), dma((32,)), dma((3,))],
        [SMEM, VMEM] + [FIX] * 3 + [ANY, FIX] + [ANY] * 5,
        20,
        (VMEM, FIX),
    )(near_info, gain, cosine, sine, far_rows, w, local, d0, fa, fb, dfa, dfb)
    mine = around(kv, Z)
    pieces = mine + [swap(v) for v in mine]
    q = kernel(
        queries,
        shape(4, 2 * CH, HEAD_SIZE),
        [
            pltpu.VMEM((2, 512, MODEL_WIDTH), jnp.bfloat16),
            pltpu.VMEM((4096, 256), jnp.bfloat16),
            table_s[0],
            dma((4,)),
            dma((32,)),
        ],
        [SMEM] + [FIX] * 4 + [ANY],
        20,
    )(near_info, cosine, sine, near_rows, far_rows, w)

    def attended(first):
        return kernel(
            functools.partial(attention, first),
            shape(512, 256),
            [
                pltpu.VMEM((2, 4096, HEAD_SIZE), jnp.bfloat16),
                pltpu.VMEM((2, 16, 2 * CH, CH), jnp.float32),
                pltpu.VMEM((2, 2 * CH, 128), jnp.float32),
                pltpu.VMEM((2, 2 * CH, 128), jnp.float32),
                pltpu.VMEM((2, 2 * CH, 128), jnp.float32),
                pltpu.SemaphoreType.DMA((8,)),
            ],
            [SMEM, SMEM, VMEM] + [ANY] * 8,
            28,
        )(qinfo, inverse.astype(jnp.int32), q, *pieces)

    qinfo = jnp.concatenate([qpos, c[None]]).astype(jnp.int32)
    far = attended(2)
    near = attended(0)
    got = [near, along_x(far, 1), along_x(far, -1), along_x(near, 2)]
    got = got + [swap(v) for v in got]
    info = jnp.stack([c, z, y, l, x]).astype(jnp.int32)
    branch, squares = kernel(
        out_project,
        (shape(512, 1024), shape(8, 128, kind=jnp.float32)),
        [
            pltpu.VMEM((512, 2048), jnp.bfloat16),
            pltpu.VMEM((2048, 1024), jnp.bfloat16),
            pltpu.SemaphoreType.DMA((40,)),
        ],
        [SMEM, VMEM, VMEM] + [ANY] * 16,
        24,
    )(info, local, target[0], *got, *outs)
    squares = squares + swap(squares)
    squares = jnp.broadcast_to(squares[None], (64, 8, 128)).reshape(512, 128)
    squares = lax.all_to_all(squares, (Z, L, H, Y), 0, 0, tiled=True)
    loss = jnp.sum(squares) / (4 * 4096 * MODEL_WIDTH)
    return (branch[None], loss)


def solution(mesh):
    split = Mesh(mesh.devices.reshape(4, 2, 2, 2, 4), (Z, L, H, C, Y))
    rows = P(Y, (Z, L), (H, C))
    weight = P((Z, L, Y), (H, C))
    return jax.shard_map(
        body,
        mesh=split,
        in_specs=(rows, rows, P(), weight, weight, weight, P((H, C), (Z, L, Y)), P()),
        out_specs=(rows, P()),
        check_vma=False,
    )
```

```python
import functools

import jax
import jax.numpy as jnp
import numpy as np
from jax import lax
from jax.experimental import pallas as pl
from jax.experimental.pallas import tpu as pltpu
from jax.sharding import Mesh
from jax.sharding import PartitionSpec as P

MODEL_WIDTH = 4096
HEAD_SIZE = 128
CH = 256
ROPE_BASE = 500000.0
Z, L, H, C, Y = "ctx_0", "ctx_1", "tp_0", "tp_1", "dp"
SIZE = {Z: 4, L: 2, H: 2, C: 2, Y: 4}
BACK = (0, 1, 3, 2)
LOG2E = 1.4426950408889634


def send(value, axes, where):
    order = [a for a in (Z, L, H, C, Y) if a in axes]
    sizes = [SIZE[a] for a in order]
    pairs = []
    for i in range(int(np.prod(sizes))):
        at = dict(zip(order, (int(k) for k in np.unravel_index(i, sizes))))
        to = where(*[at[a] for a in axes])
        if to is not None:
            goal = dict(zip(axes, to))
            pairs.append((i, int(np.ravel_multi_index([goal[a] for a in order], sizes))))
    return lax.ppermute(value, tuple(order), pairs)


def swap(value):
    return send(value, (C,), lambda c: (1 - c,))


def around(value, axis):
    out = [value]
    for by in BACK[1:]:
        out.append(send(value, (axis,), lambda i, by=by: ((i + by) % 4,)))
    return out


def along_x(value, step):
    def where(h, l):
        x = (2 * h + l + step) % 4
        return (x // 2, x % 2)

    return send(value, (H, L), where)


def fetch(layout, info, sources, x_s, sem):
    moves = []
    for src, (slot, rows, size) in zip(sources, layout):
        col = pl.multiple_of(info[slot] * 1024, 1024)
        copy = pltpu.make_async_copy(
            src, x_s.at[pl.ds(rows, size), pl.ds(col, 1024)], sem.at[len(moves)]
        )
        copy.start()
        moves.append((copy, rows, size, col))
    return moves


def normalise(moves, gain, x_s, r_s, out_ref, out_sem):
    tile = 64
    r_s[...] = jnp.zeros((512, 128), jnp.float32)
    for copy, first, size, col in moves:
        copy.wait()

        def squares(t, carry, first=first, col=col):
            rows = pl.ds(pl.multiple_of(first + t * tile, tile), tile)
            part = r_s[rows, :]
            for k in range(8):
                x = x_s[rows, pl.ds(col + k * 128, 128)].astype(jnp.float32)
                part = part + x * x
            r_s[rows, :] = part
            return carry

        lax.fori_loop(0, size // tile, squares, 0)
    mean = jnp.sum(r_s[...], axis=1, keepdims=True) * (1.0 / MODEL_WIDTH)
    r_s[...] = jnp.broadcast_to(lax.rsqrt(mean + 1e-05), (512, 128))

    def scale(t, carry):
        rows = pl.ds(pl.multiple_of(t * 32, 32), 32)
        r = r_s[rows, :]
        for k in range(32):
            cols = slice(k * 128, k * 128 + 128)
            x = x_s[rows, cols].astype(jnp.float32)
            x_s[rows, cols] = (x * r * gain[:, cols]).astype(jnp.bfloat16)
        return carry

    copies = []
    for b in range(2):
        lax.fori_loop(b * 8, b * 8 + 8, scale, 0)
        rows = pl.ds(b * 256, 256)
        copies.append(pltpu.make_async_copy(x_s.at[rows, :], out_ref.at[rows, :], out_sem.at[b]))
        copies[-1].start()
    return copies


def norm(layout, info, gain, *rest):
    count = len(layout)
    out_ref, x_s, r_s, sem, out_sem = rest[count:]
    moves = fetch(layout, info, rest[:count], x_s, sem)
    for copy in normalise(moves, gain, x_s, r_s, out_ref, out_sem):
        copy.wait()


def weights_in(first, width, info, pieces, w_s, sem):
    c, z, y = info[4], info[5], info[6]
    waits = []
    for k, w in enumerate(pieces):
        for n in range(4):
            dz, dy = (BACK[k], BACK[n]) if k < 4 else (BACK[n], BACK[k - 4])
            part = c if k < 4 else 1 - c
            row = lax.rem(z + 4 - dz, 4) * 1024 + part * 512 + lax.rem(y + 4 - dy, 4) * 128
            copy = pltpu.make_async_copy(
                w.at[n, :, pl.ds(first, width)],
                w_s.at[pl.ds(pl.multiple_of(row, 128), 128), :],
                sem.at[len(waits)],
            )
            copy.start()
            waits.append(copy)
    return waits


def rope(v, cs, sn):
    cb = jnp.concatenate([cs, cs], axis=1)
    sb = jnp.concatenate([-sn, sn], axis=1)
    return v * cb + pltpu.roll(v, 64, 1) * sb


def norm_keys(layout, info, gain, cosine, sine, far, *rest):
    count = len(layout)
    pieces, rest = rest[:8], rest[8:]
    kv_ref, out_ref, x_s, far_s, w_s, t_s, r_s, sem, out_sem, w_sem, f_sem = rest[count:]
    c = info[4]
    moves = fetch(layout, info, rest[:count], x_s, sem)
    waits = weights_in(256, 128, info, pieces, w_s, w_sem)
    for k, (src, dst) in enumerate(((far, far_s), (cosine, t_s.at[0]), (sine, t_s.at[1]))):
        waits.append(pltpu.make_async_copy(src, dst, f_sem.at[k]))
        waits[-1].start()
    copies = normalise(moves, gain, x_s, r_s, out_ref, out_sem)
    for copy in waits:
        copy.wait()
    for side, n in enumerate((x_s, far_s)):
        rows = pl.ds(side * 512, 512)
        v = jnp.dot(n[...], w_s[...], preferred_element_type=jnp.float32)
        turned = rope(v, t_s[0, rows, :], t_s[1, rows, :])
        kv_ref[rows, :] = jnp.where(c == 0, turned, v).astype(jnp.bfloat16)
    for copy in copies:
        copy.wait()


def queries(info, cosine, sine, near, far, *rest):
    pieces = rest[:8]
    q_ref, n_s, w_s, t_s, sem, w_sem = rest[8:]
    waits = weights_in(0, 256, info, pieces, w_s, w_sem)
    for k, (src, dst) in enumerate(
        ((cosine, t_s.at[0]), (sine, t_s.at[1]), (near, n_s.at[0]), (far, n_s.at[1]))
    ):
        waits.append(pltpu.make_async_copy(src, dst, sem.at[k]))
        waits[-1].start()
    for copy in waits[:-1]:
        copy.wait()
    for side in range(2):
        if side == 1:
            waits[-1].wait()
        out = jnp.dot(n_s[side], w_s[...], preferred_element_type=jnp.float32)
        rows = pl.ds(side * 512, 512)
        for i in range(2):
            v = out[:, i * 128 : i * 128 + 128]
            v = rope(v, t_s[0, rows, :], t_s[1, rows, :]).astype(jnp.bfloat16)
            for b in range(2):
                q_ref[side * 2 + b, i * CH : i * CH + CH, :] = v[b * CH : b * CH + CH]


def attention(first, qpos, where, q_ref, *rest):
    pieces = rest[:8]
    out_ref, kv_s, s_s, m_s, l_s, o_s, sem = rest[8:]
    c = qpos[4]
    copies = []
    for k, piece in enumerate(pieces):
        kind = c if k < 4 else 1 - c
        copies.append(
            pltpu.make_async_copy(
                piece, kv_s.at[kind, pl.ds((k % 4) * 1024, 1024), :], sem.at[k]
            )
        )
        copies[-1].start()
    size = 2 * CH
    factor = LOG2E / HEAD_SIZE**0.5
    m_s[...] = jnp.full((2, size, 128), -1e30, jnp.float32)
    l_s[...] = jnp.zeros((2, size, 128), jnp.float32)
    o_s[...] = jnp.zeros((2, size, 128), jnp.float32)
    for copy in copies:
        copy.wait()
    here = [qpos[first], qpos[first + 1]]
    pairs = [here[0] // 2, here[1] // 2]

    def keys(kind, p):
        return kv_s[kind, pl.ds(pl.multiple_of(where[p] * CH, CH), CH), :]

    def dots(b, t):
        return [
            lax.dot_general(
                q_ref[first + b],
                keys(0, 2 * t + i),
                (((1,), (1,)), ((), ())),
                preferred_element_type=jnp.float32,
            )
            for i in range(2)
        ]

    def keep(b, t, s0, s1):
        s_s[b, 2 * t] = s0
        s_s[b, 2 * t + 1] = s1
        top = jnp.maximum(
            jnp.maximum(s0[:, :128], s0[:, 128:]), jnp.maximum(s1[:, :128], s1[:, 128:])
        )
        m_s[b] = jnp.maximum(m_s[b], top)

    def scores(b, t):
        keep(b, t, *dots(b, t))

    def last_scores(b):
        t = pairs[b]
        s0, s1 = dots(b, t)
        row = lax.rem(lax.broadcasted_iota(jnp.int32, (size, CH), 0), CH)
        gap = row - lax.broadcasted_iota(jnp.int32, (size, CH), 1) + (here[b] - 2 * t) * CH
        keep(b, t, jnp.where(gap >= 0, s0, -1e30), jnp.where(gap >= CH, s1, -1e30))
        m_s[b] = jnp.broadcast_to(jnp.max(m_s[b], axis=1, keepdims=True), (size, 128))

    def weigh(b, t):
        m = m_s[b]
        total = l_s[b]
        acc = o_s[b]
        for i in range(2):
            s = s_s[b, 2 * t + i]
            p0 = jnp.exp2((s[:, :128] - m) * factor)
            p1 = jnp.exp2((s[:, 128:] - m) * factor)
            total = total + (p0 + p1)
            p = jnp.concatenate([p0, p1], axis=1).astype(jnp.bfloat16)
            acc = acc + jnp.dot(p, keys(1, 2 * t + i), preferred_element_type=jnp.float32)
        l_s[b] = total
        o_s[b] = acc

    def store(b):
        total = jnp.sum(l_s[b], axis=1, keepdims=True)
        o = (o_s[b] / total).astype(jnp.bfloat16)
        for i in range(2):
            out_ref[b * CH : b * CH + CH, i * 128 : i * 128 + 128] = o[i * CH : i * CH + CH]

    def loop(low, high, *work):
        def step(t, carry):
            for f, b in work:
                f(b, t)
            return carry

        lax.fori_loop(low, high, step, 0)

    loop(0, pairs[0], (scores, 0))
    last_scores(0)
    both = jnp.minimum(pairs[0] + 1, pairs[1])
    loop(0, both, (scores, 1), (weigh, 0))
    loop(both, pairs[1], (scores, 1))
    loop(both, pairs[0] + 1, (weigh, 0))
    store(0)
    last_scores(1)
    loop(0, pairs[1] + 1, (weigh, 1))
    store(1)


def out_project(info, hidden, target, *rest):
    pieces = rest[:8]
    weights = rest[8:16]
    out_ref, loss_ref, a_s, w_s, sem = rest[16:]
    c, z, y, l, x = info[0], info[1], info[2], info[3], info[4]
    waits = []

    def start(src, dst):
        copy = pltpu.make_async_copy(src, dst, sem.at[len(waits)])
        copy.start()
        waits.append(copy)

    for k, piece in enumerate(pieces):
        group = lax.rem(x + (0, 3, 1, 2)[k % 4], 4)
        core = c if k < 4 else 1 - c
        col = pl.multiple_of(group * 512 + core * 256, 256)
        start(piece, a_s.at[:, pl.ds(col, 256)])
    for i in range(2):
        for k, w in enumerate(weights):
            yy = lax.rem(y + 4 - BACK[k % 4], 4)
            for n in range(2):
                zz = lax.rem(z + 4 - BACK[k // 4 * 2 + n], 4)
                col = (lax.rem(l + i, 2) * 4 + yy) * 128
                start(
                    w.at[n, i],
                    w_s.at[
                        pl.ds(pl.multiple_of(zz * 512, 512), 512),
                        pl.ds(pl.multiple_of(col, 128), 128),
                    ],
                )
    for copy in waits:
        copy.wait()
    loss = jnp.zeros((8, 128), jnp.float32)
    for t in range(4):
        cols = slice(t * 256, t * 256 + 256)
        branch = jnp.dot(
            a_s[...], w_s[:, cols], preferred_element_type=jnp.float32
        ).astype(jnp.bfloat16)
        out_ref[:, cols] = branch
        r = hidden[:, cols].astype(jnp.float32) + branch.astype(jnp.float32)
        r = r - target[:, cols].astype(jnp.float32)
        r = (r * r).reshape(64, 8, 256)
        r = jnp.sum(r, axis=0)
        loss = loss + (r[:, :128] + r[:, 128:])
    loss_ref[...] = loss


def kernel(body, out_shape, scratch, ins, mib, outs=None):
    if outs is None:
        outs = jax.tree.map(lambda s: VMEM, out_shape)
    out_shape = jax.tree.map(
        lambda s, o: pltpu.HBM(s.shape, s.dtype) if o is FIX else s, out_shape, outs
    )
    call = pl.pallas_call(
        body,
        out_shape=out_shape,
        in_specs=ins,
        out_specs=outs,
        scratch_shapes=scratch,
        compiler_params=pltpu.CompilerParams(vmem_limit_bytes=mib * 2**20),
    )

    def run(*args):
        return call(
            *[
                pltpu.with_memory_space_constraint(v, pltpu.HBM) if i is FIX else v
                for v, i in zip(args, ins)
            ]
        )

    return run


SMEM = pl.BlockSpec(memory_space=pltpu.SMEM)
VMEM = pl.BlockSpec(memory_space=pltpu.VMEM)
ANY = pl.BlockSpec(memory_space=pl.ANY)
FIX = pl.BlockSpec(memory_space=pl.ANY)


def shape(*dims, kind=jnp.bfloat16):
    return jax.ShapeDtypeStruct(dims, kind)


def body(hidden, target, gain, w_query, w_key, value_matrix, w_out, block_order):
    z, l, h, c, y = (lax.axis_index(a) for a in (Z, L, H, C, Y))
    x = 2 * h + l
    local = hidden[0]
    w0 = jnp.concatenate([w_query[:, :256], w_key], axis=1)
    w1 = jnp.concatenate([w_query[:, 256:], value_matrix], axis=1)
    wa = send(jnp.where(l == 0, w0, w1), (L, C), lambda l, c: (c, l))
    wb = send(jnp.where(l == 0, w1, w0), (L, C), lambda l, c: (c, 1 - l))
    low, high = local[:256], local[256:]
    sal, sah = along_x(low, 1), along_x(high, 1)
    sbl, sbh = along_x(low, -1), along_x(high, -1)
    d0 = swap(local)
    w = around(jnp.stack(around(wa, Y)), Z)
    w = w + around(jnp.stack(around(wb, Z)), Y)
    fa, fb = along_x(sal, 1), along_x(sbh, -1)
    dal, dah, dbl, dbh = (
        swap(v) for v in (sal, sah, sbl, sbh)
    )
    dfa, dfb = swap(fa), swap(fb)

    def turn(flip):
        return send(
            w_out, (Z, L, H, C), lambda z, l, h, c: (2 * h + c, (l + flip) % 2, z // 2, z % 2)
        )

    o = jnp.stack([turn(0), turn(1)])
    o = around(o, Z)
    oa, ob = jnp.stack(o[:2]), jnp.stack(o[2:])

    def along_y(value, by):
        return send(value, (Y,), lambda i: ((i + by) % 4,))

    oa1, ob1 = along_y(oa, 1), along_y(ob, 1)
    oa3, ob3 = along_y(oa, 3), along_y(ob, 3)
    oa2, ob2 = along_y(oa1, 1), along_y(ob3, 3)
    outs = [oa, oa1, oa3, oa2, ob, ob1, ob3, ob2]
    slots = lax.iota(jnp.int32, 16)

    def places(index):
        return jnp.sum(jnp.where(index[:, None] == slots[None, :], block_order[None, :], 0), axis=1)

    two = lax.iota(jnp.int32, 2)
    sides = jnp.stack([l, 1 - l])
    zs = (z + 4 - jnp.array(BACK, jnp.int32)) % 4
    index = (zs[:, None, None] * 2 + sides[None, :, None]) * 2 + two[None, None, :]
    kpos = places(index.reshape(16))
    qpos = kpos[:4]
    inverse = jnp.sum(jnp.where(kpos[None, :] == slots[:, None], slots[None, :], 0), axis=1)
    rows = (qpos[:, None] * CH + lax.iota(jnp.int32, CH)[None, :]).reshape(1024)
    half = HEAD_SIZE // 2
    freqs = ROPE_BASE ** (-(jnp.arange(half, dtype=jnp.float32) * 2.0) / HEAD_SIZE)
    angles = rows.astype(jnp.float32)[:, None] * freqs[None, :]
    cosine, sine = jnp.cos(angles), jnp.sin(angles)
    ha, hb = ((x + 3) % 4) // 2, ((x + 1) % 4) // 2

    far_info = jnp.stack([2 * ha + c, 2 * ha + 1 - c, 2 * hb + c, 2 * hb + 1 - c, c])
    near_info = jnp.stack([2 * h + c, 2 * h + 1 - c, 2 - 2 * h + c, 3 - 2 * h - c, c, z, y])
    far_info, near_info = far_info.astype(jnp.int32), near_info.astype(jnp.int32)
    gain = gain.reshape(1, MODEL_WIDTH)
    dma = pltpu.SemaphoreType.DMA
    rows_s = [pltpu.VMEM((512, MODEL_WIDTH), jnp.bfloat16)]
    table_s = [pltpu.VMEM((2, 1024, 64), jnp.float32), pltpu.VMEM((512, 128), jnp.float32)]
    layout = tuple((k // 2, k % 2 * 256, 256) for k in range(8))
    far_rows = kernel(
        functools.partial(norm, layout),
        shape(512, MODEL_WIDTH),
        rows_s + table_s[1:] + [dma((8,)), dma((2,))],
        [SMEM, VMEM] + [ANY] * 8,
        12,
        FIX,
    )(far_info, gain, sal, sah, dal, dah, sbl, sbh, dbl, dbh)
    layout = ((0, 0, 512), (1, 0, 512), (2, 0, 256), (2, 256, 256), (3, 0, 256), (3, 256, 256))
    kv, near_rows = kernel(
        functools.partial(norm_keys, layout),
        (shape(1024, HEAD_SIZE), shape(512, MODEL_WIDTH)),
        rows_s * 2
        + [pltpu.VMEM((4096, 128), jnp.bfloat16)]
        + table_s
        + [dma((6,)), dma((2,)), dma((32,)), dma((3,))],
        [SMEM, VMEM] + [FIX] * 3 + [ANY] * 8 + [FIX] + [ANY] * 5,
        20,
        (VMEM, FIX),
    )(near_info, gain, cosine, sine, far_rows, *w, local, d0, fa, fb, dfa, dfb)
    mine = around(kv, Z)
    pieces = mine + [swap(v) for v in mine]
    q = kernel(
        queries,
        shape(4, 2 * CH, HEAD_SIZE),
        [
            pltpu.VMEM((2, 512, MODEL_WIDTH), jnp.bfloat16),
            pltpu.VMEM((4096, 256), jnp.bfloat16),
            table_s[0],
            dma((4,)),
            dma((32,)),
        ],
        [SMEM] + [FIX] * 4 + [ANY] * 8,
        20,
    )(near_info, cosine, sine, near_rows, far_rows, *w)

    def attended(first):
        return kernel(
            functools.partial(attention, first),
            shape(512, 256),
            [
                pltpu.VMEM((2, 4096, HEAD_SIZE), jnp.bfloat16),
                pltpu.VMEM((2, 16, 2 * CH, CH), jnp.float32),
                pltpu.VMEM((2, 2 * CH, 128), jnp.float32),
                pltpu.VMEM((2, 2 * CH, 128), jnp.float32),
                pltpu.VMEM((2, 2 * CH, 128), jnp.float32),
                pltpu.SemaphoreType.DMA((8,)),
            ],
            [SMEM, SMEM, VMEM] + [ANY] * 8,
            28,
        )(qinfo, inverse.astype(jnp.int32), q, *pieces)

    qinfo = jnp.concatenate([qpos, c[None]]).astype(jnp.int32)
    far = attended(2)
    near = attended(0)
    got = [near, along_x(far, 1), along_x(far, -1), along_x(near, 2)]
    got = got + [swap(v) for v in got]
    info = jnp.stack([c, z, y, l, x]).astype(jnp.int32)
    branch, squares = kernel(
        out_project,
        (shape(512, 1024), shape(8, 128, kind=jnp.float32)),
        [
            pltpu.VMEM((512, 2048), jnp.bfloat16),
            pltpu.VMEM((2048, 1024), jnp.bfloat16),
            pltpu.SemaphoreType.DMA((40,)),
        ],
        [SMEM, VMEM, VMEM] + [ANY] * 16,
        24,
    )(info, local, target[0], *got, *outs)
    squares = squares + swap(squares)
    squares = jnp.broadcast_to(squares[None], (64, 8, 128)).reshape(512, 128)
    squares = lax.all_to_all(squares, (Z, L, H, Y), 0, 0, tiled=True)
    loss = jnp.sum(squares) / (4 * 4096 * MODEL_WIDTH)
    return (branch[None], loss)


def solution(mesh):
    split = Mesh(mesh.devices.reshape(4, 2, 2, 2, 4), (Z, L, H, C, Y))
    rows = P(Y, (Z, L), (H, C))
    weight = P((Z, L, Y), (H, C))
    return jax.shard_map(
        body,
        mesh=split,
        in_specs=(rows, rows, P(), weight, weight, weight, P((H, C), (Z, L, Y)), P()),
        out_specs=(rows, P()),
        check_vma=False,
    )
```

```python
import functools

import jax
import jax.numpy as jnp
import numpy as np
from jax import lax
from jax.experimental import pallas as pl
from jax.experimental.pallas import tpu as pltpu
from jax.sharding import Mesh
from jax.sharding import PartitionSpec as P

MODEL_WIDTH = 4096
HEAD_SIZE = 128
CH = 256
ROPE_BASE = 500000.0
Z, L, H, C, Y = "ctx_0", "ctx_1", "tp_0", "tp_1", "dp"
SIZE = {Z: 4, L: 2, H: 2, C: 2, Y: 4}
BACK = (0, 1, 3, 2)
LOG2E = 1.4426950408889634


def send(value, axes, where):
    order = [a for a in (Z, L, H, C, Y) if a in axes]
    sizes = [SIZE[a] for a in order]
    pairs = []
    for i in range(int(np.prod(sizes))):
        at = dict(zip(order, (int(k) for k in np.unravel_index(i, sizes))))
        to = where(*[at[a] for a in axes])
        if to is not None:
            goal = dict(zip(axes, to))
            pairs.append((i, int(np.ravel_multi_index([goal[a] for a in order], sizes))))
    return lax.ppermute(value, tuple(order), pairs)


def swap(value):
    return send(value, (C,), lambda c: (1 - c,))


def around(value, axis):
    out = [value]
    for by in BACK[1:]:
        out.append(send(value, (axis,), lambda i, by=by: ((i + by) % 4,)))
    return out


def along_x(value, step):
    def where(h, l):
        x = (2 * h + l + step) % 4
        return (x // 2, x % 2)

    return send(value, (H, L), where)


def fetch(layout, info, sources, x_s, sem):
    moves = []
    for src, (slot, rows, size) in zip(sources, layout):
        col = pl.multiple_of(info[slot] * 1024, 1024)
        copy = pltpu.make_async_copy(
            src, x_s.at[pl.ds(rows, size), pl.ds(col, 1024)], sem.at[len(moves)]
        )
        copy.start()
        moves.append((copy, rows, size, col))
    return moves


def normalise(moves, gain, x_s, r_s, out_ref, out_sem):
    tile = 64
    r_s[...] = jnp.zeros((512, 128), jnp.float32)
    for copy, first, size, col in moves:
        copy.wait()

        def squares(t, carry, first=first, col=col):
            rows = pl.ds(pl.multiple_of(first + t * tile, tile), tile)
            part = r_s[rows, :]
            for k in range(8):
                x = x_s[rows, pl.ds(col + k * 128, 128)].astype(jnp.float32)
                part = part + x * x
            r_s[rows, :] = part
            return carry

        lax.fori_loop(0, size // tile, squares, 0)
    mean = jnp.sum(r_s[...], axis=1, keepdims=True) * (1.0 / MODEL_WIDTH)
    r_s[...] = jnp.broadcast_to(lax.rsqrt(mean + 1e-05), (512, 128))

    def scale(t, carry):
        rows = pl.ds(pl.multiple_of(t * 32, 32), 32)
        r = r_s[rows, :]
        for k in range(32):
            cols = slice(k * 128, k * 128 + 128)
            x = x_s[rows, cols].astype(jnp.float32)
            x_s[rows, cols] = (x * r * gain[:, cols]).astype(jnp.bfloat16)
        return carry

    copies = []
    for b in range(2):
        lax.fori_loop(b * 8, b * 8 + 8, scale, 0)
        rows = pl.ds(b * 256, 256)
        copies.append(pltpu.make_async_copy(x_s.at[rows, :], out_ref.at[rows, :], out_sem.at[b]))
        copies[-1].start()
    return copies


def norm(layout, info, gain, *rest):
    count = len(layout)
    out_ref, x_s, r_s, sem, out_sem = rest[count:]
    moves = fetch(layout, info, rest[:count], x_s, sem)
    for copy in normalise(moves, gain, x_s, r_s, out_ref, out_sem):
        copy.wait()


def weights_in(first, width, info, pieces, w_s, sem):
    c, z, y = info[4], info[5], info[6]
    waits = []
    for k, w in enumerate(pieces):
        for n in range(4):
            dz, dy = (BACK[k], BACK[n]) if k < 4 else (BACK[n], BACK[k - 4])
            part = c if k < 4 else 1 - c
            row = lax.rem(z + 4 - dz, 4) * 1024 + part * 512 + lax.rem(y + 4 - dy, 4) * 128
            copy = pltpu.make_async_copy(
                w.at[n, :, pl.ds(first, width)],
                w_s.at[pl.ds(pl.multiple_of(row, 128), 128), :],
                sem.at[len(waits)],
            )
            copy.start()
            waits.append(copy)
    return waits


def rope(v, cs, sn):
    cb = jnp.concatenate([cs, cs], axis=1)
    sb = jnp.concatenate([-sn, sn], axis=1)
    return v * cb + pltpu.roll(v, 64, 1) * sb


def norm_keys(layout, info, gain, cosine, sine, far, *rest):
    count = len(layout)
    pieces, rest = rest[:8], rest[8:]
    kv_ref, out_ref, x_s, far_s, w_s, t_s, r_s, sem, out_sem, w_sem, f_sem = rest[count:]
    c = info[4]
    moves = fetch(layout, info, rest[:count], x_s, sem)
    waits = weights_in(256, 128, info, pieces, w_s, w_sem)
    for k, (src, dst) in enumerate(((far, far_s), (cosine, t_s.at[0]), (sine, t_s.at[1]))):
        waits.append(pltpu.make_async_copy(src, dst, f_sem.at[k]))
        waits[-1].start()
    copies = normalise(moves, gain, x_s, r_s, out_ref, out_sem)
    for copy in waits:
        copy.wait()
    for side, n in enumerate((x_s, far_s)):
        rows = pl.ds(side * 512, 512)
        v = jnp.dot(n[...], w_s[...], preferred_element_type=jnp.float32)
        turned = rope(v, t_s[0, rows, :], t_s[1, rows, :])
        kv_ref[rows, :] = jnp.where(c == 0, turned, v).astype(jnp.bfloat16)
    for copy in copies:
        copy.wait()


def queries(info, cosine, sine, near, far, *rest):
    pieces = rest[:8]
    q_ref, n_s, w_s, t_s, sem, w_sem = rest[8:]
    waits = weights_in(0, 256, info, pieces, w_s, w_sem)
    for k, src in enumerate((cosine, sine)):
        waits.append(pltpu.make_async_copy(src, t_s.at[k], sem.at[k]))
        waits[-1].start()
    moves = []
    for b in range(4):
        src = near if b < 2 else far
        copy = pltpu.make_async_copy(
            src.at[pl.ds(b % 2 * CH, CH), :], n_s.at[pl.ds(b * CH, CH), :], sem.at[2 + b]
        )
        copy.start()
        moves.append(copy)
    for copy in waits:
        copy.wait()
    for b in range(4):
        moves[b].wait()
        rows = pl.ds(b * CH, CH)
        out = jnp.dot(n_s[rows, :], w_s[...], preferred_element_type=jnp.float32)
        for i in range(2):
            v = out[:, i * 128 : i * 128 + 128]
            v = rope(v, t_s[0, rows, :], t_s[1, rows, :]).astype(jnp.bfloat16)
            q_ref[b, i * CH : i * CH + CH, :] = v


def attention(first, qpos, where, q_ref, *rest):
    pieces = rest[:8]
    out_ref, kv_s, s_s, m_s, l_s, o_s, sem = rest[8:]
    c = qpos[4]
    copies = []
    for k, piece in enumerate(pieces):
        kind = c if k < 4 else 1 - c
        copies.append(
            pltpu.make_async_copy(
                piece, kv_s.at[kind, pl.ds((k % 4) * 1024, 1024), :], sem.at[k]
            )
        )
        copies[-1].start()
    size = 2 * CH
    factor = LOG2E / HEAD_SIZE**0.5
    m_s[...] = jnp.full((2, size, 128), -1e30, jnp.float32)
    l_s[...] = jnp.zeros((2, size, 128), jnp.float32)
    o_s[...] = jnp.zeros((2, size, 128), jnp.float32)
    for copy in copies:
        copy.wait()
    here = [qpos[first], qpos[first + 1]]
    pairs = [here[0] // 2, here[1] // 2]

    def keys(kind, p):
        return kv_s[kind, pl.ds(pl.multiple_of(where[p] * CH, CH), CH), :]

    half = size // 2

    def dots(b, t, h):
        return [
            lax.dot_general(
                q_ref[first + b, h * half : h * half + half, :],
                keys(0, 2 * t + i),
                (((1,), (1,)), ((), ())),
                preferred_element_type=jnp.float32,
            )
            for i in range(2)
        ]

    def keep(b, t, h, s0, s1):
        rows = slice(h * half, h * half + half)
        s_s[b, 2 * t, rows, :] = s0
        s_s[b, 2 * t + 1, rows, :] = s1
        top = jnp.maximum(
            jnp.maximum(s0[:, :128], s0[:, 128:]), jnp.maximum(s1[:, :128], s1[:, 128:])
        )
        m_s[b, rows, :] = jnp.maximum(m_s[b, rows, :], top)

    def scores(b, t):
        for h in range(2):
            keep(b, t, h, *dots(b, t, h))

    def last_scores(b):
        t = pairs[b]
        row = lax.broadcasted_iota(jnp.int32, (half, CH), 0)
        gap = row - lax.broadcasted_iota(jnp.int32, (half, CH), 1) + (here[b] - 2 * t) * CH
        for h in range(2):
            s0, s1 = dots(b, t, h)
            keep(b, t, h, jnp.where(gap >= 0, s0, -1e30), jnp.where(gap >= CH, s1, -1e30))
        m_s[b] = jnp.broadcast_to(jnp.max(m_s[b], axis=1, keepdims=True), (size, 128))

    def weigh(b, t):
        v = jnp.concatenate([keys(1, 2 * t), keys(1, 2 * t + 1)], axis=0)
        for h in range(2):
            rows = slice(h * half, h * half + half)
            m = m_s[b, rows, :]
            p = [
                jnp.exp2((s_s[b, 2 * t + k // 2, rows, k % 2 * 128 : k % 2 * 128 + 128] - m) * factor)
                for k in range(4)
            ]
            l_s[b, rows, :] += (p[0] + p[1]) + (p[2] + p[3])
            p = jnp.concatenate([x.astype(jnp.bfloat16) for x in p], axis=1)
            o_s[b, rows, :] += jnp.dot(p, v, preferred_element_type=jnp.float32)

    def store(b):
        total = jnp.sum(l_s[b], axis=1, keepdims=True)
        o = (o_s[b] / total).astype(jnp.bfloat16)
        for i in range(2):
            out_ref[b * CH : b * CH + CH, i * 128 : i * 128 + 128] = o[i * CH : i * CH + CH]

    def loop(low, high, *work):
        def step(t, carry):
            for f, b in work:
                f(b, t)
            return carry

        lax.fori_loop(low, high, step, 0)

    loop(0, pairs[0], (scores, 0))
    last_scores(0)
    both = jnp.minimum(pairs[0] + 1, pairs[1])
    loop(0, both, (scores, 1), (weigh, 0))
    loop(both, pairs[1], (scores, 1))
    loop(both, pairs[0] + 1, (weigh, 0))
    store(0)
    last_scores(1)
    loop(0, pairs[1] + 1, (weigh, 1))
    store(1)


def out_project(info, hidden, target, *rest):
    pieces = rest[:8]
    weights = rest[8:12]
    out_ref, loss_ref, a_s, w_s, sem = rest[12:]
    c, z, y, l, x = info[0], info[1], info[2], info[3], info[4]
    count = 0

    def start(src, dst):
        nonlocal count
        copy = pltpu.make_async_copy(src, dst, sem.at[count])
        copy.start()
        count += 1
        return copy

    waits = []
    for k, piece in enumerate(pieces):
        group = lax.rem(x + (0, 3, 1, 2)[k % 4], 4)
        core = c if k < 4 else 1 - c
        col = pl.multiple_of(group * 512 + core * 256, 256)
        waits.append(start(piece, a_s.at[:, pl.ds(col, 256)]))
    slabs = []
    for t in range(4):
        slab = []
        for k in range(2):
            w = weights[t % 2 * 2 + k]
            for n, dz in enumerate(BACK):
                row = pl.multiple_of(lax.rem(z + 4 - dz, 4) * 512, 512)
                slab.append(
                    start(
                        w.at[n, t // 2],
                        w_s.at[t, pl.ds(row, 512), k * 128 : k * 128 + 128],
                    )
                )
        slabs.append(slab)
    for copy in waits:
        copy.wait()
    loss = jnp.zeros((8, 128), jnp.float32)
    for t in range(4):
        for copy in slabs[t]:
            copy.wait()
        out = jnp.dot(a_s[...], w_s[t], preferred_element_type=jnp.float32)
        for k in range(2):
            yy = lax.rem(y + 4 - BACK[t % 2 * 2 + k], 4)
            col = (lax.rem(l + t // 2, 2) * 4 + yy) * 128
            cols = pl.ds(pl.multiple_of(col, 128), 128)
            branch = out[:, k * 128 : k * 128 + 128].astype(jnp.bfloat16)
            out_ref[:, cols] = branch
            r = hidden[:, cols].astype(jnp.float32) + branch.astype(jnp.float32)
            r = r - target[:, cols].astype(jnp.float32)
            loss = loss + jnp.sum((r * r).reshape(64, 8, 128), axis=0)
    loss_ref[...] = loss


def kernel(body, out_shape, scratch, ins, mib, outs=None):
    if outs is None:
        outs = jax.tree.map(lambda s: VMEM, out_shape)
    out_shape = jax.tree.map(
        lambda s, o: pltpu.HBM(s.shape, s.dtype) if o is FIX else s, out_shape, outs
    )
    call = pl.pallas_call(
        body,
        out_shape=out_shape,
        in_specs=ins,
        out_specs=outs,
        scratch_shapes=scratch,
        compiler_params=pltpu.CompilerParams(vmem_limit_bytes=mib * 2**20),
    )

    def run(*args):
        return call(
            *[
                pltpu.with_memory_space_constraint(v, pltpu.HBM) if i is FIX else v
                for v, i in zip(args, ins)
            ]
        )

    return run


SMEM = pl.BlockSpec(memory_space=pltpu.SMEM)
VMEM = pl.BlockSpec(memory_space=pltpu.VMEM)
ANY = pl.BlockSpec(memory_space=pl.ANY)
FIX = pl.BlockSpec(memory_space=pl.ANY)


def shape(*dims, kind=jnp.bfloat16):
    return jax.ShapeDtypeStruct(dims, kind)


def body(hidden, target, gain, w_query, w_key, value_matrix, w_out, block_order):
    z, l, h, c, y = (lax.axis_index(a) for a in (Z, L, H, C, Y))
    x = 2 * h + l
    local = hidden[0]
    w0 = jnp.concatenate([w_query[:, :256], w_key], axis=1)
    w1 = jnp.concatenate([w_query[:, 256:], value_matrix], axis=1)
    wa = send(jnp.where(l == 0, w0, w1), (L, C), lambda l, c: (c, l))
    wb = send(jnp.where(l == 0, w1, w0), (L, C), lambda l, c: (c, 1 - l))
    sa, sb = along_x(local, 1), along_x(local, -1)
    s2 = along_x(local, 2)
    d0 = swap(local)
    w = around(jnp.stack(around(wa, Y)), Z)
    w = w + around(jnp.stack(around(wb, Z)), Y)
    da, db, d2 = swap(sa), swap(sb), swap(s2)

    def turn(flip):
        return send(
            w_out, (Z, L, H, C), lambda z, l, h, c: (2 * h + c, (l + flip) % 2, z // 2, z % 2)
        )

    o = jnp.stack([turn(0), turn(1)])
    o = around(o, Z)
    o = jnp.stack(o)
    outs = around(o, Y)
    slots = lax.iota(jnp.int32, 16)

    def places(index):
        return jnp.sum(jnp.where(index[:, None] == slots[None, :], block_order[None, :], 0), axis=1)

    two = lax.iota(jnp.int32, 2)
    sides = jnp.stack([l, 1 - l])
    zs = (z + 4 - jnp.array(BACK, jnp.int32)) % 4
    index = (zs[:, None, None] * 2 + sides[None, :, None]) * 2 + two[None, None, :]
    kpos = places(index.reshape(16))
    qpos = kpos[:4]
    inverse = jnp.sum(jnp.where(kpos[None, :] == slots[:, None], slots[None, :], 0), axis=1)
    rows = (qpos[:, None] * CH + lax.iota(jnp.int32, CH)[None, :]).reshape(1024)
    half = HEAD_SIZE // 2
    freqs = ROPE_BASE ** (-(jnp.arange(half, dtype=jnp.float32) * 2.0) / HEAD_SIZE)
    angles = rows.astype(jnp.float32)[:, None] * freqs[None, :]
    cosine, sine = jnp.cos(angles), jnp.sin(angles)
    ha, hb = ((x + 3) % 4) // 2, ((x + 1) % 4) // 2

    far_info = jnp.stack([2 * ha + c, 2 * ha + 1 - c, 2 * hb + c, 2 * hb + 1 - c, c])
    near_info = jnp.stack([2 * h + c, 2 * h + 1 - c, 2 - 2 * h + c, 3 - 2 * h - c, c, z, y])
    far_info, near_info = far_info.astype(jnp.int32), near_info.astype(jnp.int32)
    gain = gain.reshape(1, MODEL_WIDTH)
    dma = pltpu.SemaphoreType.DMA
    rows_s = [pltpu.VMEM((512, MODEL_WIDTH), jnp.bfloat16)]
    table_s = [pltpu.VMEM((2, 1024, 64), jnp.float32), pltpu.VMEM((512, 128), jnp.float32)]
    layout = tuple((k, 0, 512) for k in range(4))
    far_rows = kernel(
        functools.partial(norm, layout),
        shape(512, MODEL_WIDTH),
        rows_s + table_s[1:] + [dma((4,)), dma((2,))],
        [SMEM, VMEM] + [ANY] * 4,
        12,
        FIX,
    )(far_info, gain, sa, da, sb, db)
    kv, near_rows = kernel(
        functools.partial(norm_keys, layout),
        (shape(1024, HEAD_SIZE), shape(512, MODEL_WIDTH)),
        rows_s * 2
        + [pltpu.VMEM((4096, 128), jnp.bfloat16)]
        + table_s
        + [dma((4,)), dma((2,)), dma((32,)), dma((3,))],
        [SMEM, VMEM] + [FIX] * 12 + [ANY] * 3,
        20,
        (VMEM, FIX),
    )(near_info, gain, cosine, sine, far_rows, *w, local, d0, s2, d2)
    mine = around(kv, Z)
    pieces = mine + [swap(v) for v in mine]
    q = kernel(
        queries,
        shape(4, 2 * CH, HEAD_SIZE),
        [
            pltpu.VMEM((1024, MODEL_WIDTH), jnp.bfloat16),
            pltpu.VMEM((4096, 256), jnp.bfloat16),
            table_s[0],
            dma((6,)),
            dma((32,)),
        ],
        [SMEM] + [FIX] * 12,
        20,
    )(near_info, cosine, sine, near_rows, far_rows, *w)

    def attended(first):
        return kernel(
            functools.partial(attention, first),
            shape(512, 256),
            [
                pltpu.VMEM((2, 4096, HEAD_SIZE), jnp.bfloat16),
                pltpu.VMEM((2, 16, 2 * CH, CH), jnp.float32),
                pltpu.VMEM((2, 2 * CH, 128), jnp.float32),
                pltpu.VMEM((2, 2 * CH, 128), jnp.float32),
                pltpu.VMEM((2, 2 * CH, 128), jnp.float32),
                pltpu.SemaphoreType.DMA((8,)),
            ],
            [SMEM, SMEM, VMEM] + [ANY] * 8,
            28,
        )(qinfo, inverse.astype(jnp.int32), q, *pieces)

    qinfo = jnp.concatenate([qpos, c[None]]).astype(jnp.int32)
    far = attended(2)
    near = attended(0)
    got = [near, along_x(far, 1), along_x(far, -1), along_x(near, 2)]
    got = got + [swap(v) for v in got]
    info = jnp.stack([c, z, y, l, x]).astype(jnp.int32)
    branch, squares = kernel(
        out_project,
        (shape(512, 1024), shape(8, 128, kind=jnp.float32)),
        [
            pltpu.VMEM((512, 2048), jnp.bfloat16),
            pltpu.VMEM((4, 2048, 256), jnp.bfloat16),
            pltpu.SemaphoreType.DMA((40,)),
        ],
        [SMEM, VMEM, VMEM] + [ANY] * 12,
        24,
    )(info, local, target[0], *got, *outs)
    squares = squares + swap(squares)
    squares = jnp.broadcast_to(squares[None], (64, 8, 128)).reshape(512, 128)
    squares = lax.all_to_all(squares, (Z, L, H, Y), 0, 0, tiled=True)
    loss = jnp.sum(squares) / (4 * 4096 * MODEL_WIDTH)
    return (branch[None], loss)


def solution(mesh):
    split = Mesh(mesh.devices.reshape(4, 2, 2, 2, 4), (Z, L, H, C, Y))
    rows = P(Y, (Z, L), (H, C))
    weight = P((Z, L, Y), (H, C))
    return jax.shard_map(
        body,
        mesh=split,
        in_specs=(rows, rows, P(), weight, weight, weight, P((H, C), (Z, L, Y)), P()),
        out_specs=(rows, P()),
        check_vma=False,
    )
```

```python
import functools

import jax
import jax.numpy as jnp
import numpy as np
from jax import lax
from jax.experimental import pallas as pl
from jax.experimental.pallas import tpu as pltpu
from jax.sharding import Mesh
from jax.sharding import PartitionSpec as P

MODEL_WIDTH = 4096
HEAD_SIZE = 128
CH = 256
ROPE_BASE = 500000.0
Z, L, H, C, Y = "ctx_0", "ctx_1", "tp_0", "tp_1", "dp"
SIZE = {Z: 4, L: 2, H: 2, C: 2, Y: 4}
BACK = (0, 1, 3, 2)
LOG2E = 1.4426950408889634


def send(value, axes, where):
    order = [a for a in (Z, L, H, C, Y) if a in axes]
    sizes = [SIZE[a] for a in order]
    pairs = []
    for i in range(int(np.prod(sizes))):
        at = dict(zip(order, (int(k) for k in np.unravel_index(i, sizes))))
        to = where(*[at[a] for a in axes])
        if to is not None:
            goal = dict(zip(axes, to))
            pairs.append((i, int(np.ravel_multi_index([goal[a] for a in order], sizes))))
    return lax.ppermute(value, tuple(order), pairs)


def swap(value):
    return send(value, (C,), lambda c: (1 - c,))


def around(value, axis):
    out = [value]
    for by in BACK[1:]:
        out.append(send(value, (axis,), lambda i, by=by: ((i + by) % 4,)))
    return out


def along_x(value, step):
    def where(h, l):
        x = (2 * h + l + step) % 4
        return (x // 2, x % 2)

    return send(value, (H, L), where)


def fetch(layout, info, sources, x_s, sem):
    moves = []
    for src, (slot, rows, size) in zip(sources, layout):
        col = pl.multiple_of(info[slot] * 1024, 1024)
        copy = pltpu.make_async_copy(
            src, x_s.at[pl.ds(rows, size), pl.ds(col, 1024)], sem.at[len(moves)]
        )
        copy.start()
        moves.append((copy, rows, size, col))
    return moves


def normalise(moves, gain, x_s, r_s):
    tile = 64
    r_s[...] = jnp.zeros((512, 128), jnp.float32)
    for copy, first, size, col in moves:
        copy.wait()

        def squares(t, carry, first=first, col=col):
            rows = pl.ds(pl.multiple_of(first + t * tile, tile), tile)
            part = r_s[rows, :]
            for k in range(8):
                x = x_s[rows, pl.ds(col + k * 128, 128)].astype(jnp.float32)
                part = part + x * x
            r_s[rows, :] = part
            return carry

        lax.fori_loop(0, size // tile, squares, 0)
    mean = jnp.sum(r_s[...], axis=1, keepdims=True) * (1.0 / MODEL_WIDTH)
    r_s[...] = jnp.broadcast_to(lax.rsqrt(mean + 1e-05), (512, 128))

    def scale(t, carry):
        rows = pl.ds(pl.multiple_of(t * 32, 32), 32)
        r = r_s[rows, :]
        for k in range(32):
            cols = slice(k * 128, k * 128 + 128)
            x = x_s[rows, cols].astype(jnp.float32)
            x_s[rows, cols] = (x * r * gain[:, cols]).astype(jnp.bfloat16)
        return carry

    for b in range(4):
        lax.fori_loop(b * 4, b * 4 + 4, scale, 0)
        yield pl.ds(b * 128, 128)


def norm(layout, info, gain, *rest):
    count = len(layout)
    out_ref, x_s, r_s, sem, out_sem = rest[count:]
    moves = fetch(layout, info, rest[:count], x_s, sem)
    copies = []
    for rows in normalise(moves, gain, x_s, r_s):
        copies.append(
            pltpu.make_async_copy(x_s.at[rows, :], out_ref.at[rows, :], out_sem.at[len(copies)])
        )
        copies[-1].start()
    for copy in copies:
        copy.wait()


def weights_in(first, width, info, pieces, w_s, sem):
    c, z, y = info[4], info[5], info[6]
    waits = []
    for k, w in enumerate(pieces):
        for n in range(4):
            dz, dy = (BACK[k], BACK[n]) if k < 4 else (BACK[n], BACK[k - 4])
            part = c if k < 4 else 1 - c
            row = lax.rem(z + 4 - dz, 4) * 1024 + part * 512 + lax.rem(y + 4 - dy, 4) * 128
            copy = pltpu.make_async_copy(
                w.at[n, :, pl.ds(first, width)],
                w_s.at[pl.ds(pl.multiple_of(row, 128), 128), :],
                sem.at[len(waits)],
            )
            copy.start()
            waits.append(copy)
    return waits


def rope(v, cs, sn):
    cb = jnp.concatenate([cs, cs], axis=1)
    sb = jnp.concatenate([-sn, sn], axis=1)
    return v * cb + pltpu.roll(v, 64, 1) * sb


def norm_keys(layout, info, gain, cosine, sine, far, *rest):
    count = len(layout)
    pieces, rest = rest[:8], rest[8:]
    kv_ref, out_ref, w_s, t_s, r_s, sem, w_sem, f_sem = rest[count:]
    c = info[4]
    moves = fetch(layout, info, rest[:count], out_ref, sem)
    waits = weights_in(256, 128, info, pieces, w_s, w_sem)
    for k, (src, dst) in enumerate(
        ((far, out_ref.at[pl.ds(512, 512), :]), (cosine, t_s.at[0]), (sine, t_s.at[1]))
    ):
        waits.append(pltpu.make_async_copy(src, dst, f_sem.at[k]))
        waits[-1].start()
    for rows in normalise(moves, gain, out_ref, r_s):
        pass
    for copy in waits:
        copy.wait()
    for side in range(2):
        rows = pl.ds(side * 512, 512)
        v = jnp.dot(out_ref[rows, :], w_s[...], preferred_element_type=jnp.float32)
        turned = rope(v, t_s[0, rows, :], t_s[1, rows, :])
        kv_ref[rows, :] = jnp.where(c == 0, turned, v).astype(jnp.bfloat16)


def queries(info, cosine, sine, rows_ref, *rest):
    pieces = rest[:8]
    q_ref, w_s, t_s, sem, w_sem = rest[8:]
    waits = weights_in(0, 256, info, pieces, w_s, w_sem)
    for k, src in enumerate((cosine, sine)):
        waits.append(pltpu.make_async_copy(src, t_s.at[k], sem.at[k]))
        waits[-1].start()
    for copy in waits:
        copy.wait()
    for side in range(2):
        rows = pl.ds(side * 512, 512)
        out = jnp.dot(rows_ref[rows, :], w_s[...], preferred_element_type=jnp.float32)
        for i in range(2):
            v = out[:, i * 128 : i * 128 + 128]
            v = rope(v, t_s[0, rows, :], t_s[1, rows, :]).astype(jnp.bfloat16)
            for b in range(2):
                q_ref[side * 2 + b, i * CH : i * CH + CH, :] = v[b * CH : b * CH + CH]


def attention(first, qpos, where, q_ref, *rest):
    pieces = rest[:8]
    out_ref, kv_s, s_s, m_s, l_s, o_s, sem = rest[8:]
    c = qpos[4]
    copies = []
    for k, piece in enumerate(pieces):
        kind = c if k < 4 else 1 - c
        copies.append(
            pltpu.make_async_copy(
                piece, kv_s.at[kind, pl.ds((k % 4) * 1024, 1024), :], sem.at[k]
            )
        )
        copies[-1].start()
    size = 2 * CH
    factor = LOG2E / HEAD_SIZE**0.5
    m_s[...] = jnp.full((2, size, 128), -1e30, jnp.float32)
    l_s[...] = jnp.zeros((2, size, 128), jnp.float32)
    o_s[...] = jnp.zeros((2, size, 128), jnp.float32)
    for copy in copies:
        copy.wait()
    here = [qpos[first], qpos[first + 1]]
    pairs = [here[0] // 2, here[1] // 2]

    def keys(kind, p):
        return kv_s[kind, pl.ds(pl.multiple_of(where[p] * CH, CH), CH), :]

    half = size // 2

    def dots(b, t, h):
        return [
            lax.dot_general(
                q_ref[first + b, h * half : h * half + half, :],
                keys(0, 2 * t + i),
                (((1,), (1,)), ((), ())),
                preferred_element_type=jnp.float32,
            )
            for i in range(2)
        ]

    def keep(b, t, h, s0, s1):
        rows = slice(h * half, h * half + half)
        s_s[b, 2 * t, rows, :] = s0
        s_s[b, 2 * t + 1, rows, :] = s1
        top = jnp.maximum(
            jnp.maximum(s0[:, :128], s0[:, 128:]), jnp.maximum(s1[:, :128], s1[:, 128:])
        )
        m_s[b, rows, :] = jnp.maximum(m_s[b, rows, :], top)

    def scores(b, t):
        for h in range(2):
            keep(b, t, h, *dots(b, t, h))

    def last_scores(b):
        t = pairs[b]
        row = lax.broadcasted_iota(jnp.int32, (half, CH), 0)
        gap = row - lax.broadcasted_iota(jnp.int32, (half, CH), 1) + (here[b] - 2 * t) * CH
        for h in range(2):
            s0, s1 = dots(b, t, h)
            keep(b, t, h, jnp.where(gap >= 0, s0, -1e30), jnp.where(gap >= CH, s1, -1e30))
        m_s[b] = jnp.broadcast_to(jnp.max(m_s[b], axis=1, keepdims=True), (size, 128))

    def weigh(b, t):
        v = jnp.concatenate([keys(1, 2 * t), keys(1, 2 * t + 1)], axis=0)
        for h in range(2):
            rows = slice(h * half, h * half + half)
            m = m_s[b, rows, :]
            p = [
                jnp.exp2((s_s[b, 2 * t + k // 2, rows, k % 2 * 128 : k % 2 * 128 + 128] - m) * factor)
                for k in range(4)
            ]
            l_s[b, rows, :] += (p[0] + p[1]) + (p[2] + p[3])
            p = jnp.concatenate([x.astype(jnp.bfloat16) for x in p], axis=1)
            o_s[b, rows, :] += jnp.dot(p, v, preferred_element_type=jnp.float32)

    def store(b):
        total = jnp.sum(l_s[b], axis=1, keepdims=True)
        o = (o_s[b] / total).astype(jnp.bfloat16)
        for i in range(2):
            out_ref[b * CH : b * CH + CH, i * 128 : i * 128 + 128] = o[i * CH : i * CH + CH]

    def loop(low, high, *work):
        def step(t, carry):
            for f, b in work:
                f(b, t)
            return carry

        lax.fori_loop(low, high, step, 0)

    loop(0, pairs[0], (scores, 0))
    last_scores(0)
    both = jnp.minimum(pairs[0] + 1, pairs[1])
    loop(0, both, (scores, 1), (weigh, 0))
    loop(both, pairs[1], (scores, 1))
    loop(both, pairs[0] + 1, (weigh, 0))
    store(0)
    last_scores(1)
    loop(0, pairs[1] + 1, (weigh, 1))
    store(1)


def out_project(info, hidden, target, *rest):
    pieces = rest[:8]
    weights = rest[8:12]
    out_ref, loss_ref, a_s, w_s, sem = rest[12:]
    c, z, y, l, x = info[0], info[1], info[2], info[3], info[4]
    count = 0

    def start(src, dst):
        nonlocal count
        copy = pltpu.make_async_copy(src, dst, sem.at[count])
        copy.start()
        count += 1
        return copy

    waits = []
    for k, piece in enumerate(pieces):
        group = lax.rem(x + (0, 3, 1, 2)[k % 4], 4)
        core = c if k < 4 else 1 - c
        col = pl.multiple_of(group * 512 + core * 256, 256)
        waits.append(start(piece, a_s.at[:, pl.ds(col, 256)]))
    slabs = []
    for part in range(2):
        slab = []
        for k, w in enumerate(weights):
            yy = lax.rem(y + 4 - BACK[k], 4)
            for n, dz in enumerate(BACK):
                row = pl.multiple_of(lax.rem(z + 4 - dz, 4) * 512, 512)
                col = pl.multiple_of((part * 4 + yy) * 128, 128)
                slab.append(
                    start(
                        w.at[n, lax.rem(part + l, 2)],
                        w_s.at[pl.ds(row, 512), pl.ds(col, 128)],
                    )
                )
        slabs.append(slab)
    for copy in waits:
        copy.wait()
    loss = jnp.zeros((8, 128), jnp.float32)
    for t in range(4):
        if t % 2 == 0:
            for copy in slabs[t // 2]:
                copy.wait()
        cols = slice(t * 256, t * 256 + 256)
        branch = jnp.dot(
            a_s[...], w_s[:, cols], preferred_element_type=jnp.float32
        ).astype(jnp.bfloat16)
        out_ref[:, cols] = branch
        r = hidden[:, cols].astype(jnp.float32) + branch.astype(jnp.float32)
        r = r - target[:, cols].astype(jnp.float32)
        r = jnp.sum((r * r).reshape(64, 8, 256), axis=0)
        loss = loss + (r[:, :128] + r[:, 128:])
    loss_ref[...] = loss


def kernel(body, out_shape, scratch, ins, mib, outs=None):
    if outs is None:
        outs = jax.tree.map(lambda s: VMEM, out_shape)
    out_shape = jax.tree.map(
        lambda s, o: pltpu.HBM(s.shape, s.dtype) if o is FIX else s, out_shape, outs
    )
    call = pl.pallas_call(
        body,
        out_shape=out_shape,
        in_specs=ins,
        out_specs=outs,
        scratch_shapes=scratch,
        compiler_params=pltpu.CompilerParams(vmem_limit_bytes=mib * 2**20),
    )

    def run(*args):
        return call(
            *[
                pltpu.with_memory_space_constraint(v, pltpu.HBM) if i is FIX else v
                for v, i in zip(args, ins)
            ]
        )

    return run


SMEM = pl.BlockSpec(memory_space=pltpu.SMEM)
VMEM = pl.BlockSpec(memory_space=pltpu.VMEM)
ANY = pl.BlockSpec(memory_space=pl.ANY)
FIX = pl.BlockSpec(memory_space=pl.ANY)


def shape(*dims, kind=jnp.bfloat16):
    return jax.ShapeDtypeStruct(dims, kind)


def body(hidden, target, gain, w_query, w_key, value_matrix, w_out, block_order):
    z, l, h, c, y = (lax.axis_index(a) for a in (Z, L, H, C, Y))
    x = 2 * h + l
    local = hidden[0]
    w0 = jnp.concatenate([w_query[:, :256], w_key], axis=1)
    w1 = jnp.concatenate([w_query[:, 256:], value_matrix], axis=1)
    wa = send(jnp.where(l == 0, w0, w1), (L, C), lambda l, c: (c, l))
    wb = send(jnp.where(l == 0, w1, w0), (L, C), lambda l, c: (c, 1 - l))
    sa, sb = along_x(local, 1), along_x(local, -1)
    s2 = along_x(local, 2)
    d0 = swap(local)
    w = around(jnp.stack(around(wa, Y)), Z)
    w = w + around(jnp.stack(around(wb, Z)), Y)
    da, db, d2 = swap(sa), swap(sb), swap(s2)

    def turn(flip):
        return send(
            w_out, (Z, L, H, C), lambda z, l, h, c: (2 * h + c, (l + flip) % 2, z // 2, z % 2)
        )

    o = jnp.stack([turn(0), turn(1)])
    o = around(o, Z)
    o = jnp.stack(o)
    outs = around(o, Y)
    slots = lax.iota(jnp.int32, 16)

    def places(index):
        return jnp.sum(jnp.where(index[:, None] == slots[None, :], block_order[None, :], 0), axis=1)

    two = lax.iota(jnp.int32, 2)
    sides = jnp.stack([l, 1 - l])
    zs = (z + 4 - jnp.array(BACK, jnp.int32)) % 4
    index = (zs[:, None, None] * 2 + sides[None, :, None]) * 2 + two[None, None, :]
    kpos = places(index.reshape(16))
    qpos = kpos[:4]
    inverse = jnp.sum(jnp.where(kpos[None, :] == slots[:, None], slots[None, :], 0), axis=1)
    rows = (qpos[:, None] * CH + lax.iota(jnp.int32, CH)[None, :]).reshape(1024)
    half = HEAD_SIZE // 2
    freqs = ROPE_BASE ** (-(jnp.arange(half, dtype=jnp.float32) * 2.0) / HEAD_SIZE)
    angles = rows.astype(jnp.float32)[:, None] * freqs[None, :]
    cosine, sine = jnp.cos(angles), jnp.sin(angles)
    ha, hb = ((x + 3) % 4) // 2, ((x + 1) % 4) // 2

    far_info = jnp.stack([2 * ha + c, 2 * ha + 1 - c, 2 * hb + c, 2 * hb + 1 - c, c])
    near_info = jnp.stack([2 * h + c, 2 * h + 1 - c, 2 - 2 * h + c, 3 - 2 * h - c, c, z, y])
    far_info, near_info = far_info.astype(jnp.int32), near_info.astype(jnp.int32)
    gain = gain.reshape(1, MODEL_WIDTH)
    dma = pltpu.SemaphoreType.DMA
    rows_s = [pltpu.VMEM((512, MODEL_WIDTH), jnp.bfloat16)]
    table_s = [pltpu.VMEM((2, 1024, 64), jnp.float32), pltpu.VMEM((512, 128), jnp.float32)]
    layout = tuple((k, 0, 512) for k in range(4))
    far_rows = kernel(
        functools.partial(norm, layout),
        shape(512, MODEL_WIDTH),
        rows_s + table_s[1:] + [dma((4,)), dma((4,))],
        [SMEM, VMEM] + [ANY] * 4,
        12,
        FIX,
    )(far_info, gain, sa, da, sb, db)
    kv, all_rows = kernel(
        functools.partial(norm_keys, layout),
        (shape(1024, HEAD_SIZE), shape(1024, MODEL_WIDTH)),
        [pltpu.VMEM((4096, 128), jnp.bfloat16)] + table_s + [dma((4,)), dma((32,)), dma((3,))],
        [SMEM, VMEM] + [FIX] * 12 + [ANY] * 3,
        20,
    )(near_info, gain, cosine, sine, far_rows, *w, local, d0, s2, d2)
    mine = around(kv, Z)
    pieces = mine + [swap(v) for v in mine]
    q = kernel(
        queries,
        shape(4, 2 * CH, HEAD_SIZE),
        [pltpu.VMEM((4096, 256), jnp.bfloat16), table_s[0], dma((2,)), dma((32,))],
        [SMEM, FIX, FIX, VMEM] + [FIX] * 8,
        20,
    )(near_info, cosine, sine, all_rows, *w)

    def attended(first):
        return kernel(
            functools.partial(attention, first),
            shape(512, 256),
            [
                pltpu.VMEM((2, 4096, HEAD_SIZE), jnp.bfloat16),
                pltpu.VMEM((2, 16, 2 * CH, CH), jnp.float32),
                pltpu.VMEM((2, 2 * CH, 128), jnp.float32),
                pltpu.VMEM((2, 2 * CH, 128), jnp.float32),
                pltpu.VMEM((2, 2 * CH, 128), jnp.float32),
                pltpu.SemaphoreType.DMA((8,)),
            ],
            [SMEM, SMEM, VMEM] + [ANY] * 8,
            28,
        )(qinfo, inverse.astype(jnp.int32), q, *pieces)

    qinfo = jnp.concatenate([qpos, c[None]]).astype(jnp.int32)
    far = attended(2)
    near = attended(0)
    got = [near, along_x(far, 1), along_x(far, -1), along_x(near, 2)]
    got = got + [swap(v) for v in got]
    info = jnp.stack([c, z, y, l, x]).astype(jnp.int32)
    branch, squares = kernel(
        out_project,
        (shape(512, 1024), shape(8, 128, kind=jnp.float32)),
        [
            pltpu.VMEM((512, 2048), jnp.bfloat16),
            pltpu.VMEM((2048, 1024), jnp.bfloat16),
            pltpu.SemaphoreType.DMA((40,)),
        ],
        [SMEM, VMEM, VMEM] + [ANY] * 12,
        24,
    )(info, local, target[0], *got, *outs)
    squares = squares + swap(squares)
    squares = jnp.broadcast_to(squares[None], (64, 8, 128)).reshape(512, 128)
    squares = lax.all_to_all(squares, (Z, L, H, Y), 0, 0, tiled=True)
    loss = jnp.sum(squares) / (4 * 4096 * MODEL_WIDTH)
    return (branch[None], loss)


def solution(mesh):
    split = Mesh(mesh.devices.reshape(4, 2, 2, 2, 4), (Z, L, H, C, Y))
    rows = P(Y, (Z, L), (H, C))
    weight = P((Z, L, Y), (H, C))
    return jax.shard_map(
        body,
        mesh=split,
        in_specs=(rows, rows, P(), weight, weight, weight, P((H, C), (Z, L, Y)), P()),
        out_specs=(rows, P()),
        check_vma=False,
    )
```

```python
import functools

import jax
import jax.numpy as jnp
import numpy as np
from jax import lax
from jax.experimental import pallas as pl
from jax.experimental.pallas import tpu as pltpu
from jax.sharding import Mesh
from jax.sharding import PartitionSpec as P

MODEL_WIDTH = 4096
HEAD_SIZE = 128
CH = 256
ROPE_BASE = 500000.0
Z, L, H, C, Y = "ctx_0", "ctx_1", "tp_0", "tp_1", "dp"
SIZE = {Z: 4, L: 2, H: 2, C: 2, Y: 4}
BACK = (0, 1, 3, 2)
LOG2E = 1.4426950408889634


def send(value, axes, where):
    order = [a for a in (Z, L, H, C, Y) if a in axes]
    sizes = [SIZE[a] for a in order]
    pairs = []
    for i in range(int(np.prod(sizes))):
        at = dict(zip(order, (int(k) for k in np.unravel_index(i, sizes))))
        to = where(*[at[a] for a in axes])
        if to is not None:
            goal = dict(zip(axes, to))
            pairs.append((i, int(np.ravel_multi_index([goal[a] for a in order], sizes))))
    return lax.ppermute(value, tuple(order), pairs)


def swap(value):
    return send(value, (C,), lambda c: (1 - c,))


def around(value, axis):
    out = [value]
    for by in BACK[1:]:
        out.append(send(value, (axis,), lambda i, by=by: ((i + by) % 4,)))
    return out


def along_x(value, step):
    def where(h, l):
        x = (2 * h + l + step) % 4
        return (x // 2, x % 2)

    return send(value, (H, L), where)


def fetch(layout, info, sources, x_s, sem):
    moves = []
    for src, (slot, rows, size) in zip(sources, layout):
        col = pl.multiple_of(info[slot] * 1024, 1024)
        copy = pltpu.make_async_copy(
            src, x_s.at[pl.ds(rows, size), pl.ds(col, 1024)], sem.at[len(moves)]
        )
        copy.start()
        moves.append((copy, rows, size, col))
    return moves


def normalise(moves, gain, x_s, r_s):
    tile = 64
    r_s[...] = jnp.zeros((512, 128), jnp.float32)
    for copy, first, size, col in moves:
        copy.wait()

        def squares(t, carry, first=first, col=col):
            rows = pl.ds(pl.multiple_of(first + t * tile, tile), tile)
            part = r_s[rows, :]
            for k in range(8):
                x = x_s[rows, pl.ds(col + k * 128, 128)].astype(jnp.float32)
                part = part + x * x
            r_s[rows, :] = part
            return carry

        lax.fori_loop(0, size // tile, squares, 0)
    mean = jnp.sum(r_s[...], axis=1, keepdims=True) * (1.0 / MODEL_WIDTH)
    r_s[...] = jnp.broadcast_to(lax.rsqrt(mean + 1e-05), (512, 128))

    def scale(t, carry):
        rows = pl.ds(pl.multiple_of(t * 32, 32), 32)
        r = r_s[rows, :]
        for k in range(32):
            cols = slice(k * 128, k * 128 + 128)
            x = x_s[rows, cols].astype(jnp.float32)
            x_s[rows, cols] = (x * r * gain[:, cols]).astype(jnp.bfloat16)
        return carry

    for b in range(4):
        lax.fori_loop(b * 4, b * 4 + 4, scale, 0)
        yield pl.ds(b * 128, 128)


def norm(layout, info, gain, *rest):
    count = len(layout)
    out_ref, x_s, r_s, sem, out_sem = rest[count:]
    moves = fetch(layout, info, rest[:count], x_s, sem)
    copies = []
    for rows in normalise(moves, gain, x_s, r_s):
        copies.append(
            pltpu.make_async_copy(x_s.at[rows, :], out_ref.at[rows, :], out_sem.at[len(copies)])
        )
        copies[-1].start()
    for copy in copies:
        copy.wait()


def weights_in(first, width, info, pieces, w_s, sem):
    c, z, y = info[4], info[5], info[6]
    waits = []
    for k, w in enumerate(pieces):
        for n in range(4):
            dz, dy = (BACK[k], BACK[n]) if k < 4 else (BACK[n], BACK[k - 4])
            part = c if k < 4 else 1 - c
            row = lax.rem(z + 4 - dz, 4) * 1024 + part * 512 + lax.rem(y + 4 - dy, 4) * 128
            copy = pltpu.make_async_copy(
                w.at[n, :, pl.ds(first, width)],
                w_s.at[pl.ds(pl.multiple_of(row, 128), 128), :],
                sem.at[len(waits)],
            )
            copy.start()
            waits.append(copy)
    return waits


def rope(v, side, t_s):
    left = lax.broadcasted_iota(jnp.int32, (512, HEAD_SIZE), 1) < HEAD_SIZE // 2
    cs, sn = t_s[0], t_s[1]
    low = left if side == 0 else jnp.logical_not(left)
    cb = jnp.where(low, cs, pltpu.roll(cs, 64, 1))
    sb = jnp.where(low, sn, pltpu.roll(sn, 64, 1))
    return v * cb + pltpu.roll(v, 64, 1) * jnp.where(left, -sb, sb)


def norm_keys(layout, info, gain, cosine, sine, far, *rest):
    count = len(layout)
    pieces, rest = rest[:8], rest[8:]
    kv_ref, out_ref, w_s, t_s, r_s, sem, w_sem, f_sem = rest[count:]
    c = info[4]
    moves = fetch(layout, info, rest[:count], out_ref, sem)
    waits = weights_in(256, 128, info, pieces, w_s, w_sem)
    for k, (src, dst) in enumerate(
        ((far, out_ref.at[pl.ds(512, 512), :]), (cosine, t_s.at[0]), (sine, t_s.at[1]))
    ):
        waits.append(pltpu.make_async_copy(src, dst, f_sem.at[k]))
        waits[-1].start()
    for rows in normalise(moves, gain, out_ref, r_s):
        pass
    for copy in waits:
        copy.wait()
    for side in range(2):
        rows = pl.ds(side * 512, 512)
        v = jnp.dot(out_ref[rows, :], w_s[...], preferred_element_type=jnp.float32)
        turned = rope(v, side, t_s)
        kv_ref[rows, :] = jnp.where(c == 0, turned, v).astype(jnp.bfloat16)


def queries(info, cosine, sine, rows_ref, *rest):
    pieces = rest[:8]
    q_ref, w_s, t_s, sem, w_sem = rest[8:]
    waits = weights_in(0, 256, info, pieces, w_s, w_sem)
    for k, src in enumerate((cosine, sine)):
        waits.append(pltpu.make_async_copy(src, t_s.at[k], sem.at[k]))
        waits[-1].start()
    for copy in waits:
        copy.wait()
    for side in range(2):
        rows = pl.ds(side * 512, 512)
        out = jnp.dot(rows_ref[rows, :], w_s[...], preferred_element_type=jnp.float32)
        for i in range(2):
            v = out[:, i * 128 : i * 128 + 128]
            v = rope(v, side, t_s).astype(jnp.bfloat16)
            for b in range(2):
                q_ref[side * 2 + b, i * CH : i * CH + CH, :] = v[b * CH : b * CH + CH]


def attention(first, qpos, where, q_ref, *rest):
    pieces = rest[:8]
    out_ref, kv_s, s_s, m_s, l_s, o_s, sem = rest[8:]
    c = qpos[4]
    copies = []
    for k, piece in enumerate(pieces):
        kind = c if k < 4 else 1 - c
        copies.append(
            pltpu.make_async_copy(
                piece, kv_s.at[kind, pl.ds((k % 4) * 1024, 1024), :], sem.at[k]
            )
        )
        copies[-1].start()
    size = 2 * CH
    factor = LOG2E / HEAD_SIZE**0.5
    m_s[...] = jnp.full((2, size, 128), -1e30, jnp.float32)
    l_s[...] = jnp.zeros((2, size, 128), jnp.float32)
    o_s[...] = jnp.zeros((2, size, 128), jnp.float32)
    for copy in copies:
        copy.wait()
    here = [qpos[first], qpos[first + 1]]
    pairs = [here[0] // 2, here[1] // 2]

    def keys(kind, p):
        return kv_s[kind, pl.ds(pl.multiple_of(where[p] * CH, CH), CH), :]

    half = size // 2

    def dots(b, t, h):
        return [
            lax.dot_general(
                q_ref[first + b, h * half : h * half + half, :],
                keys(0, 2 * t + i),
                (((1,), (1,)), ((), ())),
                preferred_element_type=jnp.float32,
            )
            for i in range(2)
        ]

    def keep(b, t, h, s0, s1):
        rows = slice(h * half, h * half + half)
        s_s[b, 2 * t, rows, :] = s0
        s_s[b, 2 * t + 1, rows, :] = s1
        top = jnp.maximum(
            jnp.maximum(s0[:, :128], s0[:, 128:]), jnp.maximum(s1[:, :128], s1[:, 128:])
        )
        m_s[b, rows, :] = jnp.maximum(m_s[b, rows, :], top)

    def scores(b, t):
        for h in range(2):
            keep(b, t, h, *dots(b, t, h))

    def last_scores(b):
        t = pairs[b]
        row = lax.broadcasted_iota(jnp.int32, (half, CH), 0)
        gap = row - lax.broadcasted_iota(jnp.int32, (half, CH), 1) + (here[b] - 2 * t) * CH
        for h in range(2):
            s0, s1 = dots(b, t, h)
            keep(b, t, h, jnp.where(gap >= 0, s0, -1e30), jnp.where(gap >= CH, s1, -1e30))
        m_s[b] = jnp.broadcast_to(jnp.max(m_s[b], axis=1, keepdims=True), (size, 128))

    def weigh(b, t):
        v = jnp.concatenate([keys(1, 2 * t), keys(1, 2 * t + 1)], axis=0)
        for h in range(2):
            rows = slice(h * half, h * half + half)
            m = m_s[b, rows, :]
            p = [
                jnp.exp2((s_s[b, 2 * t + k // 2, rows, k % 2 * 128 : k % 2 * 128 + 128] - m) * factor)
                for k in range(4)
            ]
            l_s[b, rows, :] += (p[0] + p[1]) + (p[2] + p[3])
            p = jnp.concatenate([x.astype(jnp.bfloat16) for x in p], axis=1)
            o_s[b, rows, :] += jnp.dot(p, v, preferred_element_type=jnp.float32)

    def store(b):
        total = jnp.sum(l_s[b], axis=1, keepdims=True)
        o = (o_s[b] / total).astype(jnp.bfloat16)
        for i in range(2):
            out_ref[b * CH : b * CH + CH, i * 128 : i * 128 + 128] = o[i * CH : i * CH + CH]

    def loop(low, high, *work):
        def step(t, carry):
            for f, b in work:
                f(b, t)
            return carry

        lax.fori_loop(low, high, step, 0)

    loop(0, pairs[0], (scores, 0))
    last_scores(0)
    both = jnp.minimum(pairs[0] + 1, pairs[1])
    loop(0, both, (scores, 1), (weigh, 0))
    loop(both, pairs[1], (scores, 1))
    loop(both, pairs[0] + 1, (weigh, 0))
    store(0)
    last_scores(1)
    loop(0, pairs[1] + 1, (weigh, 1))
    store(1)


def out_project(info, hidden, target, *rest):
    pieces = rest[:8]
    weights = rest[8:16]
    out_ref, loss_ref, a_s, w_s, sem = rest[16:]
    c, z, y, l, x = info[0], info[1], info[2], info[3], info[4]
    count = 0

    def start(src, dst):
        nonlocal count
        copy = pltpu.make_async_copy(src, dst, sem.at[count])
        copy.start()
        count += 1
        return copy

    waits = []
    for k, piece in enumerate(pieces):
        group = lax.rem(x + (0, 3, 1, 2)[k % 4], 4)
        core = c if k < 4 else 1 - c
        col = pl.multiple_of(group * 512 + core * 256, 256)
        waits.append(start(piece, a_s.at[:, pl.ds(col, 256)]))
    slabs = []
    for part in range(2):
        slab = []
        for k, w in enumerate(weights):
            yy = lax.rem(y + 4 - BACK[k % 4], 4)
            for n in range(2):
                zz = lax.rem(z + 4 - BACK[k // 4 * 2 + n], 4)
                row = pl.multiple_of(zz * 512, 512)
                col = pl.multiple_of((part * 4 + yy) * 128, 128)
                slab.append(
                    start(
                        w.at[n, lax.rem(part + l, 2)],
                        w_s.at[pl.ds(row, 512), pl.ds(col, 128)],
                    )
                )
        slabs.append(slab)
    for copy in waits:
        copy.wait()
    loss = jnp.zeros((8, 128), jnp.float32)
    for t in range(4):
        if t % 2 == 0:
            for copy in slabs[t // 2]:
                copy.wait()
        cols = slice(t * 256, t * 256 + 256)
        branch = jnp.dot(
            a_s[...], w_s[:, cols], preferred_element_type=jnp.float32
        ).astype(jnp.bfloat16)
        out_ref[:, cols] = branch
        r = hidden[:, cols].astype(jnp.float32) + branch.astype(jnp.float32)
        r = r - target[:, cols].astype(jnp.float32)
        r = jnp.sum((r * r).reshape(64, 8, 256), axis=0)
        loss = loss + (r[:, :128] + r[:, 128:])
    loss_ref[...] = loss


def kernel(body, out_shape, scratch, ins, mib, outs=None):
    if outs is None:
        outs = jax.tree.map(lambda s: VMEM, out_shape)
    out_shape = jax.tree.map(
        lambda s, o: pltpu.HBM(s.shape, s.dtype) if o is FIX else s, out_shape, outs
    )
    call = pl.pallas_call(
        body,
        out_shape=out_shape,
        in_specs=ins,
        out_specs=outs,
        scratch_shapes=scratch,
        compiler_params=pltpu.CompilerParams(vmem_limit_bytes=mib * 2**20),
    )

    def run(*args):
        return call(
            *[
                pltpu.with_memory_space_constraint(v, pltpu.HBM) if i is FIX else v
                for v, i in zip(args, ins)
            ]
        )

    return run


SMEM = pl.BlockSpec(memory_space=pltpu.SMEM)
VMEM = pl.BlockSpec(memory_space=pltpu.VMEM)
ANY = pl.BlockSpec(memory_space=pl.ANY)
FIX = pl.BlockSpec(memory_space=pl.ANY)


def shape(*dims, kind=jnp.bfloat16):
    return jax.ShapeDtypeStruct(dims, kind)


def body(hidden, target, gain, w_query, w_key, value_matrix, w_out, block_order):
    z, l, h, c, y = (lax.axis_index(a) for a in (Z, L, H, C, Y))
    x = 2 * h + l
    local = hidden[0]
    w0 = jnp.concatenate([w_query[:, :256], w_key], axis=1)
    w1 = jnp.concatenate([w_query[:, 256:], value_matrix], axis=1)
    wa = send(jnp.where(l == 0, w0, w1), (L, C), lambda l, c: (c, l))
    wb = send(jnp.where(l == 0, w1, w0), (L, C), lambda l, c: (c, 1 - l))
    low, high = local[:256], local[256:]
    sal, sah = along_x(low, 1), along_x(high, 1)
    sbl, sbh = along_x(low, -1), along_x(high, -1)
    d0 = swap(local)
    w = around(jnp.stack(around(wa, Y)), Z)
    w = w + around(jnp.stack(around(wb, Z)), Y)
    fa, fb = along_x(sal, 1), along_x(sbh, -1)
    dal, dah, dbl, dbh = (
        swap(v) for v in (sal, sah, sbl, sbh)
    )
    dfa, dfb = swap(fa), swap(fb)

    def turn(flip):
        return send(
            w_out, (Z, L, H, C), lambda z, l, h, c: (2 * h + c, (l + flip) % 2, z // 2, z % 2)
        )

    o = jnp.stack([turn(0), turn(1)])
    o = around(o, Z)
    oa, ob = jnp.stack(o[:2]), jnp.stack(o[2:])

    def along_y(value, by):
        return send(value, (Y,), lambda i: ((i + by) % 4,))

    oa1, ob1 = along_y(oa, 1), along_y(ob, 1)
    oa3, ob3 = along_y(oa, 3), along_y(ob, 3)
    oa2, ob2 = along_y(oa1, 1), along_y(ob3, 3)
    outs = [oa, oa1, oa3, oa2, ob, ob1, ob3, ob2]
    slots = lax.iota(jnp.int32, 16)

    def places(index):
        return jnp.sum(jnp.where(index[:, None] == slots[None, :], block_order[None, :], 0), axis=1)

    two = lax.iota(jnp.int32, 2)
    sides = jnp.stack([l, 1 - l])
    zs = (z + 4 - jnp.array(BACK, jnp.int32)) % 4
    index = (zs[:, None, None] * 2 + sides[None, :, None]) * 2 + two[None, None, :]
    kpos = places(index.reshape(16))
    qpos = kpos[:4]
    inverse = jnp.sum(jnp.where(kpos[None, :] == slots[:, None], slots[None, :], 0), axis=1)
    rows = (qpos[:, None] * CH + lax.iota(jnp.int32, CH)[None, :]).reshape(2, 512)
    half = HEAD_SIZE // 2
    freqs = ROPE_BASE ** (-(jnp.arange(half, dtype=jnp.float32) * 2.0) / HEAD_SIZE)
    spread = jnp.where(
        lax.iota(jnp.int32, HEAD_SIZE)[None, :] < half, rows[0][:, None], rows[1][:, None]
    ).astype(jnp.float32)
    angles = spread * jnp.concatenate([freqs, freqs])[None, :]
    cosine, sine = jnp.cos(angles), jnp.sin(angles)
    ha, hb = ((x + 3) % 4) // 2, ((x + 1) % 4) // 2

    far_info = jnp.stack([2 * ha + c, 2 * ha + 1 - c, 2 * hb + c, 2 * hb + 1 - c, c])
    near_info = jnp.stack([2 * h + c, 2 * h + 1 - c, 2 - 2 * h + c, 3 - 2 * h - c, c, z, y])
    far_info, near_info = far_info.astype(jnp.int32), near_info.astype(jnp.int32)
    gain = gain.reshape(1, MODEL_WIDTH)
    dma = pltpu.SemaphoreType.DMA
    rows_s = [pltpu.VMEM((512, MODEL_WIDTH), jnp.bfloat16)]
    table_s = [pltpu.VMEM((2, 512, 128), jnp.float32), pltpu.VMEM((512, 128), jnp.float32)]
    layout = tuple((k // 2, k % 2 * 256, 256) for k in range(8))
    far_rows = kernel(
        functools.partial(norm, layout),
        shape(512, MODEL_WIDTH),
        rows_s + table_s[1:] + [dma((8,)), dma((4,))],
        [SMEM, VMEM] + [ANY] * 8,
        12,
        FIX,
    )(far_info, gain, sal, sah, dal, dah, sbl, sbh, dbl, dbh)
    layout = ((0, 0, 512), (1, 0, 512), (2, 0, 256), (2, 256, 256), (3, 0, 256), (3, 256, 256))
    kv, all_rows = kernel(
        functools.partial(norm_keys, layout),
        (shape(1024, HEAD_SIZE), shape(1024, MODEL_WIDTH)),
        [pltpu.VMEM((4096, 128), jnp.bfloat16)] + table_s + [dma((6,)), dma((32,)), dma((3,))],
        [SMEM, VMEM] + [FIX] * 12 + [ANY] * 5,
        20,
    )(near_info, gain, cosine, sine, far_rows, *w, local, d0, fa, fb, dfa, dfb)
    mine = around(kv, Z)
    pieces = mine + [swap(v) for v in mine]
    q = kernel(
        queries,
        shape(4, 2 * CH, HEAD_SIZE),
        [pltpu.VMEM((4096, 256), jnp.bfloat16), table_s[0], dma((2,)), dma((32,))],
        [SMEM, FIX, FIX, VMEM] + [FIX] * 8,
        20,
    )(near_info, cosine, sine, all_rows, *w)

    def attended(first):
        return kernel(
            functools.partial(attention, first),
            shape(512, 256),
            [
                pltpu.VMEM((2, 4096, HEAD_SIZE), jnp.bfloat16),
                pltpu.VMEM((2, 16, 2 * CH, CH), jnp.float32),
                pltpu.VMEM((2, 2 * CH, 128), jnp.float32),
                pltpu.VMEM((2, 2 * CH, 128), jnp.float32),
                pltpu.VMEM((2, 2 * CH, 128), jnp.float32),
                pltpu.SemaphoreType.DMA((8,)),
            ],
            [SMEM, SMEM, VMEM] + [ANY] * 8,
            28,
        )(qinfo, inverse.astype(jnp.int32), q, *pieces)

    qinfo = jnp.concatenate([qpos, c[None]]).astype(jnp.int32)
    far = attended(2)
    near = attended(0)
    got = [near, along_x(far, 1), along_x(far, -1), along_x(near, 2)]
    got = got + [swap(v) for v in got]
    info = jnp.stack([c, z, y, l, x]).astype(jnp.int32)
    branch, squares = kernel(
        out_project,
        (shape(512, 1024), shape(8, 128, kind=jnp.float32)),
        [
            pltpu.VMEM((512, 2048), jnp.bfloat16),
            pltpu.VMEM((2048, 1024), jnp.bfloat16),
            pltpu.SemaphoreType.DMA((40,)),
        ],
        [SMEM, VMEM, VMEM] + [ANY] * 16,
        24,
    )(info, local, target[0], *got, *outs)
    squares = squares + swap(squares)
    squares = jnp.broadcast_to(squares[None], (64, 8, 128)).reshape(512, 128)
    squares = lax.all_to_all(squares, (Z, L, H, Y), 0, 0, tiled=True)
    loss = jnp.sum(squares) / (4 * 4096 * MODEL_WIDTH)
    return (branch[None], loss)


def solution(mesh):
    split = Mesh(mesh.devices.reshape(4, 2, 2, 2, 4), (Z, L, H, C, Y))
    rows = P(Y, (Z, L), (H, C))
    weight = P((Z, L, Y), (H, C))
    return jax.shard_map(
        body,
        mesh=split,
        in_specs=(rows, rows, P(), weight, weight, weight, P((H, C), (Z, L, Y)), P()),
        out_specs=(rows, P()),
        check_vma=False,
    )
```

```python
import functools

import jax
import jax.numpy as jnp
import numpy as np
from jax import lax
from jax.experimental import pallas as pl
from jax.experimental.pallas import tpu as pltpu
from jax.sharding import Mesh
from jax.sharding import PartitionSpec as P

MODEL_WIDTH = 4096
HEAD_SIZE = 128
CH = 256
ROPE_BASE = 500000.0
Z, L, H, C, Y = "ctx_0", "ctx_1", "tp_0", "tp_1", "dp"
SIZE = {Z: 4, L: 2, H: 2, C: 2, Y: 4}
BACK = (0, 1, 3, 2)
LOG2E = 1.4426950408889634


def send(value, axes, where):
    order = [a for a in (Z, L, H, C, Y) if a in axes]
    sizes = [SIZE[a] for a in order]
    pairs = []
    for i in range(int(np.prod(sizes))):
        at = dict(zip(order, (int(k) for k in np.unravel_index(i, sizes))))
        to = where(*[at[a] for a in axes])
        if to is not None:
            goal = dict(zip(axes, to))
            pairs.append((i, int(np.ravel_multi_index([goal[a] for a in order], sizes))))
    return lax.ppermute(value, tuple(order), pairs)


def swap(value):
    return send(value, (C,), lambda c: (1 - c,))


def around(value, axis):
    out = [value]
    for by in BACK[1:]:
        out.append(send(value, (axis,), lambda i, by=by: ((i + by) % 4,)))
    return out


def along_x(value, step, core=None):
    def where(h, l, c):
        x = (2 * h + l + step) % 4
        return (x // 2, x % 2, c) if core in (None, c) else None

    return send(value, (H, L, C), where)


def fetch(layout, info, sources, x_s, sem):
    moves = []
    for k, (slot, rows, *picks) in enumerate(layout):
        col = pl.multiple_of(info[slot] * 1024, 1024)
        goal = x_s.at[pl.ds(rows, 512), pl.ds(col, 1024)]
        copies = [pltpu.make_async_copy(sources[p], goal, sem.at[k]) for p in picks]
        if len(picks) == 1:
            copies[0].start()
        else:
            for core in range(2):

                @pl.when(info[4] == core)
                def _(copy=copies[core]):
                    copy.start()

        moves.append((copies[0], rows, 512, col))
    return moves


def normalise(moves, base, gain, x_s, r_s):
    tile = 64
    r_s[...] = jnp.zeros((512, 128), jnp.float32)
    for copy, first, size, col in moves:
        copy.wait()

        def squares(t, carry, first=first, col=col):
            at = pl.multiple_of(first + t * tile, tile)
            rows = pl.ds(at - base, tile)
            part = r_s[rows, :]
            for k in range(8):
                x = x_s[pl.ds(at, tile), pl.ds(col + k * 128, 128)].astype(jnp.float32)
                part = part + x * x
            r_s[rows, :] = part
            return carry

        lax.fori_loop(0, size // tile, squares, 0)
    mean = jnp.sum(r_s[...], axis=1, keepdims=True) * (1.0 / MODEL_WIDTH)
    r_s[...] = jnp.broadcast_to(lax.rsqrt(mean + 1e-05), (512, 128))

    def scale(t, carry):
        at = pl.multiple_of(t * 32, 32)
        r = r_s[pl.ds(at, 32), :]
        rows = pl.ds(at + base, 32)
        for k in range(32):
            cols = slice(k * 128, k * 128 + 128)
            x = x_s[rows, cols].astype(jnp.float32)
            x_s[rows, cols] = (x * r * gain[:, cols]).astype(jnp.bfloat16)
        return carry

    lax.fori_loop(0, 16, scale, 0)


def weights_in(first, width, info, pieces, w_s, sem):
    c, z, y = info[4], info[5], info[6]
    waits = []
    for k, w in enumerate(pieces):
        for n in range(4):
            dz, dy = (BACK[k], BACK[n]) if k < 4 else (BACK[n], BACK[k - 4])
            part = c if k < 4 else 1 - c
            row = lax.rem(z + 4 - dz, 4) * 1024 + part * 512 + lax.rem(y + 4 - dy, 4) * 128
            copy = pltpu.make_async_copy(
                w.at[n, :, pl.ds(first, width)],
                w_s.at[pl.ds(pl.multiple_of(row, 128), 128), :],
                sem.at[len(waits)],
            )
            copy.start()
            waits.append(copy)
    return waits


def rope(v, side, t_s):
    left = lax.broadcasted_iota(jnp.int32, (512, HEAD_SIZE), 1) < HEAD_SIZE // 2
    cs, sn = t_s[0], t_s[1]
    low = left if side == 0 else jnp.logical_not(left)
    cb = jnp.where(low, cs, pltpu.roll(cs, 64, 1))
    sb = jnp.where(low, sn, pltpu.roll(sn, 64, 1))
    return v * cb + pltpu.roll(v, 64, 1) * jnp.where(left, -sb, sb)


def norm_keys(layout, info, gain, cosine, sine, *rest):
    pieces, sources, rest = rest[:8], rest[8:18], rest[18:]
    kv_ref, out_ref, w_s, t_s, r_s, sem, w_sem, f_sem = rest
    c = info[4]
    moves = fetch(layout, info, sources, out_ref, sem)
    waits = weights_in(256, 128, info, pieces, w_s, w_sem)
    for k, src in enumerate((cosine, sine)):
        waits.append(pltpu.make_async_copy(src, t_s.at[k], f_sem.at[k]))
        waits[-1].start()
    for side in (1, 0):
        part = [m for m in moves if m[1] // 512 == side]
        normalise(part, side * 512, gain, out_ref, r_s)
    for copy in waits:
        copy.wait()
    for side in range(2):
        rows = pl.ds(side * 512, 512)
        v = jnp.dot(out_ref[rows, :], w_s[...], preferred_element_type=jnp.float32)
        turned = rope(v, side, t_s)
        kv_ref[rows, :] = jnp.where(c == 0, turned, v).astype(jnp.bfloat16)


def queries(info, cosine, sine, rows_ref, *rest):
    pieces = rest[:8]
    q_ref, w_s, t_s, sem, w_sem = rest[8:]
    waits = weights_in(0, 256, info, pieces, w_s, w_sem)
    for k, src in enumerate((cosine, sine)):
        waits.append(pltpu.make_async_copy(src, t_s.at[k], sem.at[k]))
        waits[-1].start()
    for copy in waits:
        copy.wait()
    for side in range(2):
        rows = pl.ds(side * 512, 512)
        out = jnp.dot(rows_ref[rows, :], w_s[...], preferred_element_type=jnp.float32)
        for i in range(2):
            v = out[:, i * 128 : i * 128 + 128]
            v = rope(v, side, t_s).astype(jnp.bfloat16)
            for b in range(2):
                q_ref[side * 2 + b, i * CH : i * CH + CH, :] = v[b * CH : b * CH + CH]


def attention(first, qpos, where, q_ref, *rest):
    pieces = rest[:8]
    out_ref, kv_s, s_s, m_s, l_s, o_s, sem = rest[8:]
    c = qpos[4]
    copies = []
    for k, piece in enumerate(pieces):
        kind = c if k < 4 else 1 - c
        copies.append(
            pltpu.make_async_copy(
                piece, kv_s.at[kind, pl.ds((k % 4) * 1024, 1024), :], sem.at[k]
            )
        )
        copies[-1].start()
    size = 2 * CH
    factor = LOG2E / HEAD_SIZE**0.5
    m_s[...] = jnp.full((2, size, 128), -1e30, jnp.float32)
    l_s[...] = jnp.zeros((2, size, 128), jnp.float32)
    o_s[...] = jnp.zeros((2, size, 128), jnp.float32)
    for copy in copies:
        copy.wait()
    here = [qpos[first], qpos[first + 1]]
    pairs = [here[0] // 2, here[1] // 2]

    def keys(kind, p):
        return kv_s[kind, pl.ds(pl.multiple_of(where[p] * CH, CH), CH), :]

    half = size // 2

    def dots(b, t, h):
        return [
            lax.dot_general(
                q_ref[first + b, h * half : h * half + half, :],
                keys(0, 2 * t + i),
                (((1,), (1,)), ((), ())),
                preferred_element_type=jnp.float32,
            )
            for i in range(2)
        ]

    def keep(b, t, h, s0, s1):
        rows = slice(h * half, h * half + half)
        s_s[b, 2 * t, rows, :] = s0
        s_s[b, 2 * t + 1, rows, :] = s1
        top = jnp.maximum(
            jnp.maximum(s0[:, :128], s0[:, 128:]), jnp.maximum(s1[:, :128], s1[:, 128:])
        )
        m_s[b, rows, :] = jnp.maximum(m_s[b, rows, :], top)

    def scores(b, t):
        for h in range(2):
            keep(b, t, h, *dots(b, t, h))

    def last_scores(b):
        t = pairs[b]
        row = lax.broadcasted_iota(jnp.int32, (half, CH), 0)
        gap = row - lax.broadcasted_iota(jnp.int32, (half, CH), 1) + (here[b] - 2 * t) * CH
        for h in range(2):
            s0, s1 = dots(b, t, h)
            keep(b, t, h, jnp.where(gap >= 0, s0, -1e30), jnp.where(gap >= CH, s1, -1e30))
        m_s[b] = jnp.broadcast_to(jnp.max(m_s[b], axis=1, keepdims=True), (size, 128))

    def weigh(b, t):
        v = jnp.concatenate([keys(1, 2 * t), keys(1, 2 * t + 1)], axis=0)
        for h in range(2):
            rows = slice(h * half, h * half + half)
            m = m_s[b, rows, :]
            p = [
                jnp.exp2((s_s[b, 2 * t + k // 2, rows, k % 2 * 128 : k % 2 * 128 + 128] - m) * factor)
                for k in range(4)
            ]
            l_s[b, rows, :] += (p[0] + p[1]) + (p[2] + p[3])
            p = jnp.concatenate([x.astype(jnp.bfloat16) for x in p], axis=1)
            o_s[b, rows, :] += jnp.dot(p, v, preferred_element_type=jnp.float32)

    def store(b):
        total = jnp.sum(l_s[b], axis=1, keepdims=True)
        o = (o_s[b] / total).astype(jnp.bfloat16)
        for i in range(2):
            out_ref[b * CH : b * CH + CH, i * 128 : i * 128 + 128] = o[i * CH : i * CH + CH]

    def loop(low, high, *work):
        def step(t, carry):
            for f, b in work:
                f(b, t)
            return carry

        lax.fori_loop(low, high, step, 0)

    loop(0, pairs[0], (scores, 0))
    last_scores(0)
    both = jnp.minimum(pairs[0] + 1, pairs[1])
    loop(0, both, (scores, 1), (weigh, 0))
    loop(both, pairs[1], (scores, 1))
    loop(both, pairs[0] + 1, (weigh, 0))
    store(0)
    last_scores(1)
    loop(0, pairs[1] + 1, (weigh, 1))
    store(1)


def assemble(info, *rest):
    weights = rest[:8]
    w_ref, sem = rest[8:]
    z, y, l = info[1], info[2], info[3]
    waits = []
    for k, w in enumerate(weights):
        yy = lax.rem(y + 4 - BACK[k % 4], 4)
        for n in range(2):
            zz = lax.rem(z + 4 - BACK[k // 4 * 2 + n], 4)
            row = pl.multiple_of(zz * 512, 512)
            for i in range(2):
                col = pl.multiple_of((lax.rem(l + i, 2) * 4 + yy) * 128, 128)
                copy = pltpu.make_async_copy(
                    w.at[n, i], w_ref.at[pl.ds(row, 512), pl.ds(col, 128)], sem.at[len(waits)]
                )
                copy.start()
                waits.append(copy)
    for copy in waits:
        copy.wait()


def out_project(info, hidden, target, w_ref, *rest):
    pieces = rest[:8]
    out_ref, loss_ref, a_s, sem = rest[8:]
    c, x = info[0], info[4]
    waits = []
    for k, piece in enumerate(pieces):
        group = lax.rem(x + (0, 3, 1, 2)[k % 4], 4)
        core = c if k < 4 else 1 - c
        col = pl.multiple_of(group * 512 + core * 256, 256)
        copy = pltpu.make_async_copy(piece, a_s.at[:, pl.ds(col, 256)], sem.at[k])
        copy.start()
        waits.append(copy)
    for copy in waits:
        copy.wait()
    loss = jnp.zeros((8, 128), jnp.float32)
    for t in range(4):
        cols = slice(t * 256, t * 256 + 256)
        branch = jnp.dot(
            a_s[...], w_ref[:, cols], preferred_element_type=jnp.float32
        ).astype(jnp.bfloat16)
        out_ref[:, cols] = branch
        r = hidden[:, cols].astype(jnp.float32) + branch.astype(jnp.float32)
        r = r - target[:, cols].astype(jnp.float32)
        r = jnp.sum((r * r).reshape(64, 8, 256), axis=0)
        loss = loss + (r[:, :128] + r[:, 128:])
    loss_ref[...] = loss


def kernel(body, out_shape, scratch, ins, mib, outs=None):
    if outs is None:
        outs = jax.tree.map(lambda s: VMEM, out_shape)
    out_shape = jax.tree.map(
        lambda s, o: pltpu.HBM(s.shape, s.dtype) if o is FIX else s, out_shape, outs
    )
    call = pl.pallas_call(
        body,
        out_shape=out_shape,
        in_specs=ins,
        out_specs=outs,
        scratch_shapes=scratch,
        compiler_params=pltpu.CompilerParams(vmem_limit_bytes=mib * 2**20),
    )

    def run(*args):
        return call(
            *[
                pltpu.with_memory_space_constraint(v, pltpu.HBM) if i is FIX else v
                for v, i in zip(args, ins)
            ]
        )

    return run


SMEM = pl.BlockSpec(memory_space=pltpu.SMEM)
VMEM = pl.BlockSpec(memory_space=pltpu.VMEM)
ANY = pl.BlockSpec(memory_space=pl.ANY)
FIX = pl.BlockSpec(memory_space=pl.ANY)


def shape(*dims, kind=jnp.bfloat16):
    return jax.ShapeDtypeStruct(dims, kind)


def body(hidden, target, gain, w_query, w_key, value_matrix, w_out, block_order):
    z, l, h, c, y = (lax.axis_index(a) for a in (Z, L, H, C, Y))
    x = 2 * h + l
    local = hidden[0]
    w0 = jnp.concatenate([w_query[:, :256], w_key], axis=1)
    w1 = jnp.concatenate([w_query[:, 256:], value_matrix], axis=1)
    wa = send(jnp.where(l == 0, w0, w1), (L, C), lambda l, c: (c, l))
    wb = send(jnp.where(l == 0, w1, w0), (L, C), lambda l, c: (c, 1 - l))
    sa, sb = along_x(local, 1), along_x(local, -1)
    d0 = swap(local)
    w = around(jnp.stack(around(wa, Y)), Z)
    w = w + around(jnp.stack(around(wb, Z)), Y)
    fa, fb = along_x(sa, 1, 0), along_x(sb, -1, 1)
    da, db = swap(sa), swap(sb)
    dfa = send(fa, (C,), lambda c: (1,) if c == 0 else None)
    dfb = send(fb, (C,), lambda c: (0,) if c == 1 else None)

    def turn(flip):
        return send(
            w_out, (Z, L, H, C), lambda z, l, h, c: (2 * h + c, (l + flip) % 2, z // 2, z % 2)
        )

    o = jnp.stack([turn(0), turn(1)])
    o = around(o, Z)
    oa, ob = jnp.stack(o[:2]), jnp.stack(o[2:])

    def along_y(value, by):
        return send(value, (Y,), lambda i: ((i + by) % 4,))

    oa1, ob1 = along_y(oa, 1), along_y(ob, 1)
    oa3, ob3 = along_y(oa, 3), along_y(ob, 3)
    oa2, ob2 = along_y(oa1, 1), along_y(ob3, 3)
    outs = [oa, oa1, oa3, oa2, ob, ob1, ob3, ob2]
    slots = lax.iota(jnp.int32, 16)

    def places(index):
        return jnp.sum(jnp.where(index[:, None] == slots[None, :], block_order[None, :], 0), axis=1)

    two = lax.iota(jnp.int32, 2)
    sides = jnp.stack([l, 1 - l])
    zs = (z + 4 - jnp.array(BACK, jnp.int32)) % 4
    index = (zs[:, None, None] * 2 + sides[None, :, None]) * 2 + two[None, None, :]
    kpos = places(index.reshape(16))
    qpos = kpos[:4]
    inverse = jnp.sum(jnp.where(kpos[None, :] == slots[:, None], slots[None, :], 0), axis=1)
    rows = (qpos[:, None] * CH + lax.iota(jnp.int32, CH)[None, :]).reshape(2, 512)
    half = HEAD_SIZE // 2
    freqs = ROPE_BASE ** (-(jnp.arange(half, dtype=jnp.float32) * 2.0) / HEAD_SIZE)
    spread = jnp.where(
        lax.iota(jnp.int32, HEAD_SIZE)[None, :] < half, rows[0][:, None], rows[1][:, None]
    ).astype(jnp.float32)
    angles = spread * jnp.concatenate([freqs, freqs])[None, :]
    cosine, sine = jnp.cos(angles), jnp.sin(angles)
    ha, hb = ((x + 3) % 4) // 2, ((x + 1) % 4) // 2

    far_chunks = [2 * ha + c, 2 * ha + 1 - c, 2 * hb + c, 2 * hb + 1 - c]
    near_chunks = [2 * h + c, 2 * h + 1 - c, 2 - 2 * h + c, 3 - 2 * h - c]
    info = jnp.stack(near_chunks + [c, z, y] + far_chunks).astype(jnp.int32)
    gain = gain.reshape(1, MODEL_WIDTH)
    dma = pltpu.SemaphoreType.DMA
    table_s = [pltpu.VMEM((2, 512, 128), jnp.float32), pltpu.VMEM((512, 128), jnp.float32)]
    layout = (
        (7, 512, 0), (8, 512, 1), (9, 512, 2), (10, 512, 3),
        (0, 0, 4), (1, 0, 5), (2, 0, 6, 7), (3, 0, 9, 8),
    )
    kv, all_rows = kernel(
        functools.partial(norm_keys, layout),
        (shape(1024, HEAD_SIZE), shape(1024, MODEL_WIDTH)),
        [pltpu.VMEM((4096, 128), jnp.bfloat16)] + table_s + [dma((8,)), dma((32,)), dma((2,))],
        [SMEM, VMEM] + [FIX] * 10 + [ANY] * 4 + [FIX] + [ANY] * 5,
        20,
    )(
        info, gain, cosine, sine, *w, sa, da, sb, db, local, d0, fa, fb, dfa, dfb
    )
    mine = around(kv, Z)
    pieces = mine + [swap(v) for v in mine]
    q = kernel(
        queries,
        shape(4, 2 * CH, HEAD_SIZE),
        [pltpu.VMEM((4096, 256), jnp.bfloat16), table_s[0], dma((2,)), dma((32,))],
        [SMEM, FIX, FIX, VMEM] + [FIX] * 8,
        20,
    )(info, cosine, sine, all_rows, *w)

    def attended(first):
        return kernel(
            functools.partial(attention, first),
            shape(512, 256),
            [
                pltpu.VMEM((2, 4096, HEAD_SIZE), jnp.bfloat16),
                pltpu.VMEM((2, 16, 2 * CH, CH), jnp.float32),
                pltpu.VMEM((2, 2 * CH, 128), jnp.float32),
                pltpu.VMEM((2, 2 * CH, 128), jnp.float32),
                pltpu.VMEM((2, 2 * CH, 128), jnp.float32),
                pltpu.SemaphoreType.DMA((8,)),
            ],
            [SMEM, SMEM, VMEM] + [ANY] * 8,
            28,
        )(qinfo, inverse.astype(jnp.int32), q, *pieces)

    qinfo = jnp.concatenate([qpos, c[None]]).astype(jnp.int32)
    far = attended(2)
    near = attended(0)
    got = [near, along_x(far, 1), along_x(far, -1), along_x(near, 2)]
    got = got + [swap(v) for v in got]
    info = jnp.stack([c, z, y, l, x]).astype(jnp.int32)
    w = kernel(assemble, shape(2048, 1024), [dma((32,))], [SMEM] + [ANY] * 8, 8)(info, *outs)
    branch, squares = kernel(
        out_project,
        (shape(512, 1024), shape(8, 128, kind=jnp.float32)),
        [pltpu.VMEM((512, 2048), jnp.bfloat16), dma((8,))],
        [SMEM, VMEM, VMEM, VMEM] + [ANY] * 8,
        20,
    )(info, local, target[0], w, *got)
    squares = squares + swap(squares)
    squares = jnp.broadcast_to(squares[None], (64, 8, 128)).reshape(512, 128)
    squares = lax.all_to_all(squares, (Z, L, H, Y), 0, 0, tiled=True)
    loss = jnp.sum(squares) / (4 * 4096 * MODEL_WIDTH)
    return (branch[None], loss)


def solution(mesh):
    split = Mesh(mesh.devices.reshape(4, 2, 2, 2, 4), (Z, L, H, C, Y))
    rows = P(Y, (Z, L), (H, C))
    weight = P((Z, L, Y), (H, C))
    return jax.shard_map(
        body,
        mesh=split,
        in_specs=(rows, rows, P(), weight, weight, weight, P((H, C), (Z, L, Y)), P()),
        out_specs=(rows, P()),
        check_vma=False,
    )
```

```python
import functools

import jax
import jax.numpy as jnp
import numpy as np
from jax import lax
from jax.experimental import pallas as pl
from jax.experimental.pallas import tpu as pltpu
from jax.sharding import Mesh
from jax.sharding import PartitionSpec as P

MODEL_WIDTH = 4096
HEAD_SIZE = 128
CH = 256
ROPE_BASE = 500000.0
Z, L, H, C, Y = "ctx_0", "ctx_1", "tp_0", "tp_1", "dp"
SIZE = {Z: 4, L: 2, H: 2, C: 2, Y: 4}
BACK = (0, 1, 3, 2)
LOG2E = 1.4426950408889634


def send(value, axes, where):
    order = [a for a in (Z, L, H, C, Y) if a in axes]
    sizes = [SIZE[a] for a in order]
    pairs = []
    for i in range(int(np.prod(sizes))):
        at = dict(zip(order, (int(k) for k in np.unravel_index(i, sizes))))
        to = where(*[at[a] for a in axes])
        if to is not None:
            goal = dict(zip(axes, to))
            pairs.append((i, int(np.ravel_multi_index([goal[a] for a in order], sizes))))
    return lax.ppermute(value, tuple(order), pairs)


def swap(value):
    return send(value, (C,), lambda c: (1 - c,))


def around(value, axis):
    out = [value]
    for by in BACK[1:]:
        out.append(send(value, (axis,), lambda i, by=by: ((i + by) % 4,)))
    return out


def along_x(value, step):
    def where(h, l):
        x = (2 * h + l + step) % 4
        return (x // 2, x % 2)

    return send(value, (H, L), where)


def fetch(layout, info, sources, x_s, sem):
    moves = []
    for src, (slot, rows, size) in zip(sources, layout):
        col = pl.multiple_of(info[slot] * 1024, 1024)
        copy = pltpu.make_async_copy(
            src, x_s.at[pl.ds(rows, size), pl.ds(col, 1024)], sem.at[len(moves)]
        )
        copy.start()
        moves.append((copy, rows, size, col))
    return moves


def normalise(moves, base, gain, x_s, r_s):
    tile = 64
    r_s[...] = jnp.zeros((512, 128), jnp.float32)
    for copy, first, size, col in moves:
        copy.wait()

        def squares(t, carry, first=first, col=col):
            at = pl.multiple_of(first + t * tile, tile)
            rows = pl.ds(at - base, tile)
            part = r_s[rows, :]
            for k in range(8):
                x = x_s[pl.ds(at, tile), pl.ds(col + k * 128, 128)].astype(jnp.float32)
                part = part + x * x
            r_s[rows, :] = part
            return carry

        lax.fori_loop(0, size // tile, squares, 0)
    mean = jnp.sum(r_s[...], axis=1, keepdims=True) * (1.0 / MODEL_WIDTH)
    r_s[...] = jnp.broadcast_to(lax.rsqrt(mean + 1e-05), (512, 128))

    def scale(t, carry):
        at = pl.multiple_of(t * 32, 32)
        r = r_s[pl.ds(at, 32), :]
        rows = pl.ds(at + base, 32)
        for k in range(32):
            cols = slice(k * 128, k * 128 + 128)
            x = x_s[rows, cols].astype(jnp.float32)
            x_s[rows, cols] = (x * r * gain[:, cols]).astype(jnp.bfloat16)
        return carry

    lax.fori_loop(0, 16, scale, 0)


def weights_in(first, width, info, pieces, w_s, sem):
    c, z, y = info[4], info[5], info[6]
    waits = []
    for k, w in enumerate(pieces):
        for n in range(4):
            dz, dy = (BACK[k], BACK[n]) if k < 4 else (BACK[n], BACK[k - 4])
            part = c if k < 4 else 1 - c
            row = lax.rem(z + 4 - dz, 4) * 1024 + part * 512 + lax.rem(y + 4 - dy, 4) * 128
            copy = pltpu.make_async_copy(
                w.at[n, :, pl.ds(first, width)],
                w_s.at[pl.ds(pl.multiple_of(row, 128), 128), :],
                sem.at[len(waits)],
            )
            copy.start()
            waits.append(copy)
    return waits


def rope(v, side, t_s):
    left = lax.broadcasted_iota(jnp.int32, (512, HEAD_SIZE), 1) < HEAD_SIZE // 2
    cs, sn = t_s[0], t_s[1]
    low = left if side == 0 else jnp.logical_not(left)
    cb = jnp.where(low, cs, pltpu.roll(cs, 64, 1))
    sb = jnp.where(low, sn, pltpu.roll(sn, 64, 1))
    return v * cb + pltpu.roll(v, 64, 1) * jnp.where(left, -sb, sb)


def norm_keys(layout, info, gain, cosine, sine, *rest):
    count = len(layout)
    pieces, rest = rest[:8], rest[8:]
    kv_ref, out_ref, w_s, t_s, r_s, sem, w_sem, f_sem = rest[count:]
    c = info[4]
    moves = fetch(layout, info, rest[:count], out_ref, sem)
    waits = weights_in(256, 128, info, pieces, w_s, w_sem)
    for k, src in enumerate((cosine, sine)):
        waits.append(pltpu.make_async_copy(src, t_s.at[k], f_sem.at[k]))
        waits[-1].start()
    for side in (1, 0):
        part = [m for m in moves if m[1] // 512 == side]
        normalise(part, side * 512, gain, out_ref, r_s)
    for copy in waits:
        copy.wait()
    for side in range(2):
        rows = pl.ds(side * 512, 512)
        v = jnp.dot(out_ref[rows, :], w_s[...], preferred_element_type=jnp.float32)
        turned = rope(v, side, t_s)
        kv_ref[rows, :] = jnp.where(c == 0, turned, v).astype(jnp.bfloat16)


def queries(info, cosine, sine, rows_ref, *rest):
    pieces = rest[:8]
    q_ref, w_s, t_s, sem, w_sem = rest[8:]
    waits = weights_in(0, 256, info, pieces, w_s, w_sem)
    for k, src in enumerate((cosine, sine)):
        waits.append(pltpu.make_async_copy(src, t_s.at[k], sem.at[k]))
        waits[-1].start()
    for copy in waits:
        copy.wait()
    for side in range(2):
        rows = pl.ds(side * 512, 512)
        out = jnp.dot(rows_ref[rows, :], w_s[...], preferred_element_type=jnp.float32)
        for i in range(2):
            v = out[:, i * 128 : i * 128 + 128]
            v = rope(v, side, t_s).astype(jnp.bfloat16)
            for b in range(2):
                q_ref[side * 2 + b, i * CH : i * CH + CH, :] = v[b * CH : b * CH + CH]


def attention(first, qpos, where, q_ref, *rest):
    pieces = rest[:8]
    out_ref, kv_s, s_s, m_s, l_s, o_s, sem = rest[8:]
    c = qpos[4]
    copies = []
    for k, piece in enumerate(pieces):
        kind = c if k < 4 else 1 - c
        copies.append(
            pltpu.make_async_copy(
                piece, kv_s.at[kind, pl.ds((k % 4) * 1024, 1024), :], sem.at[k]
            )
        )
        copies[-1].start()
    size = 2 * CH
    factor = LOG2E / HEAD_SIZE**0.5
    m_s[...] = jnp.full((2, size, 128), -1e30, jnp.float32)
    l_s[...] = jnp.zeros((2, size, 128), jnp.float32)
    o_s[...] = jnp.zeros((2, size, 128), jnp.float32)
    for copy in copies:
        copy.wait()
    here = [qpos[first], qpos[first + 1]]
    pairs = [here[0] // 2, here[1] // 2]

    def keys(kind, p):
        return kv_s[kind, pl.ds(pl.multiple_of(where[p] * CH, CH), CH), :]

    half = size // 2

    def dots(b, t, h):
        return [
            lax.dot_general(
                q_ref[first + b, h * half : h * half + half, :],
                keys(0, 2 * t + i),
                (((1,), (1,)), ((), ())),
                preferred_element_type=jnp.float32,
            )
            for i in range(2)
        ]

    def keep(b, t, h, s0, s1):
        rows = slice(h * half, h * half + half)
        s_s[b, 2 * t, rows, :] = s0
        s_s[b, 2 * t + 1, rows, :] = s1
        top = jnp.maximum(
            jnp.maximum(s0[:, :128], s0[:, 128:]), jnp.maximum(s1[:, :128], s1[:, 128:])
        )
        m_s[b, rows, :] = jnp.maximum(m_s[b, rows, :], top)

    def scores(b, t):
        for h in range(2):
            keep(b, t, h, *dots(b, t, h))

    def last_scores(b):
        t = pairs[b]
        row = lax.broadcasted_iota(jnp.int32, (half, CH), 0)
        gap = row - lax.broadcasted_iota(jnp.int32, (half, CH), 1) + (here[b] - 2 * t) * CH
        for h in range(2):
            s0, s1 = dots(b, t, h)
            keep(b, t, h, jnp.where(gap >= 0, s0, -1e30), jnp.where(gap >= CH, s1, -1e30))
        m_s[b] = jnp.broadcast_to(jnp.max(m_s[b], axis=1, keepdims=True), (size, 128))

    def weigh(b, t):
        v = jnp.concatenate([keys(1, 2 * t), keys(1, 2 * t + 1)], axis=0)
        for h in range(2):
            rows = slice(h * half, h * half + half)
            m = m_s[b, rows, :]
            p = [
                jnp.exp2((s_s[b, 2 * t + k // 2, rows, k % 2 * 128 : k % 2 * 128 + 128] - m) * factor)
                for k in range(4)
            ]
            l_s[b, rows, :] += (p[0] + p[1]) + (p[2] + p[3])
            p = jnp.concatenate([x.astype(jnp.bfloat16) for x in p], axis=1)
            o_s[b, rows, :] += jnp.dot(p, v, preferred_element_type=jnp.float32)

    def store(b):
        total = jnp.sum(l_s[b], axis=1, keepdims=True)
        o = (o_s[b] / total).astype(jnp.bfloat16)
        for i in range(2):
            out_ref[b * CH : b * CH + CH, i * 128 : i * 128 + 128] = o[i * CH : i * CH + CH]

    def loop(low, high, *work):
        def step(t, carry):
            for f, b in work:
                f(b, t)
            return carry

        lax.fori_loop(low, high, step, 0)

    loop(0, pairs[0], (scores, 0))
    last_scores(0)
    both = jnp.minimum(pairs[0] + 1, pairs[1])
    loop(0, both, (scores, 1), (weigh, 0))
    loop(both, pairs[1], (scores, 1))
    loop(both, pairs[0] + 1, (weigh, 0))
    store(0)
    last_scores(1)
    loop(0, pairs[1] + 1, (weigh, 1))
    store(1)


def assemble(info, *rest):
    weights = rest[:8]
    w_ref, sem = rest[8:]
    z, y, l = info[1], info[2], info[3]
    waits = []
    for k, w in enumerate(weights):
        yy = lax.rem(y + 4 - BACK[k % 4], 4)
        for n in range(2):
            zz = lax.rem(z + 4 - BACK[k // 4 * 2 + n], 4)
            row = pl.multiple_of(zz * 512, 512)
            for i in range(2):
                col = pl.multiple_of((lax.rem(l + i, 2) * 4 + yy) * 128, 128)
                copy = pltpu.make_async_copy(
                    w.at[n, i], w_ref.at[pl.ds(row, 512), pl.ds(col, 128)], sem.at[len(waits)]
                )
                copy.start()
                waits.append(copy)
    for copy in waits:
        copy.wait()


def out_project(info, hidden, target, w_ref, *rest):
    pieces = rest[:8]
    out_ref, loss_ref, a_s, sem = rest[8:]
    c, x = info[0], info[4]
    waits = []
    for k, piece in enumerate(pieces):
        group = lax.rem(x + (0, 3, 1, 2)[k % 4], 4)
        core = c if k < 4 else 1 - c
        col = pl.multiple_of(group * 512 + core * 256, 256)
        copy = pltpu.make_async_copy(piece, a_s.at[:, pl.ds(col, 256)], sem.at[k])
        copy.start()
        waits.append(copy)
    for copy in waits:
        copy.wait()
    loss = jnp.zeros((8, 128), jnp.float32)
    for t in range(4):
        cols = slice(t * 256, t * 256 + 256)
        branch = jnp.dot(
            a_s[...], w_ref[:, cols], preferred_element_type=jnp.float32
        ).astype(jnp.bfloat16)
        out_ref[:, cols] = branch
        r = hidden[:, cols].astype(jnp.float32) + branch.astype(jnp.float32)
        r = r - target[:, cols].astype(jnp.float32)
        r = jnp.sum((r * r).reshape(64, 8, 256), axis=0)
        loss = loss + (r[:, :128] + r[:, 128:])
    loss_ref[...] = loss


def kernel(body, out_shape, scratch, ins, mib, outs=None):
    if outs is None:
        outs = jax.tree.map(lambda s: VMEM, out_shape)
    out_shape = jax.tree.map(
        lambda s, o: pltpu.HBM(s.shape, s.dtype) if o is FIX else s, out_shape, outs
    )
    call = pl.pallas_call(
        body,
        out_shape=out_shape,
        in_specs=ins,
        out_specs=outs,
        scratch_shapes=scratch,
        compiler_params=pltpu.CompilerParams(vmem_limit_bytes=mib * 2**20),
    )

    def run(*args):
        return call(
            *[
                pltpu.with_memory_space_constraint(v, pltpu.HBM) if i is FIX else v
                for v, i in zip(args, ins)
            ]
        )

    return run


SMEM = pl.BlockSpec(memory_space=pltpu.SMEM)
VMEM = pl.BlockSpec(memory_space=pltpu.VMEM)
ANY = pl.BlockSpec(memory_space=pl.ANY)
FIX = pl.BlockSpec(memory_space=pl.ANY)


def shape(*dims, kind=jnp.bfloat16):
    return jax.ShapeDtypeStruct(dims, kind)


def body(hidden, target, gain, w_query, w_key, value_matrix, w_out, block_order):
    z, l, h, c, y = (lax.axis_index(a) for a in (Z, L, H, C, Y))
    x = 2 * h + l
    local = hidden[0]
    w0 = jnp.concatenate([w_query[:, :256], w_key], axis=1)
    w1 = jnp.concatenate([w_query[:, 256:], value_matrix], axis=1)
    wa = send(jnp.where(l == 0, w0, w1), (L, C), lambda l, c: (c, l))
    wb = send(jnp.where(l == 0, w1, w0), (L, C), lambda l, c: (c, 1 - l))
    low, high = local[:256], local[256:]
    sal, sah = along_x(low, 1), along_x(high, 1)
    sbl, sbh = along_x(low, -1), along_x(high, -1)
    d0 = swap(local)
    w = around(jnp.stack(around(wa, Y)), Z)
    w = w + around(jnp.stack(around(wb, Z)), Y)
    fa, fb = along_x(sal, 1), along_x(sbh, -1)
    dal, dah, dbl, dbh = (
        swap(v) for v in (sal, sah, sbl, sbh)
    )
    dfa, dfb = swap(fa), swap(fb)

    def turn(flip):
        return send(
            w_out, (Z, L, H, C), lambda z, l, h, c: (2 * h + c, (l + flip) % 2, z // 2, z % 2)
        )

    o = jnp.stack([turn(0), turn(1)])
    o = around(o, Z)
    oa, ob = jnp.stack(o[:2]), jnp.stack(o[2:])

    def along_y(value, by):
        return send(value, (Y,), lambda i: ((i + by) % 4,))

    oa1, ob1 = along_y(oa, 1), along_y(ob, 1)
    oa3, ob3 = along_y(oa, 3), along_y(ob, 3)
    oa2, ob2 = along_y(oa1, 1), along_y(ob3, 3)
    outs = [oa, oa1, oa3, oa2, ob, ob1, ob3, ob2]
    slots = lax.iota(jnp.int32, 16)

    def places(index):
        return jnp.sum(jnp.where(index[:, None] == slots[None, :], block_order[None, :], 0), axis=1)

    two = lax.iota(jnp.int32, 2)
    sides = jnp.stack([l, 1 - l])
    zs = (z + 4 - jnp.array(BACK, jnp.int32)) % 4
    index = (zs[:, None, None] * 2 + sides[None, :, None]) * 2 + two[None, None, :]
    kpos = places(index.reshape(16))
    qpos = kpos[:4]
    inverse = jnp.sum(jnp.where(kpos[None, :] == slots[:, None], slots[None, :], 0), axis=1)
    rows = (qpos[:, None] * CH + lax.iota(jnp.int32, CH)[None, :]).reshape(2, 512)
    half = HEAD_SIZE // 2
    freqs = ROPE_BASE ** (-(jnp.arange(half, dtype=jnp.float32) * 2.0) / HEAD_SIZE)
    spread = jnp.where(
        lax.iota(jnp.int32, HEAD_SIZE)[None, :] < half, rows[0][:, None], rows[1][:, None]
    ).astype(jnp.float32)
    angles = spread * jnp.concatenate([freqs, freqs])[None, :]
    cosine, sine = jnp.cos(angles), jnp.sin(angles)
    ha, hb = ((x + 3) % 4) // 2, ((x + 1) % 4) // 2

    far_chunks = [2 * ha + c, 2 * ha + 1 - c, 2 * hb + c, 2 * hb + 1 - c]
    near_chunks = [2 * h + c, 2 * h + 1 - c, 2 - 2 * h + c, 3 - 2 * h - c]
    info = jnp.stack(near_chunks + [c, z, y] + far_chunks).astype(jnp.int32)
    gain = gain.reshape(1, MODEL_WIDTH)
    dma = pltpu.SemaphoreType.DMA
    table_s = [pltpu.VMEM((2, 512, 128), jnp.float32), pltpu.VMEM((512, 128), jnp.float32)]
    layout = tuple((7 + k // 2, 512 + k % 2 * 256, 256) for k in range(8)) + (
        (0, 0, 512), (1, 0, 512), (2, 0, 256), (2, 256, 256), (3, 0, 256), (3, 256, 256),
    )
    kv, all_rows = kernel(
        functools.partial(norm_keys, layout),
        (shape(1024, HEAD_SIZE), shape(1024, MODEL_WIDTH)),
        [pltpu.VMEM((4096, 128), jnp.bfloat16)] + table_s + [dma((14,)), dma((32,)), dma((2,))],
        [SMEM, VMEM] + [FIX] * 10 + [ANY] * 8 + [FIX] + [ANY] * 5,
        20,
    )(
        info, gain, cosine, sine, *w, sal, sah, dal, dah, sbl, sbh, dbl, dbh,
        local, d0, fa, fb, dfa, dfb,
    )
    mine = around(kv, Z)
    pieces = mine + [swap(v) for v in mine]
    q = kernel(
        queries,
        shape(4, 2 * CH, HEAD_SIZE),
        [pltpu.VMEM((4096, 256), jnp.bfloat16), table_s[0], dma((2,)), dma((32,))],
        [SMEM, FIX, FIX, VMEM] + [FIX] * 8,
        20,
    )(info, cosine, sine, all_rows, *w)

    def attended(first):
        return kernel(
            functools.partial(attention, first),
            shape(512, 256),
            [
                pltpu.VMEM((2, 4096, HEAD_SIZE), jnp.bfloat16),
                pltpu.VMEM((2, 16, 2 * CH, CH), jnp.float32),
                pltpu.VMEM((2, 2 * CH, 128), jnp.float32),
                pltpu.VMEM((2, 2 * CH, 128), jnp.float32),
                pltpu.VMEM((2, 2 * CH, 128), jnp.float32),
                pltpu.SemaphoreType.DMA((8,)),
            ],
            [SMEM, SMEM, VMEM] + [ANY] * 8,
            28,
        )(qinfo, inverse.astype(jnp.int32), q, *pieces)

    qinfo = jnp.concatenate([qpos, c[None]]).astype(jnp.int32)
    far = attended(2)
    near = attended(0)
    got = [near, along_x(far, 1), along_x(far, -1), along_x(near, 2)]
    got = got + [swap(v) for v in got]
    info = jnp.stack([c, z, y, l, x]).astype(jnp.int32)
    w = kernel(assemble, shape(2048, 1024), [dma((32,))], [SMEM] + [ANY] * 8, 8)(info, *outs)
    branch, squares = kernel(
        out_project,
        (shape(512, 1024), shape(8, 128, kind=jnp.float32)),
        [pltpu.VMEM((512, 2048), jnp.bfloat16), dma((8,))],
        [SMEM, VMEM, VMEM, VMEM] + [ANY] * 8,
        20,
    )(info, local, target[0], w, *got)
    squares = squares + swap(squares)
    squares = jnp.broadcast_to(squares[None], (64, 8, 128)).reshape(512, 128)
    squares = lax.all_to_all(squares, (Z, L, H, Y), 0, 0, tiled=True)
    loss = jnp.sum(squares) / (4 * 4096 * MODEL_WIDTH)
    return (branch[None], loss)


def solution(mesh):
    split = Mesh(mesh.devices.reshape(4, 2, 2, 2, 4), (Z, L, H, C, Y))
    rows = P(Y, (Z, L), (H, C))
    weight = P((Z, L, Y), (H, C))
    return jax.shard_map(
        body,
        mesh=split,
        in_specs=(rows, rows, P(), weight, weight, weight, P((H, C), (Z, L, Y)), P()),
        out_specs=(rows, P()),
        check_vma=False,
    )
```

```python
import functools

import jax
import jax.numpy as jnp
import numpy as np
from jax import lax
from jax.experimental import pallas as pl
from jax.experimental.pallas import tpu as pltpu
from jax.sharding import Mesh
from jax.sharding import PartitionSpec as P

MODEL_WIDTH = 4096
HEAD_SIZE = 128
CH = 256
ROPE_BASE = 500000.0
Z, L, H, C, Y = "ctx_0", "ctx_1", "tp_0", "tp_1", "dp"
SIZE = {Z: 4, L: 2, H: 2, C: 2, Y: 4}
BACK = (0, 1, 3, 2)
LOG2E = 1.4426950408889634


def send(value, axes, where):
    order = [a for a in (Z, L, H, C, Y) if a in axes]
    sizes = [SIZE[a] for a in order]
    pairs = []
    for i in range(int(np.prod(sizes))):
        at = dict(zip(order, (int(k) for k in np.unravel_index(i, sizes))))
        to = where(*[at[a] for a in axes])
        if to is not None:
            goal = dict(zip(axes, to))
            pairs.append((i, int(np.ravel_multi_index([goal[a] for a in order], sizes))))
    return lax.ppermute(value, tuple(order), pairs)


def swap(value):
    return send(value, (C,), lambda c: (1 - c,))


def around(value, axis):
    out = [value]
    for by in BACK[1:]:
        out.append(send(value, (axis,), lambda i, by=by: ((i + by) % 4,)))
    return out


def along_x(value, step):
    def where(h, l):
        x = (2 * h + l + step) % 4
        return (x // 2, x % 2)

    return send(value, (H, L), where)


def fetch(layout, info, sources, x_s, sem):
    moves = []
    for src, (slot, rows, size) in zip(sources, layout):
        col = pl.multiple_of(info[slot] * 1024, 1024)
        copy = pltpu.make_async_copy(
            src, x_s.at[pl.ds(rows, size), pl.ds(col, 1024)], sem.at[len(moves)]
        )
        copy.start()
        moves.append((copy, rows, size, col))
    return moves


def normalise(moves, base, gain, x_s, r_s):
    tile = 64
    r_s[...] = jnp.zeros((512, 128), jnp.float32)
    for copy, first, size, col in moves:
        copy.wait()

        def squares(t, carry, first=first, col=col):
            at = pl.multiple_of(first + t * tile, tile)
            rows = pl.ds(at - base, tile)
            part = r_s[rows, :]
            for k in range(8):
                x = x_s[pl.ds(at, tile), pl.ds(col + k * 128, 128)].astype(jnp.float32)
                part = part + x * x
            r_s[rows, :] = part
            return carry

        lax.fori_loop(0, size // tile, squares, 0)
    mean = jnp.sum(r_s[...], axis=1, keepdims=True) * (1.0 / MODEL_WIDTH)
    r_s[...] = jnp.broadcast_to(lax.rsqrt(mean + 1e-05), (512, 128))

    def scale(t, carry):
        at = pl.multiple_of(t * 32, 32)
        r = r_s[pl.ds(at, 32), :]
        rows = pl.ds(at + base, 32)
        for k in range(32):
            cols = slice(k * 128, k * 128 + 128)
            x = x_s[rows, cols].astype(jnp.float32)
            x_s[rows, cols] = (x * r * gain[:, cols]).astype(jnp.bfloat16)
        return carry

    lax.fori_loop(0, 16, scale, 0)


def weights_in(first, width, info, pieces, w_s, sem):
    c, z, y = info[4], info[5], info[6]
    waits = []
    for k, w in enumerate(pieces):
        for n in range(4):
            dz, dy = (BACK[k], BACK[n]) if k < 4 else (BACK[n], BACK[k - 4])
            part = c if k < 4 else 1 - c
            row = lax.rem(z + 4 - dz, 4) * 1024 + part * 512 + lax.rem(y + 4 - dy, 4) * 128
            copy = pltpu.make_async_copy(
                w.at[n, :, pl.ds(first, width)],
                w_s.at[pl.ds(pl.multiple_of(row, 128), 128), :],
                sem.at[len(waits)],
            )
            copy.start()
            waits.append(copy)
    return waits


def rope(v, side, t_s):
    left = lax.broadcasted_iota(jnp.int32, (512, HEAD_SIZE), 1) < HEAD_SIZE // 2
    cs, sn = t_s[0], t_s[1]
    low = left if side == 0 else jnp.logical_not(left)
    cb = jnp.where(low, cs, pltpu.roll(cs, 64, 1))
    sb = jnp.where(low, sn, pltpu.roll(sn, 64, 1))
    return v * cb + pltpu.roll(v, 64, 1) * jnp.where(left, -sb, sb)


def norm_keys(layout, info, gain, cosine, sine, *rest):
    count = len(layout)
    pieces, rest = rest[:8], rest[8:]
    kv_ref, out_ref, w_s, t_s, r_s, sem, w_sem, f_sem = rest[count:]
    c = info[4]
    moves = fetch(layout, info, rest[:count], out_ref, sem)
    waits = weights_in(256, 128, info, pieces, w_s, w_sem)
    for k, src in enumerate((cosine, sine)):
        waits.append(pltpu.make_async_copy(src, t_s.at[k], f_sem.at[k]))
        waits[-1].start()
    for side in (1, 0):
        part = [m for m in moves if m[1] // 512 == side]
        normalise(part, side * 512, gain, out_ref, r_s)
    for copy in waits:
        copy.wait()
    for side in range(2):
        rows = pl.ds(side * 512, 512)
        v = jnp.dot(out_ref[rows, :], w_s[...], preferred_element_type=jnp.float32)
        turned = rope(v, side, t_s)
        kv_ref[rows, :] = jnp.where(c == 0, turned, v).astype(jnp.bfloat16)


def queries(info, cosine, sine, rows_ref, *rest):
    pieces = rest[:8]
    q_ref, w_s, t_s, sem, w_sem = rest[8:]
    waits = weights_in(0, 256, info, pieces, w_s, w_sem)
    for k, src in enumerate((cosine, sine)):
        waits.append(pltpu.make_async_copy(src, t_s.at[k], sem.at[k]))
        waits[-1].start()
    for copy in waits:
        copy.wait()
    for side in range(2):
        rows = pl.ds(side * 512, 512)
        out = jnp.dot(rows_ref[rows, :], w_s[...], preferred_element_type=jnp.float32)
        for i in range(2):
            v = out[:, i * 128 : i * 128 + 128]
            v = rope(v, side, t_s).astype(jnp.bfloat16)
            for b in range(2):
                q_ref[side * 2 + b, i * CH : i * CH + CH, :] = v[b * CH : b * CH + CH]


def attention(first, qpos, where, q_ref, *rest):
    pieces = rest[:8]
    out_ref, kv_s, s_s, m_s, l_s, o_s, sem = rest[8:]
    c = qpos[4]
    copies = []
    for k, piece in enumerate(pieces):
        kind = c if k < 4 else 1 - c
        copies.append(
            pltpu.make_async_copy(
                piece, kv_s.at[kind, pl.ds((k % 4) * 1024, 1024), :], sem.at[k]
            )
        )
        copies[-1].start()
    size = 2 * CH
    factor = LOG2E / HEAD_SIZE**0.5
    m_s[...] = jnp.full((2, size, 128), -1e30, jnp.float32)
    l_s[...] = jnp.zeros((2, size, 128), jnp.float32)
    o_s[...] = jnp.zeros((2, size, 128), jnp.float32)
    for copy in copies:
        copy.wait()
    here = [qpos[first], qpos[first + 1]]
    pairs = [here[0] // 2, here[1] // 2]

    def keys(kind, p):
        return kv_s[kind, pl.ds(pl.multiple_of(where[p] * CH, CH), CH), :]

    half = size // 2

    def dots(b, t, h):
        return [
            lax.dot_general(
                q_ref[first + b, h * half : h * half + half, :],
                keys(0, 2 * t + i),
                (((1,), (1,)), ((), ())),
                preferred_element_type=jnp.float32,
            )
            for i in range(2)
        ]

    def keep(b, t, h, s0, s1):
        rows = slice(h * half, h * half + half)
        s_s[b, 2 * t, rows, :] = s0
        s_s[b, 2 * t + 1, rows, :] = s1
        top = jnp.maximum(
            jnp.maximum(s0[:, :128], s0[:, 128:]), jnp.maximum(s1[:, :128], s1[:, 128:])
        )
        m_s[b, rows, :] = jnp.maximum(m_s[b, rows, :], top)

    def scores(b, t):
        for h in range(2):
            keep(b, t, h, *dots(b, t, h))

    def last_scores(b):
        t = pairs[b]
        row = lax.broadcasted_iota(jnp.int32, (half, CH), 0)
        gap = row - lax.broadcasted_iota(jnp.int32, (half, CH), 1) + (here[b] - 2 * t) * CH
        for h in range(2):
            s0, s1 = dots(b, t, h)
            keep(b, t, h, jnp.where(gap >= 0, s0, -1e30), jnp.where(gap >= CH, s1, -1e30))
        m_s[b] = jnp.broadcast_to(jnp.max(m_s[b], axis=1, keepdims=True), (size, 128))

    def weigh(b, t):
        v = jnp.concatenate([keys(1, 2 * t), keys(1, 2 * t + 1)], axis=0)
        for h in range(2):
            rows = slice(h * half, h * half + half)
            m = m_s[b, rows, :]
            p = [
                jnp.exp2((s_s[b, 2 * t + k // 2, rows, k % 2 * 128 : k % 2 * 128 + 128] - m) * factor)
                for k in range(4)
            ]
            l_s[b, rows, :] += (p[0] + p[1]) + (p[2] + p[3])
            p = jnp.concatenate([x.astype(jnp.bfloat16) for x in p], axis=1)
            o_s[b, rows, :] += jnp.dot(p, v, preferred_element_type=jnp.float32)

    def store(b):
        total = jnp.sum(l_s[b], axis=1, keepdims=True)
        o = (o_s[b] / total).astype(jnp.bfloat16)
        for i in range(2):
            out_ref[b * CH : b * CH + CH, i * 128 : i * 128 + 128] = o[i * CH : i * CH + CH]

    def loop(low, high, *work):
        def step(t, carry):
            for f, b in work:
                f(b, t)
            return carry

        lax.fori_loop(low, high, step, 0)

    loop(0, pairs[0], (scores, 0))
    last_scores(0)
    both = jnp.minimum(pairs[0] + 1, pairs[1])
    loop(0, both, (scores, 1), (weigh, 0))
    loop(both, pairs[1], (scores, 1))
    loop(both, pairs[0] + 1, (weigh, 0))
    store(0)
    last_scores(1)
    loop(0, pairs[1] + 1, (weigh, 1))
    store(1)


def assemble(info, *rest):
    weights = rest[:4]
    w_ref, sem = rest[4:]
    z, y, l = info[1], info[2], info[3]
    waits = []
    for k, w in enumerate(weights):
        yy = lax.rem(y + 4 - BACK[k], 4)
        for n, dz in enumerate(BACK):
            row = pl.multiple_of(lax.rem(z + 4 - dz, 4) * 512, 512)
            for i in range(2):
                col = pl.multiple_of((lax.rem(l + i, 2) * 4 + yy) * 128, 128)
                copy = pltpu.make_async_copy(
                    w.at[n, i], w_ref.at[pl.ds(row, 512), pl.ds(col, 128)], sem.at[len(waits)]
                )
                copy.start()
                waits.append(copy)
    for copy in waits:
        copy.wait()


def out_project(info, hidden, target, w_ref, *rest):
    pieces = rest[:8]
    out_ref, loss_ref, a_s, sem = rest[8:]
    c, x = info[0], info[4]
    waits = []
    for k, piece in enumerate(pieces):
        group = lax.rem(x + (0, 3, 1, 2)[k % 4], 4)
        core = c if k < 4 else 1 - c
        col = pl.multiple_of(group * 512 + core * 256, 256)
        copy = pltpu.make_async_copy(piece, a_s.at[:, pl.ds(col, 256)], sem.at[k])
        copy.start()
        waits.append(copy)
    for copy in waits:
        copy.wait()
    loss = jnp.zeros((8, 128), jnp.float32)
    for t in range(4):
        cols = slice(t * 256, t * 256 + 256)
        branch = jnp.dot(
            a_s[...], w_ref[:, cols], preferred_element_type=jnp.float32
        ).astype(jnp.bfloat16)
        out_ref[:, cols] = branch
        r = hidden[:, cols].astype(jnp.float32) + branch.astype(jnp.float32)
        r = r - target[:, cols].astype(jnp.float32)
        r = jnp.sum((r * r).reshape(64, 8, 256), axis=0)
        loss = loss + (r[:, :128] + r[:, 128:])
    loss_ref[...] = loss


def kernel(body, out_shape, scratch, ins, mib, outs=None):
    if outs is None:
        outs = jax.tree.map(lambda s: VMEM, out_shape)
    out_shape = jax.tree.map(
        lambda s, o: pltpu.HBM(s.shape, s.dtype) if o is FIX else s, out_shape, outs
    )
    call = pl.pallas_call(
        body,
        out_shape=out_shape,
        in_specs=ins,
        out_specs=outs,
        scratch_shapes=scratch,
        compiler_params=pltpu.CompilerParams(vmem_limit_bytes=mib * 2**20),
    )

    def run(*args):
        return call(
            *[
                pltpu.with_memory_space_constraint(v, pltpu.HBM) if i is FIX else v
                for v, i in zip(args, ins)
            ]
        )

    return run


SMEM = pl.BlockSpec(memory_space=pltpu.SMEM)
VMEM = pl.BlockSpec(memory_space=pltpu.VMEM)
ANY = pl.BlockSpec(memory_space=pl.ANY)
FIX = pl.BlockSpec(memory_space=pl.ANY)


def shape(*dims, kind=jnp.bfloat16):
    return jax.ShapeDtypeStruct(dims, kind)


def body(hidden, target, gain, w_query, w_key, value_matrix, w_out, block_order):
    z, l, h, c, y = (lax.axis_index(a) for a in (Z, L, H, C, Y))
    x = 2 * h + l
    local = hidden[0]
    w0 = jnp.concatenate([w_query[:, :256], w_key], axis=1)
    w1 = jnp.concatenate([w_query[:, 256:], value_matrix], axis=1)
    wa = send(jnp.where(l == 0, w0, w1), (L, C), lambda l, c: (c, l))
    wb = send(jnp.where(l == 0, w1, w0), (L, C), lambda l, c: (c, 1 - l))
    low, high = local[:256], local[256:]
    sal, sah = along_x(low, 1), along_x(high, 1)
    sbl, sbh = along_x(low, -1), along_x(high, -1)
    d0 = swap(local)
    w = around(jnp.stack(around(wa, Y)), Z)
    w = w + around(jnp.stack(around(wb, Z)), Y)
    fa, fb = along_x(sal, 1), along_x(sbh, -1)
    dal, dah, dbl, dbh = (
        swap(v) for v in (sal, sah, sbl, sbh)
    )
    dfa, dfb = swap(fa), swap(fb)

    def turn(flip):
        return send(
            w_out, (Z, L, H, C), lambda z, l, h, c: (2 * h + c, (l + flip) % 2, z // 2, z % 2)
        )

    o = jnp.stack([turn(0), turn(1)])
    o = around(o, Z)
    o = jnp.stack(o)
    outs = around(o, Y)
    slots = lax.iota(jnp.int32, 16)

    def places(index):
        return jnp.sum(jnp.where(index[:, None] == slots[None, :], block_order[None, :], 0), axis=1)

    two = lax.iota(jnp.int32, 2)
    sides = jnp.stack([l, 1 - l])
    zs = (z + 4 - jnp.array(BACK, jnp.int32)) % 4
    index = (zs[:, None, None] * 2 + sides[None, :, None]) * 2 + two[None, None, :]
    kpos = places(index.reshape(16))
    qpos = kpos[:4]
    inverse = jnp.sum(jnp.where(kpos[None, :] == slots[:, None], slots[None, :], 0), axis=1)
    rows = (qpos[:, None] * CH + lax.iota(jnp.int32, CH)[None, :]).reshape(2, 512)
    half = HEAD_SIZE // 2
    freqs = ROPE_BASE ** (-(jnp.arange(half, dtype=jnp.float32) * 2.0) / HEAD_SIZE)
    spread = jnp.where(
        lax.iota(jnp.int32, HEAD_SIZE)[None, :] < half, rows[0][:, None], rows[1][:, None]
    ).astype(jnp.float32)
    angles = spread * jnp.concatenate([freqs, freqs])[None, :]
    cosine, sine = jnp.cos(angles), jnp.sin(angles)
    ha, hb = ((x + 3) % 4) // 2, ((x + 1) % 4) // 2

    far_chunks = [2 * ha + c, 2 * ha + 1 - c, 2 * hb + c, 2 * hb + 1 - c]
    near_chunks = [2 * h + c, 2 * h + 1 - c, 2 - 2 * h + c, 3 - 2 * h - c]
    info = jnp.stack(near_chunks + [c, z, y] + far_chunks).astype(jnp.int32)
    gain = gain.reshape(1, MODEL_WIDTH)
    dma = pltpu.SemaphoreType.DMA
    table_s = [pltpu.VMEM((2, 512, 128), jnp.float32), pltpu.VMEM((512, 128), jnp.float32)]
    layout = tuple((7 + k // 2, 512 + k % 2 * 256, 256) for k in range(8)) + (
        (0, 0, 512), (1, 0, 512), (2, 0, 256), (2, 256, 256), (3, 0, 256), (3, 256, 256),
    )
    kv, all_rows = kernel(
        functools.partial(norm_keys, layout),
        (shape(1024, HEAD_SIZE), shape(1024, MODEL_WIDTH)),
        [pltpu.VMEM((4096, 128), jnp.bfloat16)] + table_s + [dma((14,)), dma((32,)), dma((2,))],
        [SMEM, VMEM] + [FIX] * 10 + [ANY] * 8 + [FIX] + [ANY] * 5,
        20,
    )(
        info, gain, cosine, sine, *w, sal, sah, dal, dah, sbl, sbh, dbl, dbh,
        local, d0, fa, fb, dfa, dfb,
    )
    mine = around(kv, Z)
    pieces = mine + [swap(v) for v in mine]
    q = kernel(
        queries,
        shape(4, 2 * CH, HEAD_SIZE),
        [pltpu.VMEM((4096, 256), jnp.bfloat16), table_s[0], dma((2,)), dma((32,))],
        [SMEM, FIX, FIX, VMEM] + [FIX] * 8,
        20,
    )(info, cosine, sine, all_rows, *w)

    def attended(first):
        return kernel(
            functools.partial(attention, first),
            shape(512, 256),
            [
                pltpu.VMEM((2, 4096, HEAD_SIZE), jnp.bfloat16),
                pltpu.VMEM((2, 16, 2 * CH, CH), jnp.float32),
                pltpu.VMEM((2, 2 * CH, 128), jnp.float32),
                pltpu.VMEM((2, 2 * CH, 128), jnp.float32),
                pltpu.VMEM((2, 2 * CH, 128), jnp.float32),
                pltpu.SemaphoreType.DMA((8,)),
            ],
            [SMEM, SMEM, VMEM] + [ANY] * 8,
            28,
        )(qinfo, inverse.astype(jnp.int32), q, *pieces)

    qinfo = jnp.concatenate([qpos, c[None]]).astype(jnp.int32)
    far = attended(2)
    near = attended(0)
    got = [near, along_x(far, 1), along_x(far, -1), along_x(near, 2)]
    got = got + [swap(v) for v in got]
    info = jnp.stack([c, z, y, l, x]).astype(jnp.int32)
    w = kernel(assemble, shape(2048, 1024), [dma((32,))], [SMEM] + [ANY] * 4, 8)(info, *outs)
    branch, squares = kernel(
        out_project,
        (shape(512, 1024), shape(8, 128, kind=jnp.float32)),
        [pltpu.VMEM((512, 2048), jnp.bfloat16), dma((8,))],
        [SMEM, VMEM, VMEM, VMEM] + [ANY] * 8,
        20,
    )(info, local, target[0], w, *got)
    squares = squares + swap(squares)
    squares = jnp.broadcast_to(squares[None], (64, 8, 128)).reshape(512, 128)
    squares = lax.all_to_all(squares, (Z, L, H, Y), 0, 0, tiled=True)
    loss = jnp.sum(squares) / (4 * 4096 * MODEL_WIDTH)
    return (branch[None], loss)


def solution(mesh):
    split = Mesh(mesh.devices.reshape(4, 2, 2, 2, 4), (Z, L, H, C, Y))
    rows = P(Y, (Z, L), (H, C))
    weight = P((Z, L, Y), (H, C))
    return jax.shard_map(
        body,
        mesh=split,
        in_specs=(rows, rows, P(), weight, weight, weight, P((H, C), (Z, L, Y)), P()),
        out_specs=(rows, P()),
        check_vma=False,
    )
```
